128 devices in a mesh: row: 8 (over z, core), col: 16 (over y, x).
Axes of the slice: x: 4, y: 4, z: 4, core: 2. Of those that a mesh axis runs over, the one named last changes fastest.
Arguments:
- load_amp: float32 [4096, 8192], P('row', 'col'), may hold values from 0.05 to 1
- load_mask: int32 [4096, 8192], P('row', 'col'), may hold values 0 or 1
- leak: float32 [4096, 8192], P('row', 'col'), may hold values from 0.001 to 0.05
- coarse_leak: float32 [1024, 2048], P('row', 'col'), may hold values from 0.01 to 0.5
- coarse_init: float32 [1024, 2048], P('row', 'col'), may hold values from 0 to 1
- via_fine: int32 [8, 32768], P('row', 'col'), may hold values from 0 to 262143
- via_coarse: int32 [8, 32768], P('row', 'col'), may hold values from 0 to 262143, as said below
- via_count: int32 [8, 256], P('row', 'col'), may hold values from 0 to 128, as said below
Outputs:
- fine_drop: float32 [4096, 8192], P('row', 'col')
- coarse_drop: float32 [1024, 2048], P('row', 'col')
The draws below stay inside these ranges and needn't reach their ends.
Inputs may be any that keep to these rules, and one draw needn't show every extreme that they name: `via_coarse`: slot s of a tile names a coarse node whose stored column lies in s // 128 * 128 to s // 128 * 128 + 127. `via_count`: slots of an owner past its count are padding and carry arbitrary indices. In each tile row some owner gets 128 live slots from every tile of that row.
All inputs are finite; a program needn't handle non-finite values. No bound on the sum of `load_mask` on one device may be relied on, other than what follows from the above.
Results may differ from the reference program's by a relative error of at most 0.00022.
Values sent between devices are 32-bit elements; how exact they have to be, the bound alone decides.
No kernel may reach another device: no remote copies, remote signals or barrier semaphores. Data moves between devices by JAX's collectives and lax.ppermute only.
A program may use at most 64 MiB of HBM per device.

```python
import math
import jax
import jax.numpy as jnp

FR = 512
FC = 512
CR = 128
CC = 128
GROUP = 16
VOWN = 128
ITERS = 4
OUTER = 1
CSWEEP = 2
NFR = 4096
NFC = 8192
NCR = 1024
NCC = 2048
VMAX = 2048
N_ROW = 8
N_COL = 16


def draw_via_coarse(key, part):
    columns = NCC // CC
    tiles_down = NCR // CR
    slot_all = jnp.arange(columns * VMAX, dtype=jnp.int32)
    owner = slot_all % VMAX // VOWN
    key_row, key_col = jax.random.split(jax.random.fold_in(key, 11))
    shape = (tiles_down, columns * VMAX)
    row_pick = jax.random.randint(key_row, shape, 0, CR, dtype=jnp.int32)
    col_pick = jax.random.randint(key_col, shape, 0, CC, dtype=jnp.int32)
    return (row_pick * NCC + owner[None, :] * CC + col_pick).astype(jnp.int32)


def draw_via_count(key, part):
    columns = NCC // CC
    tiles_down = NCR // CR
    key_base, key_full = jax.random.split(jax.random.fold_in(key, 23))
    base = jax.random.randint(key_base, (tiles_down, columns * columns), 0, VOWN + 1, dtype=jnp.int32)
    chosen = jax.random.randint(key_full, (tiles_down, 1), 0, columns, dtype=jnp.int32)
    owner = jnp.arange(columns * columns, dtype=jnp.int32) % columns
    return jnp.where(owner[None, :] == chosen, VOWN, base).astype(jnp.int32)


def touch_ends(array, stream_key, low, high):
    shape = array.shape
    place = [jax.random.randint(jax.random.fold_in(stream_key, axis), (), 0, shape[axis]) for axis in range(len(shape))]
    array = array.at[tuple(place)].set(low)
    longest = shape.index(max(shape))
    place[longest] = (place[longest] + 1) % shape[longest]
    return array.at[tuple(place)].set(high)


def levels(own_key, dims, cuts, low, top_value):
    level, own = 1.0, jax.random.fold_in(own_key, 6)
    for dim, blocks in cuts:
        draws = jnp.exp(jax.random.uniform(jax.random.fold_in(own, dim), (blocks,), jnp.float32, low / len(cuts), top_value / len(cuts)))
        level = level * jnp.repeat(draws, dims[dim] // blocks).reshape([-1 if axis == dim else 1 for axis in range(len(dims))])
    return level


def setup_inputs(seed: int = 0) -> dict:
    key_of = jax.random.split(jax.random.key(seed), 9)
    load_amp = jnp.clip(jnp.exp(math.log(1.0) - 2.9957323 * jax.random.uniform(key_of[0], (NFR, NFC), jnp.float32) ** levels(key_of[0], (NFR, NFC), ((0, 8), (1, 16)), -0.2, 0.2)), 0.05, 1.0)
    load_mask = touch_ends((jax.random.randint(key_of[1], (NFR, NFC), 0, 2) < 1).astype(jnp.int32), jax.random.fold_in(key_of[1], 1), 0, 1)
    leak = jnp.clip(jnp.exp(math.log(0.05) - 3.912023 * jax.random.uniform(key_of[2], (NFR, NFC), jnp.float32) ** levels(key_of[2], (NFR, NFC), ((0, 8), (1, 16)), -0.2, 0.2)), 0.001, 0.05)
    coarse_leak = jnp.clip(jnp.exp(math.log(0.5) - 3.912023 * jax.random.uniform(key_of[3], (NCR, NCC), jnp.float32) ** levels(key_of[3], (NCR, NCC), ((0, 8), (1, 16)), -0.2, 0.2)), 0.01, 0.5)
    coarse_init = jnp.clip(1.0 * jax.random.uniform(key_of[4], (NCR, NCC), jnp.float32) ** levels(key_of[4], (NCR, NCC), ((0, 8), (1, 16)), -0.2, 0.2), 0.0, 1.0)
    via_fine = touch_ends(jax.random.randint(key_of[5], (N_ROW, VMAX * N_COL), 0, FR * FC), jax.random.fold_in(key_of[5], 1), 0, (FR * FC) - 1).astype(jnp.int32)
    via_coarse = draw_via_coarse(jax.random.fold_in(key_of[8], 71), 0)
    via_count = draw_via_count(jax.random.fold_in(key_of[8], 71), 0)
    return {"load_amp": load_amp, "load_mask": load_mask, "leak": leak, "coarse_leak": coarse_leak, "coarse_init": coarse_init, "via_fine": via_fine, "via_coarse": via_coarse, "via_count": via_count}


via_conductance = 2.0
coarse_conductance = 4.0
relaxation = 0.8


def fine_apply(field, diagonal):
    padded = jnp.pad(field, 1)
    beside = padded[2:, 1:-1] + padded[:-2, 1:-1] + padded[1:-1, 2:] + padded[1:-1, :-2]
    return diagonal * field - beside


def to_physical(stored):
    return stored.reshape(NCR, N_COL, CC // GROUP, GROUP).transpose(0, 2, 1, 3).reshape(NCR, NCC)


def to_stored(physical):
    return physical.reshape(NCR, CC // GROUP, N_COL, GROUP).transpose(0, 2, 1, 3).reshape(NCR, NCC)


def coarse_apply(stored, diagonal):
    padded = jnp.pad(to_physical(stored), 1)
    beside = padded[2:, 1:-1] + padded[:-2, 1:-1] + padded[1:-1, 2:] + padded[1:-1, :-2]
    return diagonal * stored - coarse_conductance * to_stored(beside)


def reference(load_amp, load_mask, leak, coarse_leak, coarse_init, via_fine, via_coarse, via_count):
    tile_row = jnp.arange(N_ROW, dtype=jnp.int32)[:, None]
    slot_all = jnp.arange(N_COL * VMAX, dtype=jnp.int32)[None, :]
    tile_col = slot_all // VMAX
    within = slot_all % VMAX
    owner = within // VOWN
    position = within % VOWN
    count_index = jnp.broadcast_to(tile_col * N_COL + owner, via_fine.shape).astype(jnp.int32)
    counts = jnp.take_along_axis(via_count, count_index, axis=1)
    weight = jnp.where(position < counts, via_conductance, 0.0).astype(jnp.float32).reshape(-1)
    fine_index = ((tile_row * FR + via_fine // FC) * NFC + tile_col * FC + via_fine % FC).reshape(-1)
    coarse_index = ((tile_row * CR + via_coarse // NCC) * NCC + via_coarse % NCC).reshape(-1)
    fine_diag = 4.0 + leak + jnp.zeros(NFR * NFC, jnp.float32).at[fine_index].add(weight).reshape(NFR, NFC)
    coarse_diag = 4.0 * coarse_conductance + coarse_leak + jnp.zeros(NCR * NCC, jnp.float32).at[coarse_index].add(weight).reshape(NCR, NCC)
    load = load_amp * load_mask.astype(jnp.float32)
    volt = coarse_init
    solution = jnp.zeros((NFR, NFC), jnp.float32)
    for outer_turn in range(OUTER):
        at_via = volt.reshape(-1)[coarse_index]
        rhs = load + jnp.zeros(NFR * NFC, jnp.float32).at[fine_index].add(weight * at_via).reshape(NFR, NFC)
        residual = rhs - fine_apply(solution, fine_diag)
        precond = residual / fine_diag
        direction = precond
        product = jnp.sum(residual * precond)
        for iteration in range(ITERS):
            image = fine_apply(direction, fine_diag)
            alpha = product / jnp.sum(direction * image)
            solution = solution + alpha * direction
            residual = residual - alpha * image
            if iteration + 1 < ITERS:
                precond = residual / fine_diag
                renewed = jnp.sum(residual * precond)
                direction = precond + (renewed / product) * direction
                product = renewed
        at_fine = weight * solution.reshape(-1)[fine_index]
        sources = jnp.zeros(NCR * NCC, jnp.float32).at[coarse_index].add(at_fine).reshape(NCR, NCC)
        for sweep_turn in range(CSWEEP):
            volt = volt + relaxation * (sources - coarse_apply(volt, coarse_diag)) / coarse_diag
    return solution, volt
```

```python
import jax
import jax.numpy as jnp
from jax import lax
from jax.experimental import pallas as pl
from jax.experimental.pallas import tpu as pltpu
from jax.sharding import PartitionSpec as P

F32 = jnp.float32
BF16 = jnp.bfloat16
HI = lax.Precision.HIGHEST
ROW, COL = "row", "col"

GROUP = 16
via_conductance = 2.0
coarse_conductance = 4.0
relaxation = 0.8

T = 512
CB = 128
NO = 16
L = 128
OFF = 16
EXT = OFF + T + 16
W = T + L

Q0, Q1, Q2 = 1.08976773, 1.76773384, 1.28562461


def iota(shape, dim):
    return lax.broadcasted_iota(jnp.int32, shape, dim)


def nt(a, b, precision=None):
    return lax.dot_general(
        a, b, (((1,), (1,)), ((), ())), precision=precision, preferred_element_type=F32
    )


def tn(a, b, precision=None):
    return lax.dot_general(
        a, b, (((0,), (0,)), ((), ())), precision=precision, preferred_element_type=F32
    )


def onehot(idx, n):
    return jnp.where(iota((n, idx.shape[1]), 0) == idx, 1.0, 0.0).astype(BF16)


def hi_lo(x):
    hi = x.astype(BF16).astype(F32)
    return hi, x - hi


def lanes(o):
    return slice(o * L, (o + 1) * L)


def diag_kernel(vf, wt, amp, mask, leak, load, invd, strips, a_s, b_s):
    for o in range(NO):
        f = vf[o : o + 1, :]
        a_s[:, lanes(o)] = onehot(f // T, T)
        b_s[:, lanes(o)] = jnp.where(iota((T, L), 0) == f % T, wt[o : o + 1, :], 0.0).astype(BF16)
    ld = amp[...] * mask[...].astype(F32)
    load[...] = ld
    inv = 1.0 / (4.0 + leak[...] + nt(a_s[...], b_s[...]))
    invd[...] = inv
    j, lane = iota((8, L), 0), iota((8, L), 1)
    first = jnp.where((j < 4) & (lane == j), 1.0, 0.0)
    last = jnp.where((j >= 4) & (lane == 120 + j), 1.0, 0.0)
    strips[0:8, :] = nt(first, ld[:, :L], HI) + nt(last, ld[:, T - L :], HI)
    strips[8:16, :] = nt(first, inv[:, :L], HI) + nt(last, inv[:, T - L :], HI)


def owner_onehots(held, r_s, c_s):
    for o in range(NO):
        h = held[o : o + 1, :]
        r_s[:, lanes(o)] = onehot(h >> 7, CB)
        c_s[:, lanes(o)] = onehot(h & (CB - 1), CB)


def lookup_kernel(held, volt, cleak, looked, cdiag, r_s, c_s):
    owner_onehots(held, r_s, c_s)
    vt = volt[...].T
    v1, rest = hi_lo(vt)
    v2, v3 = hi_lo(rest)
    for o in range(NO):
        pick = r_s[:, lanes(o)]
        rows = jnp.zeros((CB, L), F32)
        for v in (v3, v2, v1):
            rows = rows + jnp.dot(v.astype(BF16), pick, preferred_element_type=F32)
        sel = c_s[:, lanes(o)].astype(F32)
        looked[o : o + 1, :] = jnp.sum(rows * sel, axis=0, keepdims=True)
    count = nt(r_s[...], c_s[...])
    cdiag[...] = 4.0 * coarse_conductance + cleak[...] + via_conductance * count


def strips_kernel(vf, val, strips, volt, send_l, send_r, a_out):
    injl = []
    j = iota((8, L), 0)
    colid = jnp.where(j < 4, j, T - 8 + j)
    hs, ls = [], []
    for o in range(NO):
        f = vf[o : o + 1, :]
        a_out[:, lanes(o)] = onehot(f // T, T)
        hi, lo = hi_lo(val[o : o + 1, :])
        on = colid == f % T
        hs.append(jnp.where(on, hi, 0.0))
        ls.append(jnp.where(on, lo, 0.0))
    lhs = jnp.concatenate(
        [jnp.concatenate(hs, axis=1), jnp.concatenate(ls, axis=1)], axis=0
    ).astype(BF16)
    inj = nt(lhs, a_out[...])
    inv = strips[8:16, :]
    z = (strips[0:8, :] + inj[0:8] + inj[8:16]) * inv
    low = iota((8, T), 0) < 4
    send_l[:, :T] = jnp.where(low, z, pltpu.roll(inv, 4, 0))
    send_r[:, :T] = jnp.where(low, pltpu.roll(z, 4, 0), inv)
    g, lane = iota((8, CB), 0), iota((8, CB), 1)
    send_l[:, T:] = nt(jnp.where(lane == g * GROUP, 1.0, 0.0), volt[...], HI)
    send_r[:, T:] = nt(jnp.where(lane == g * GROUP + GROUP - 1, 1.0, 0.0), volt[...], HI)


def rhs_kernel(vf, val, load, invd, a, z, b_s):
    for o in range(NO):
        f = vf[o : o + 1, :]
        hi, lo = hi_lo(val[o : o + 1, :])
        on = iota((T, L), 0) == f % T
        b_s[:, lanes(o)] = jnp.where(on, hi, 0.0).astype(BF16)
        b_s[:, lanes(NO + o)] = jnp.where(on, lo, 0.0).astype(BF16)
    inj = nt(a[...], b_s[:, : NO * L]) + nt(a[...], b_s[:, NO * L :])
    z[...] = (load[...] + inj) * invd[...]


def edge_kernel(flags, z, invd, got_l, got_r, volt, zcol, icol, send_u, send_d):
    left = jnp.where(flags[1] > 0, 1.0, 0.0)
    right = jnp.where(flags[1] < NO - 1, 1.0, 0.0)
    j, lane = iota((8, L), 0), iota((8, L), 1)
    gl, gr = got_l[:, :T], got_r[:, :T]
    zc = tn(gr, jnp.where((j < 4) & (lane == j), right, 0.0), HI) + tn(
        gl, jnp.where((j < 4) & (lane == 124 + j), left, 0.0), HI
    )
    ic = tn(gr, jnp.where((j >= 4) & (lane == j - 4), right, 0.0), HI) + tn(
        gl, jnp.where((j >= 4) & (lane == 120 + j), left, 0.0), HI
    )
    zcol[...] = zc
    icol[...] = ic
    low = iota((8, W), 0) < 4
    zt = jnp.concatenate([z[0:8, :], zc[0:8]], axis=1)
    it = jnp.concatenate([invd[0:8, :], ic[0:8]], axis=1)
    zb = jnp.concatenate([z[T - 8 :, :], zc[T - 8 :]], axis=1)
    ib = jnp.concatenate([invd[T - 8 :, :], ic[T - 8 :]], axis=1)
    send_u[:, :W] = jnp.where(low, zt, pltpu.roll(it, 4, 0))
    send_d[:, :W] = jnp.where(low, pltpu.roll(zb, 4, 0), ib)
    send_u[:, W:] = volt[0:8, :]
    send_d[:, W:] = volt[CB - 8 :, :]


def neighbours(ref, start, rows):
    block = ref[pl.ds(start - 8, rows + 16), :]
    mid = block[8 : rows + 8]
    near = block[7 : rows + 7] + block[9 : rows + 9]
    return mid, near + pltpu.roll(mid, 1, 1) + pltpu.roll(mid, W - 1, 1)


def basis_kernel(flags, z, invd, zcol, icol, got_u, got_d, w_o, n1_o, n2_o, part, ie, ze, we, n1e, n2e):
    up = jnp.where(flags[0] > 0, 1.0, 0.0)
    down = jnp.where(flags[0] < 7, 1.0, 0.0)
    low = iota((8, W), 0) < 4
    top, bot = got_u[:, :W], got_d[:, :W]
    zero = jnp.zeros((8, W), F32)
    for e, own, col, t, b in (
        (ze, z, zcol, pltpu.roll(top, 4, 0), bot),
        (ie, invd, icol, top, pltpu.roll(bot, 4, 0)),
    ):
        e[0:8, :] = zero
        e[8:16, :] = jnp.where(low, 0.0, t) * up
        e[OFF : OFF + T, :T] = own[...]
        e[OFF : OFF + T, T:] = col[...]
        e[OFF + T : OFF + T + 8, :] = jnp.where(low, b, 0.0) * down
        e[OFF + T + 8 :, :] = zero
    for e in (we, n1e):
        e[0:8, :] = zero
        e[EXT - 8 :, :] = zero
    rows = 24

    def apply_to(src, dst, minus):
        def step(i, carry):
            start = pl.multiple_of(8 + i * rows, 8)
            mid, near = neighbours(src, start, rows)
            near = near * ie[pl.ds(start, rows), :]
            dst[pl.ds(start, rows), :] = mid - near if minus else near
            return carry

        lax.fori_loop(0, (EXT - 16) // rows, step, 0)

    apply_to(ze, we, True)
    apply_to(we, n1e, False)
    apply_to(n1e, n2e, False)

    def fold(p):
        return (p[:, 0:128] + p[:, 128:256]) + (p[:, 256:384] + p[:, 384:512])

    def gram(i, acc):
        start = pl.multiple_of(OFF + i * 8, 8)
        out = pl.multiple_of(i * 8, 8)
        n2w, near = neighbours(n2e, start, 8)
        inv = ie[pl.ds(start, 8), :T]
        n3 = near[:, :T] * inv
        n2 = n2w[:, :T]
        zz = ze[pl.ds(start, 8), :T]
        w = we[pl.ds(start, 8), :T]
        n1 = n1e[pl.ds(start, 8), :T]
        w_o[pl.ds(out, 8), :] = w
        n1_o[pl.ds(out, 8), :] = n1
        n2_o[pl.ds(out, 8), :] = n2
        d = 1.0 / inv
        bw, bn1, bn2 = w - n1, n1 - n2, n2 - n3
        e = (zz - Q0 * w - Q1 * n1 - Q2 * n2, w, n1, n2 - 0.25 * w)
        be = (w - Q0 * bw - Q1 * bn1 - Q2 * bn2, bw, bn1, bn2 - 0.25 * bw)
        new = []
        k = 0
        for p in range(4):
            de = d * e[p]
            for q in range(p, 4):
                new.append(acc[k] + fold(de * be[q]))
                k += 1
            new.append(acc[k] + fold(de * zz))
            k += 1
        return tuple(new)

    acc = lax.fori_loop(0, T // 8, gram, tuple(jnp.zeros((8, L), F32) for _ in range(14)))
    rows14 = jnp.concatenate(
        [jnp.sum(a, axis=0, keepdims=True) for a in acc] + [jnp.zeros((L - 14, L), F32)], axis=0
    )
    sums = nt(jnp.ones((8, L), F32), rows14, HI)
    part[...] = jnp.broadcast_to(sums[0:1, :], (L, L))


def solve_kernel(parts, z, w, n1, n2, vf, wt, x_o, cur, hi_s, lo_s):
    tot = jnp.sum(parts[...], axis=0, keepdims=True)
    lane = iota((1, L), 1)

    def pick(k):
        return jnp.sum(jnp.where(lane == k, tot, 0.0), axis=1, keepdims=True)

    h, b = {}, []
    k = 0
    for p in range(4):
        for q in range(p, 4):
            h[p, q] = pick(k)
            k += 1
        b.append(pick(k))
        k += 1
    floor = [3e-7 * h[p, p] for p in range(4)]
    inv = []
    for p in range(4):
        inv.append(jnp.where(h[p, p] > floor[p], 1.0 / h[p, p], 0.0))
        for q in range(p + 1, 4):
            f = h[p, q] * inv[p]
            for r in range(q, 4):
                h[q, r] = h[q, r] - f * h[p, r]
            b[q] = b[q] - f * b[p]
    c = [None] * 4
    for p in (3, 2, 1, 0):
        s = b[p]
        for q in range(p + 1, 4):
            s = s - h[p, q] * c[q]
        c[p] = s * inv[p]
    d1 = c[1] - Q0 * c[0] - 0.25 * c[3]
    d2 = c[2] - Q1 * c[0]
    d3 = c[3] - Q2 * c[0]
    x = c[0] * z[...] + d1 * w[...] + d2 * n1[...] + d3 * n2[...]
    x_o[...] = x
    hi, lo = hi_lo(x)
    hi_s[...] = hi.astype(BF16)
    lo_s[...] = lo.astype(BF16)
    for o in range(NO):
        f = vf[o : o + 1, :]
        sel = onehot(f % T, T)
        y = jnp.dot(hi_s[...], sel, preferred_element_type=F32) + jnp.dot(
            lo_s[...], sel, preferred_element_type=F32
        )
        y = jnp.where(iota((T, L), 0) == f // T, y, 0.0)
        cur[o : o + 1, :] = jnp.sum(y, axis=0, keepdims=True) * wt[o : o + 1, :]


def coarse_neighbours(flags, u, above, below, from_l, from_r):
    up = jnp.where(flags[0] > 0, 1.0, 0.0)
    down = jnp.where(flags[0] < 7, 1.0, 0.0)
    r, lane = iota((CB, CB), 0), iota((CB, CB), 1)
    g, gl = iota((8, CB), 0), iota((8, CB), 1)
    turned_l = jnp.where(g == 0, 0.0, pltpu.roll(from_l, 1, 0))
    turned_r = jnp.where(g == 7, 0.0, pltpu.roll(from_r, 7, 0))
    from_l = jnp.where(flags[1] == 0, turned_l, from_l)
    from_r = jnp.where(flags[1] == NO - 1, turned_r, from_r)
    seam_l = tn(from_l, jnp.where(gl == g * GROUP, 1.0, 0.0), HI)
    seam_r = tn(from_r, jnp.where(gl == g * GROUP + GROUP - 1, 1.0, 0.0), HI)
    beside = jnp.where(r == 0, above * up, pltpu.roll(u, 1, 0))
    beside += jnp.where(r == CB - 1, below * down, pltpu.roll(u, CB - 1, 0))
    beside += jnp.where(lane % GROUP == 0, seam_l, pltpu.roll(u, 1, 1))
    beside += jnp.where(lane % GROUP == GROUP - 1, seam_r, pltpu.roll(u, CB - 1, 1))
    return beside


def sweep(u, src, diag, beside):
    return u + relaxation * (src - (diag * u - coarse_conductance * beside)) / diag


def sweep1_kernel(flags, held, arrived, volt, cdiag, got_l, got_r, got_u, got_d, u_o, src_o, sl, sr, su, sd, r_s, c_s):
    for o in range(NO):
        h = held[o : o + 1, :]
        r_s[:, lanes(o)] = onehot(h >> 7, CB)
        on = iota((CB, L), 0) == (h & (CB - 1))
        v = arrived[o : o + 1, :]
        hi, lo = hi_lo(v)
        c_s[:, lanes(o)] = jnp.where(on, hi, 0.0).astype(BF16)
        c_s[:, lanes(NO + o)] = jnp.where(on, lo, 0.0).astype(BF16)
    src = nt(r_s[...], c_s[:, : NO * L]) + nt(r_s[...], c_s[:, NO * L :])
    u = volt[...]
    beside = coarse_neighbours(
        flags, u, got_u[7:8, W:], got_d[0:1, W:], got_l[:, T:], got_r[:, T:]
    )
    u = sweep(u, src, cdiag[...], beside)
    u_o[...] = u
    src_o[...] = src
    g, lane = iota((8, CB), 0), iota((8, CB), 1)
    sl[...] = nt(jnp.where(lane == g * GROUP, 1.0, 0.0), u, HI)
    sr[...] = nt(jnp.where(lane == g * GROUP + GROUP - 1, 1.0, 0.0), u, HI)
    su[...] = u[0:8, :]
    sd[...] = u[CB - 8 :, :]


def sweep2_kernel(flags, u, src, cdiag, got_l, got_r, got_u, got_d, u_o):
    beside = coarse_neighbours(flags, u[...], got_u[7:8, :], got_d[0:1, :], got_l[...], got_r[...])
    u_o[...] = sweep(u[...], src[...], cdiag[...], beside)


VM = pl.BlockSpec(memory_space=pltpu.VMEM)
SM = pl.BlockSpec(memory_space=pltpu.SMEM)


def call(body, outs, n_in, scratch=(), flags=False, flops=0):
    specs = ([SM] if flags else []) + [VM] * (n_in - (1 if flags else 0))
    shapes = [jax.ShapeDtypeStruct(s, d) for s, d in outs]
    return pl.pallas_call(
        body,
        out_shape=shapes,
        in_specs=specs,
        out_specs=[VM] * len(outs),
        scratch_shapes=[pltpu.VMEM(s, d) for s, d in scratch],
        cost_estimate=pl.CostEstimate(flops=flops, bytes_accessed=0, transcendentals=0),
    )


def ring(axis):
    n = lax.axis_size(axis)
    up = [(i, (i + 1) % n) for i in range(n)]
    return up, [(b, a) for a, b in up]


def swap(axis, to_low, to_high):
    up, down = ring(axis)
    return lax.ppermute(to_high, axis, up), lax.ppermute(to_low, axis, down)


def spread(x):
    return lax.all_to_all(x, COL, split_axis=0, concat_axis=0, tiled=True)


def per_device(load_amp, load_mask, leak, coarse_leak, coarse_init, via_fine, via_coarse, via_count):
    flags = jnp.where(
        jnp.arange(2, dtype=jnp.int32) == 0, lax.axis_index(ROW), lax.axis_index(COL)
    ).astype(jnp.int32)
    live = jnp.arange(L, dtype=jnp.int32)[None, :] < via_count.reshape(NO, 1)
    weight = jnp.where(live, via_conductance, 0.0).astype(F32)
    fine = via_fine.reshape(NO, L)
    coarse = via_coarse.reshape(NO, L)
    width = CB * NO
    request = jnp.where(live, coarse // width * CB + coarse % width % CB, -1)
    held = spread(request)

    tile, block, slots = ((T, T), F32), ((CB, CB), F32), ((NO, L), F32)
    load, invd, strips = call(
        diag_kernel, [tile, tile, ((16, T), F32)], 5,
        [((T, NO * L), BF16), ((T, NO * L), BF16)], flops=20_000_000_000,
    )(fine, weight, load_amp, load_mask, leak)

    looked, cdiag = call(
        lookup_kernel, [slots, block], 3, [((CB, NO * L), BF16), ((CB, NO * L), BF16)],
    )(held, coarse_init, coarse_leak)
    val = spread(looked) * weight

    side = ((8, W), F32)
    send_l, send_r, a = call(strips_kernel, [side, side, ((T, NO * L), BF16)], 4)(
        fine, val, strips, coarse_init
    )
    got_l, got_r = swap(COL, send_l, send_r)
    z = call(rhs_kernel, [tile], 5, [((T, 2 * NO * L), BF16)], flops=20_000_000_000)(
        fine, val, load, invd, a
    )[0]
    strip, rim = ((T, L), F32), ((8, W + CB), F32)
    zcol, icol, send_u, send_d = call(edge_kernel, [strip, strip, rim, rim], 6, flags=True)(
        flags, z, invd, got_l, got_r, coarse_init
    )
    got_u, got_d = swap(ROW, send_u, send_d)
    ext = ((EXT, W), F32)
    w, n1, n2, part = call(
        basis_kernel, [tile, tile, tile, ((L, L), F32)], 7, [ext] * 5, flags=True,
    )(flags, z, invd, zcol, icol, got_u, got_d)
    parts = lax.all_to_all(part, (ROW, COL), split_axis=0, concat_axis=0, tiled=True)
    fine_drop, current = call(
        solve_kernel, [tile, slots], 7, [((T, T), BF16), ((T, T), BF16)],
    )(parts, z, w, n1, n2, fine, weight)
    arrived = spread(current)
    seam, edge = ((8, CB), F32), ((8, CB), F32)
    u, src, sl, sr, su, sd = call(
        sweep1_kernel, [block, block, seam, seam, edge, edge], 9,
        [((CB, NO * L), BF16), ((CB, 2 * NO * L), BF16)], flags=True,
    )(flags, held, arrived, coarse_init, cdiag, got_l, got_r, got_u, got_d)
    hl, hr = swap(COL, sl, sr)
    hu, hd = swap(ROW, su, sd)
    coarse_drop = call(sweep2_kernel, [block], 8, flags=True)(
        flags, u, src, cdiag, hl, hr, hu, hd
    )[0]
    return fine_drop, coarse_drop


def solution(mesh):
    spec = P(ROW, COL)
    return jax.shard_map(
        per_device, mesh=mesh, in_specs=(spec,) * 8, out_specs=(spec, spec), check_vma=False
    )
```

```python
import jax
import jax.numpy as jnp
from jax import lax
from jax.experimental import pallas as pl
from jax.experimental.pallas import tpu as pltpu
from jax.sharding import PartitionSpec as P


F32 = jnp.float32
BF16 = jnp.bfloat16
HI = lax.Precision.HIGHEST
ROW, COL = "row", "col"

GROUP = 16
via_conductance = 2.0
coarse_conductance = 4.0
relaxation = 0.8

T = 512
CB = 128
NO = 16
L = 128
OFF = 16
EXT = OFF + T + 16
W = T + L

Q0, Q1, Q2 = 1.08976773, 1.76773384, 1.28562461


def iota(shape, dim):
    return lax.broadcasted_iota(jnp.int32, shape, dim)


def nt(a, b, precision=None):
    return lax.dot_general(
        a, b, (((1,), (1,)), ((), ())), precision=precision, preferred_element_type=F32
    )


def tn(a, b, precision=None):
    return lax.dot_general(
        a, b, (((0,), (0,)), ((), ())), precision=precision, preferred_element_type=F32
    )


def onehot(idx, n):
    return jnp.where(iota((n, idx.shape[1]), 0) == idx, 1.0, 0.0).astype(BF16)


def hi_lo(x):
    hi = x.astype(BF16).astype(F32)
    return hi, x - hi


def lanes(o):
    return slice(o * L, (o + 1) * L)


def diag_kernel(vf, wt, amp, mask, leak, zl, invd, strips, rims, a_s, b_s):
    for o in range(NO):
        f = vf[o : o + 1, :]
        a_s[:, lanes(o)] = onehot(f // T, T)
        b_s[:, lanes(o)] = jnp.where(iota((T, L), 0) == f % T, wt[o : o + 1, :], 0.0).astype(BF16)
    inv = 1.0 / (4.0 + leak[...] + nt(a_s[...], b_s[...]))
    z = amp[...] * mask[...].astype(F32) * inv
    zl[...] = z
    invd[...] = inv
    j, lane = iota((8, L), 0), iota((8, L), 1)
    first = jnp.where((j < 4) & (lane == j), 1.0, 0.0)
    last = jnp.where((j >= 4) & (lane == 120 + j), 1.0, 0.0)
    strips[0:8, :] = nt(first, z[:, :L], HI) + nt(last, z[:, T - L :], HI)
    strips[8:16, :] = nt(first, inv[:, :L], HI) + nt(last, inv[:, T - L :], HI)
    rims[0:8, :] = inv[0:8]
    rims[8:16, :] = inv[T - 8 :]


def lookup_kernel(held, volt, looked):
    v1, rest = hi_lo(volt[...].T)
    v2, v3 = hi_lo(rest)
    v = jnp.concatenate([v3, v2, v1], axis=0).astype(BF16)
    for i in range(NO // 2):
        h = jnp.concatenate([held[2 * i : 2 * i + 1, :], held[2 * i + 1 : 2 * i + 2, :]], axis=1)
        y = jnp.dot(v, onehot(h >> 7, CB), preferred_element_type=F32)
        y = y[:CB] + y[CB : 2 * CB] + y[2 * CB :]
        y = jnp.where(iota((CB, 2 * L), 0) == (h & (CB - 1)), y, 0.0)
        y = jnp.sum(y, axis=0, keepdims=True)
        looked[2 * i : 2 * i + 1, :] = y[:, :L]
        looked[2 * i + 1 : 2 * i + 2, :] = y[:, L:]


def strips_kernel(vf, wt, at_via, strips, volt, a_o, send_l, send_r):
    j = iota((8, L), 0)
    colid = jnp.where(j < 4, j, T - 8 + j)
    hs, ls = [], []
    for o in range(NO):
        f = vf[o : o + 1, :]
        a_o[:, lanes(o)] = onehot(f // T, T)
        hi, lo = hi_lo(at_via[o : o + 1, :] * wt[o : o + 1, :])
        on = colid == f % T
        hs.append(jnp.where(on, hi, 0.0))
        ls.append(jnp.where(on, lo, 0.0))
    lhs = jnp.concatenate(
        [jnp.concatenate(hs, axis=1), jnp.concatenate(ls, axis=1)], axis=0
    ).astype(BF16)
    inj = nt(lhs, a_o[...])
    inv = strips[8:16, :]
    z = strips[0:8, :] + (inj[0:8] + inj[8:16]) * inv
    low = iota((8, T), 0) < 4
    send_l[:, :T] = jnp.where(low, z, pltpu.roll(inv, 4, 0))
    send_r[:, :T] = jnp.where(low, pltpu.roll(z, 4, 0), inv)
    g, lane = iota((8, CB), 0), iota((8, CB), 1)
    send_l[:, T:] = nt(jnp.where(lane == g * GROUP, 1.0, 0.0), volt[...], HI)
    send_r[:, T:] = nt(jnp.where(lane == g * GROUP + GROUP - 1, 1.0, 0.0), volt[...], HI)


def rhs_kernel(vf, wt, at_via, zl, invd, a, z, rims, b_s):
    for o in range(NO):
        hi, lo = hi_lo(at_via[o : o + 1, :] * wt[o : o + 1, :])
        on = iota((T, L), 0) == vf[o : o + 1, :] % T
        b_s[:, lanes(o)] = jnp.where(on, hi, 0.0).astype(BF16)
        b_s[:, lanes(NO + o)] = jnp.where(on, lo, 0.0).astype(BF16)
    inj = nt(a[...], b_s[:, : NO * L]) + nt(a[...], b_s[:, NO * L :])
    zz = zl[...] + inj * invd[...]
    z[...] = zz
    rims[0:8, :] = zz[0:8]
    rims[8:16, :] = zz[T - 8 :]


def halo_columns(flags, gl, gr):
    left = jnp.where(flags[1] > 0, 1.0, 0.0)
    right = jnp.where(flags[1] < NO - 1, 1.0, 0.0)
    j, lane = iota((8, L), 0), iota((8, L), 1)
    zc = tn(gr, jnp.where((j < 4) & (lane == j), right, 0.0), HI) + tn(
        gl, jnp.where((j < 4) & (lane == 124 + j), left, 0.0), HI
    )
    ic = tn(gr, jnp.where((j >= 4) & (lane == j - 4), right, 0.0), HI) + tn(
        gl, jnp.where((j >= 4) & (lane == 120 + j), left, 0.0), HI
    )
    return zc, ic


def edge_kernel(flags, zr, ir, got_l, got_r, volt, send_u, send_d):
    zt, it = halo_columns(flags, got_l[:, :L], got_r[:, :L])
    zb, ib = halo_columns(flags, got_l[:, T - L : T], got_r[:, T - L : T])
    low = iota((8, W), 0) < 4
    zt = jnp.concatenate([zr[0:8, :], zt[0:8]], axis=1)
    it = jnp.concatenate([ir[0:8, :], it[0:8]], axis=1)
    zb = jnp.concatenate([zr[8:16, :], zb[L - 8 :]], axis=1)
    ib = jnp.concatenate([ir[8:16, :], ib[L - 8 :]], axis=1)
    send_u[:, :W] = jnp.where(low, zt, pltpu.roll(it, 4, 0))
    send_d[:, :W] = jnp.where(low, pltpu.roll(zb, 4, 0), ib)
    send_u[:, W:] = volt[0:8, :]
    send_d[:, W:] = volt[CB - 8 :, :]


def beside(block):
    n = block.shape[0]
    rows = pltpu.roll(block, 1, 0) + pltpu.roll(block, n - 1, 0)
    return rows + (pltpu.roll(block, 1, 1) + pltpu.roll(block, W - 1, 1))


def beside_mid(block):
    n = block.shape[0]
    mid = block[8 : n - 8]
    rows = pltpu.roll(block, 1, 0)[8 : n - 8] + pltpu.roll(block, n - 1, 0)[8 : n - 8]
    return mid, rows + (pltpu.roll(mid, 1, 1) + pltpu.roll(mid, W - 1, 1))


def fold(p):
    return (p[:, 0:128] + p[:, 128:256]) + (p[:, 256:384] + p[:, 384:512])


def gram_step(acc, zz, w, n1, n2, n3, inv):
    d = 1.0 / inv
    bw, bn1, bn2 = w - n1, n1 - n2, n2 - n3
    e = (zz - Q0 * w - Q1 * n1 - Q2 * n2, w, n1, n2)
    be = (w - Q0 * bw - Q1 * bn1 - Q2 * bn2, bw, bn1, bn2)
    new = []
    k = 0
    for p in range(4):
        de = d * e[p]
        for q in range(p, 4):
            new.append(acc[k] + fold(de * be[q]))
            k += 1
        new.append(acc[k] + fold(de * zz))
        k += 1
    return tuple(new)


def zeros14():
    return tuple(jnp.zeros((8, L), F32) for _ in range(14))


def basis_kernel(flags, z, invd, got_l, got_r, hist, acc_o, ie, ze, we, n1e, n2e, sem):
    zc, ic = halo_columns(flags, got_l[:, :T], got_r[:, :T])
    zero = jnp.zeros((OFF, W), F32)
    for e, own, col in ((ze, z, zc), (ie, invd, ic)):
        e[0:OFF, :] = zero
        e[OFF : OFF + T, :T] = own[...]
        e[OFF : OFF + T, T:] = col
        e[OFF + T :, :] = zero
    for e in (we, n1e, n2e):
        e[0:OFF, :] = zero
        e[OFF + T :, :] = zero
    rows = 32

    def save(k, e):
        copy = pltpu.make_async_copy(e.at[pl.ds(OFF, T), pl.ds(0, T)], hist.at[k], sem.at[k])
        copy.start()
        return copy

    def apply_to(src, dst, minus):
        def step(i, carry):
            start = pl.multiple_of(OFF + i * rows, 8)
            mid, near = beside_mid(src[pl.ds(start - 8, rows + 16), :])
            near = near * ie[pl.ds(start, rows), :]
            dst[pl.ds(start, rows), :] = mid - near if minus else near
            return carry

        lax.fori_loop(0, T // rows, step, 0)

    copies = [save(0, ze)]
    apply_to(ze, we, True)
    copies.append(save(1, we))
    apply_to(we, n1e, False)
    copies.append(save(2, n1e))
    apply_to(n1e, n2e, False)
    copies.append(save(3, n2e))

    def gram(i, acc):
        start = pl.multiple_of(OFF + i * 8, 8)
        mid, near = beside_mid(n2e[pl.ds(start - 8, 24), :])
        inv = ie[pl.ds(start, 8), :T]
        rows8 = pl.ds(start, 8)
        return gram_step(
            acc, ze[rows8, :T], we[rows8, :T], n1e[rows8, :T], mid[:, :T], near[:, :T] * inv, inv
        )

    acc = lax.fori_loop(1, T // 8 - 1, gram, zeros14())
    for k in range(14):
        acc_o[8 * k : 8 * k + 8, :] = acc[k]
    for copy in copies:
        copy.wait()


def rim_kernel(flags, z, invd, got_l, got_r, got_u, got_d, acc_i, rims, part):
    up = jnp.where(flags[0] > 0, 1.0, 0.0)
    down = jnp.where(flags[0] < 7, 1.0, 0.0)
    low = iota((8, W), 0) < 4
    acc = tuple(acc_i[8 * k : 8 * k + 8, :] for k in range(14))
    top, bot = got_u[:, :W], got_d[:, :W]
    for end in (0, 1):
        cols = slice(0, L) if end == 0 else slice(T - L, T)
        rows = slice(0, 16) if end == 0 else slice(T - 16, T)
        part_of = slice(0, 16) if end == 0 else slice(L - 16, L)
        zc, ic = halo_columns(flags, got_l[:, cols], got_r[:, cols])
        z16 = jnp.concatenate([z[rows, :], zc[part_of]], axis=1)
        i16 = jnp.concatenate([invd[rows, :], ic[part_of]], axis=1)
        if end == 0:
            zb = jnp.concatenate([jnp.where(low, 0.0, pltpu.roll(top, 4, 0)) * up, z16], axis=0)
            ib = jnp.concatenate([jnp.where(low, 0.0, top) * up, i16], axis=0)
            own = slice(8, 16)
        else:
            zb = jnp.concatenate([z16, jnp.where(low, bot, 0.0) * down], axis=0)
            ib = jnp.concatenate([i16, jnp.where(low, pltpu.roll(bot, 4, 0), 0.0) * down], axis=0)
            own = slice(8, 16)
        w = zb - ib * beside(zb)
        n1 = ib * beside(w)
        n2 = ib * beside(n1)
        n3 = ib * beside(n2)
        zo, wo, n1o, n2o, n3o, io = (x[own, :T] for x in (zb, w, n1, n2, n3, ib))
        acc = gram_step(acc, zo, wo, n1o, n2o, n3o, io)
        for k, x in enumerate((wo, n1o, n2o)):
            rims[16 * k + 8 * end : 16 * k + 8 * end + 8, :] = x
    rows14 = jnp.concatenate(
        [jnp.sum(a, axis=0, keepdims=True) for a in acc] + [jnp.zeros((L - 14, L), F32)], axis=0
    )
    sums = nt(jnp.ones((8, L), F32), rows14, HI)
    part[...] = sums


def gather_kernel(hist, rims, vf, wt, g_o, x_s, hl_s, c_s, a_s, sem):
    copies = [pltpu.make_async_copy(hist.at[k], x_s.at[k], sem.at[k]) for k in range(4)]
    for copy in copies:
        copy.start()
    for o in range(NO):
        f = vf[o : o + 1, :]
        c_s[:, lanes(o)] = onehot(f % T, T)
        a_s[:, lanes(o)] = onehot(f // T, T)
        g_o[8 * o + 4 : 8 * o + 8, :] = jnp.zeros((4, L), F32)
    for k in range(4):
        copies[k].wait()
        if k:
            x_s[k, 0:8, :] = rims[16 * k - 16 : 16 * k - 8, :]
            x_s[k, T - 8 :, :] = rims[16 * k - 8 : 16 * k, :]
        hi, lo = hi_lo(x_s[k])
        hl_s[0:T, :] = hi.astype(BF16)
        hl_s[T:, :] = lo.astype(BF16)
        for i in range(NO // 2):
            two = slice(2 * i * L, 2 * (i + 1) * L)
            sel = c_s[:, two]
            y = jnp.dot(hl_s[0:T, :], sel, preferred_element_type=F32) + jnp.dot(
                hl_s[T:, :], sel, preferred_element_type=F32
            )
            y = jnp.sum(y * a_s[:, two].astype(F32), axis=0, keepdims=True)
            for o in (2 * i, 2 * i + 1):
                g_o[8 * o + k : 8 * o + k + 1, :] = y[:, (o % 2) * L : (o % 2 + 1) * L] * wt[o : o + 1, :]


def pack_kernel(g, rows, out):
    out[...] = g[...]
    total = jnp.sum(rows[...], axis=0, keepdims=True)
    for o in range(NO):
        out[8 * o + 4 : 8 * o + 5, :] = total


def solve(tot):
    lane = iota((1, L), 1)

    def pick(k):
        return jnp.sum(jnp.where(lane == k, tot, 0.0), axis=1, keepdims=True)

    h, b = {}, []
    k = 0
    for p in range(4):
        for q in range(p, 4):
            h[p, q] = pick(k)
            k += 1
        b.append(pick(k))
        k += 1
    floor = [3e-7 * h[p, p] for p in range(4)]
    inv = []
    for p in range(4):
        inv.append(jnp.where(h[p, p] > floor[p], 1.0 / h[p, p], 0.0))
        for q in range(p + 1, 4):
            f = h[p, q] * inv[p]
            for r in range(q, 4):
                h[q, r] = h[q, r] - f * h[p, r]
            b[q] = b[q] - f * b[p]
    c = [None] * 4
    for p in (3, 2, 1, 0):
        s = b[p]
        for q in range(p + 1, 4):
            s = s - h[p, q] * c[q]
        c[p] = s * inv[p]
    return c[0], c[1] - Q0 * c[0], c[2] - Q1 * c[0], c[3] - Q2 * c[0]


def combine_kernel(coef, hist, rims, x_o):
    c = [coef[k : k + 1, 0:1] for k in range(4)]
    inner = slice(8, T - 8)
    x_o[inner, :] = (c[0] * hist[0, inner, :] + c[1] * hist[1, inner, :]) + (
        c[2] * hist[2, inner, :] + c[3] * hist[3, inner, :]
    )
    for end, rows in ((0, slice(0, 8)), (1, slice(T - 8, T))):
        x = c[0] * hist[0, rows, :]
        for k in range(3):
            x += c[k + 1] * rims[16 * k + 8 * end : 16 * k + 8 * end + 8, :]
        x_o[rows, :] = x


def coarse_neighbours(flags, u, above, below, from_l, from_r):
    up = jnp.where(flags[0] > 0, 1.0, 0.0)
    down = jnp.where(flags[0] < 7, 1.0, 0.0)
    r, lane = iota((CB, CB), 0), iota((CB, CB), 1)
    g, gl = iota((8, CB), 0), iota((8, CB), 1)
    turned_l = jnp.where(g == 0, 0.0, pltpu.roll(from_l, 1, 0))
    turned_r = jnp.where(g == 7, 0.0, pltpu.roll(from_r, 7, 0))
    from_l = jnp.where(flags[1] == 0, turned_l, from_l)
    from_r = jnp.where(flags[1] == NO - 1, turned_r, from_r)
    seam_l = tn(from_l, jnp.where(gl == g * GROUP, 1.0, 0.0), HI)
    seam_r = tn(from_r, jnp.where(gl == g * GROUP + GROUP - 1, 1.0, 0.0), HI)
    near = jnp.where(r == 0, above * up, pltpu.roll(u, 1, 0))
    near += jnp.where(r == CB - 1, below * down, pltpu.roll(u, CB - 1, 0))
    near += jnp.where(lane % GROUP == 0, seam_l, pltpu.roll(u, 1, 1))
    near += jnp.where(lane % GROUP == GROUP - 1, seam_r, pltpu.roll(u, CB - 1, 1))
    return near


def base_kernel(
    flags, held, volt, cleak, got_l, got_r, got_u, got_d, cdiag, scale, base, r_o, c_o
):
    for o in range(NO):
        h = held[o : o + 1, :]
        r_o[:, lanes(o)] = onehot(h >> 7, CB)
        c_o[:, lanes(o)] = onehot(h & (CB - 1), CB)
    count = nt(r_o[...], c_o[...])
    diag = 4.0 * coarse_conductance + cleak[...] + via_conductance * count
    u = volt[...]
    near = coarse_neighbours(flags, u, got_u[7:8, W:], got_d[0:1, W:], got_l[:, T:], got_r[:, T:])
    cdiag[...] = diag
    scale[...] = relaxation / diag
    base[...] = u - relaxation * (diag * u - coarse_conductance * near) / diag


def sweep1_kernel(arrived, scale, base, r, c, coef, u_o, src_o, sl, sr, su, sd, v_s):
    tot = arrived[4:5, :]
    for o in range(1, NO):
        tot += arrived[8 * o + 4 : 8 * o + 5, :]
    d = solve(tot)
    sub = iota((8, L), 0)
    cf = jnp.zeros((8, L), F32)
    for k in range(4):
        cf = jnp.where(sub == k, d[k], cf)
    coef[...] = cf
    for o in range(NO):
        v = jnp.sum(arrived[8 * o : 8 * o + 8, :] * cf, axis=0, keepdims=True)
        hi, lo = hi_lo(v)
        on = c[:, lanes(o)]
        v_s[:, lanes(o)] = on * hi.astype(BF16)
        v_s[:, lanes(NO + o)] = on * lo.astype(BF16)
    src = nt(r[...], v_s[:, : NO * L]) + nt(r[...], v_s[:, NO * L :])
    u = base[...] + scale[...] * src
    u_o[...] = u
    src_o[...] = src
    g, gl = iota((8, CB), 0), iota((8, CB), 1)
    sl[...] = nt(jnp.where(gl == g * GROUP, 1.0, 0.0), u, HI)
    sr[...] = nt(jnp.where(gl == g * GROUP + GROUP - 1, 1.0, 0.0), u, HI)
    su[...] = u[0:8, :]
    sd[...] = u[CB - 8 :, :]


def sweep2_kernel(flags, u, src, cdiag, scale, got_l, got_r, got_u, got_d, u_o):
    near = coarse_neighbours(flags, u[...], got_u[7:8, :], got_d[0:1, :], got_l[...], got_r[...])
    u_o[...] = u[...] + scale[...] * (src[...] - (cdiag[...] * u[...] - coarse_conductance * near))


VM = pl.BlockSpec(memory_space=pltpu.VMEM)
SM = pl.BlockSpec(memory_space=pltpu.SMEM)
ANY = pl.BlockSpec(memory_space=pltpu.HBM)
vmem = pltpu.MemorySpace.VMEM
hbm = jax.ShapeDtypeStruct


def keep(*args):
    return [pltpu.with_memory_space_constraint(x, pltpu.VMEM) for x in args]


def leave(*args):
    return [pltpu.with_memory_space_constraint(x, pltpu.HBM) for x in args]


def call(body, outs, args, scratch=(), flags=None, flops=0, any_in=0, any_out=0):
    specs = ([] if flags is None else [SM]) + [ANY] * any_in + [VM] * (len(args) - any_in)
    return pl.pallas_call(
        body,
        out_shape=outs,
        in_specs=specs,
        out_specs=[ANY] * any_out + [VM] * (len(outs) - any_out),
        scratch_shapes=list(scratch),
        cost_estimate=pl.CostEstimate(flops=flops, bytes_accessed=0, transcendentals=0),
        compiler_params=pltpu.CompilerParams(vmem_limit_bytes=20 * 2**20),
    )(*([] if flags is None else [flags]), *args)


def ring(axis):
    n = lax.axis_size(axis)
    up = [(i, (i + 1) % n) for i in range(n)]
    return up, [(b, a) for a, b in up]


def swap(axis, to_low, to_high):
    up, down = ring(axis)
    return lax.ppermute(to_high, axis, up), lax.ppermute(to_low, axis, down)


def spread(x, axis=COL):
    return lax.all_to_all(x, axis, split_axis=0, concat_axis=0, tiled=True)


def per_device(load_amp, load_mask, leak, coarse_leak, coarse_init, via_fine, via_coarse, via_count):
    flags = jnp.where(
        jnp.arange(2, dtype=jnp.int32) == 0, lax.axis_index(ROW), lax.axis_index(COL)
    ).astype(jnp.int32)
    live = jnp.arange(L, dtype=jnp.int32)[None, :] < via_count.reshape(NO, 1)
    wt = jnp.where(live, via_conductance, 0.0).astype(F32)
    fine = via_fine.reshape(NO, L)
    coarse = via_coarse.reshape(NO, L)
    request = jnp.where(live, ((coarse >> 11) << 7) | (coarse & (CB - 1)), -1)
    held = spread(request)

    tile, block, slots = vmem((T, T), F32), vmem((CB, CB), F32), vmem((NO, L), F32)
    hot, chot = vmem((T, NO * L), BF16), vmem((CB, NO * L), BF16)
    hots = vmem((T, 2 * NO * L), BF16)
    rim16, side, seam = vmem((16, T), F32), vmem((8, W), F32), vmem((8, CB), F32)
    ext, packed = vmem((EXT, W), F32), ((L, L), F32)
    dmas = pltpu.SemaphoreType.DMA((4,))
    big = 20_000_000_000

    zl, invd, strips, irims = call(
        diag_kernel, [tile, tile, rim16, rim16],
        keep(fine, wt) + leave(load_amp, load_mask, leak), [hot, hot], flops=big,
    )
    looked = call(lookup_kernel, [slots], keep(held, coarse_init))[0]
    at_via = spread(looked)
    a, send_l, send_r = call(
        strips_kernel, [hot, side, side], keep(fine, wt, at_via, strips, coarse_init)
    )
    got_l, got_r = swap(COL, send_l, send_r)
    z, zrims = call(
        rhs_kernel, [tile, rim16], keep(fine, wt, at_via, zl, invd, a), [hots], flops=big
    )
    rim = vmem((8, W + CB), F32)
    send_u, send_d = call(
        edge_kernel, [rim, rim], keep(zrims, irims, got_l, got_r, coarse_init), flags=flags
    )
    got_u, got_d = swap(ROW, send_u, send_d)
    hist, acc = call(
        basis_kernel, [pltpu.MemorySpace.HBM((4, T, T), F32), vmem((112, L), F32)], keep(z, invd, got_l, got_r),
        [ext] * 5 + [dmas], flags=flags, flops=big, any_out=1,
    )
    rims, part = call(
        rim_kernel, [vmem((48, T), F32), vmem((8, L), F32)],
        keep(z, invd, got_l, got_r, got_u, got_d, acc), flags=flags,
    )
    rows = spread(part, ROW)
    g = call(
        gather_kernel, [vmem(*packed)], leave(hist) + keep(rims, fine, wt),
        [vmem((4, T, T), F32), vmem((2 * T, T), BF16), hot, hot, dmas], flops=big, any_in=1,
    )[0]
    arrived = spread(call(pack_kernel, [vmem(*packed)], keep(g, rows))[0])
    cdiag, scale, base, r_hot, c_hot = call(
        base_kernel, [block, block, block, chot, chot],
        keep(held, coarse_init, coarse_leak, got_l, got_r, got_u, got_d), flags=flags, flops=big,
    )
    coef, u, src, sl, sr, su, sd = call(
        sweep1_kernel, [seam, block, block, seam, seam, seam, seam],
        keep(arrived, scale, base, r_hot, c_hot), [vmem((CB, 2 * NO * L), BF16)],
    )
    hl, hr = swap(COL, sl, sr)
    hu, hd = swap(ROW, su, sd)
    fine_drop = call(
        combine_kernel, [hbm((T, T), F32)], keep(coef) + leave(hist) + keep(rims), flops=big // 4
    )[0]
    coarse_drop = call(
        sweep2_kernel, [hbm((CB, CB), F32)], keep(u, src, cdiag, scale, hl, hr, hu, hd), flags=flags
    )[0]
    return fine_drop, coarse_drop


def solution(mesh):
    spec = P(ROW, COL)

    return jax.shard_map(
        per_device, mesh=mesh, in_specs=(spec,) * 8, out_specs=(spec, spec), check_vma=False
    )
```

```python
import jax
import jax.numpy as jnp
from jax import lax
from jax.experimental import pallas as pl
from jax.experimental.pallas import tpu as pltpu
from jax.sharding import PartitionSpec as P


F32 = jnp.float32
BF16 = jnp.bfloat16
HI = lax.Precision.HIGHEST
ROW, COL = "row", "col"

GROUP = 16
via_conductance = 2.0
coarse_conductance = 4.0
relaxation = 0.8

T = 512
CB = 128
NO = 16
L = 128
OFF = 16
EXT = OFF + T + 16
W = T + L

Q = (1.08976773, 1.76773384, 1.28562461)
RHO = (1.0 - Q[0], Q[0] - Q[1], Q[1] - Q[2], Q[2])
LT = T // L
SLAB = 4 * LT + 1
SUMS = 8
STEPS = 4


def iota(shape, dim):
    return lax.broadcasted_iota(jnp.int32, shape, dim)


def nt(a, b, precision=None):
    return lax.dot_general(
        a, b, (((1,), (1,)), ((), ())), precision=precision, preferred_element_type=F32
    )


def tn(a, b, precision=None):
    return lax.dot_general(
        a, b, (((0,), (0,)), ((), ())), precision=precision, preferred_element_type=F32
    )


def onehot(idx, n):
    return jnp.where(iota((n, idx.shape[1]), 0) == idx, 1.0, 0.0).astype(BF16)


def hi_lo(x):
    hi = x.astype(BF16).astype(F32)
    return hi, x - hi


def lanes(o):
    return slice(o * L, (o + 1) * L)


def diag_kernel(vf, wt, amp, mask, leak, zl, invd, strips, rims, a_s, b_s):
    for o in range(NO):
        f = vf[o : o + 1, :]
        a_s[:, lanes(o)] = onehot(f // T, T)
        b_s[:, lanes(o)] = jnp.where(iota((T, L), 0) == f % T, wt[o : o + 1, :], 0.0).astype(BF16)
    inv = 1.0 / (4.0 + leak[...] + nt(a_s[...], b_s[...]))
    z = amp[...] * mask[...].astype(F32) * inv
    zl[...] = z
    invd[...] = inv
    j, lane = iota((8, L), 0), iota((8, L), 1)
    first = jnp.where((j < 4) & (lane == j), 1.0, 0.0)
    last = jnp.where((j >= 4) & (lane == 120 + j), 1.0, 0.0)
    strips[0:8, :] = nt(first, z[:, :L], HI) + nt(last, z[:, T - L :], HI)
    strips[8:16, :] = nt(first, inv[:, :L], HI) + nt(last, inv[:, T - L :], HI)
    rims[0:8, :] = inv[0:8]
    rims[8:16, :] = inv[T - 8 :]


def lookup_kernel(held, volt, looked):
    v1, rest = hi_lo(volt[...].T)
    v2, v3 = hi_lo(rest)
    v = jnp.concatenate([v3, v2, v1], axis=0).astype(BF16)
    for i in range(NO // 2):
        h = jnp.concatenate([held[2 * i : 2 * i + 1, :], held[2 * i + 1 : 2 * i + 2, :]], axis=1)
        y = jnp.dot(v, onehot(h >> 7, CB), preferred_element_type=F32)
        y = y[:CB] + y[CB : 2 * CB] + y[2 * CB :]
        y = jnp.where(iota((CB, 2 * L), 0) == (h & (CB - 1)), y, 0.0)
        y = jnp.sum(y, axis=0, keepdims=True)
        looked[2 * i : 2 * i + 1, :] = y[:, :L]
        looked[2 * i + 1 : 2 * i + 2, :] = y[:, L:]


def strips_kernel(vf, wt, at_via, strips, volt, a_o, send_l, send_r):
    j = iota((8, L), 0)
    colid = jnp.where(j < 4, j, T - 8 + j)
    hs, ls = [], []
    for o in range(NO):
        f = vf[o : o + 1, :]
        a_o[:, lanes(o)] = onehot(f // T, T)
        hi, lo = hi_lo(at_via[o : o + 1, :] * wt[o : o + 1, :])
        on = colid == f % T
        hs.append(jnp.where(on, hi, 0.0))
        ls.append(jnp.where(on, lo, 0.0))
    lhs = jnp.concatenate(
        [jnp.concatenate(hs, axis=1), jnp.concatenate(ls, axis=1)], axis=0
    ).astype(BF16)
    inj = nt(lhs, a_o[...])
    inv = strips[8:16, :]
    z = strips[0:8, :] + (inj[0:8] + inj[8:16]) * inv
    low = iota((8, T), 0) < 4
    send_l[:, :T] = jnp.where(low, z, pltpu.roll(inv, 4, 0))
    send_r[:, :T] = jnp.where(low, pltpu.roll(z, 4, 0), inv)
    g, lane = iota((8, CB), 0), iota((8, CB), 1)
    send_l[:, T:] = nt(jnp.where(lane == g * GROUP, 1.0, 0.0), volt[...], HI)
    send_r[:, T:] = nt(jnp.where(lane == g * GROUP + GROUP - 1, 1.0, 0.0), volt[...], HI)


def rhs_kernel(vf, wt, at_via, zl, invd, a, z, rims, b_s):
    for o in range(NO):
        hi, lo = hi_lo(at_via[o : o + 1, :] * wt[o : o + 1, :])
        on = iota((T, L), 0) == vf[o : o + 1, :] % T
        b_s[:, lanes(o)] = jnp.where(on, hi, 0.0).astype(BF16)
        b_s[:, lanes(NO + o)] = jnp.where(on, lo, 0.0).astype(BF16)
    inj = nt(a[...], b_s[:, : NO * L]) + nt(a[...], b_s[:, NO * L :])
    zz = zl[...] + inj * invd[...]
    z[...] = zz
    rims[0:8, :] = zz[0:8]
    rims[8:16, :] = zz[T - 8 :]


def halo_columns(flags, gl, gr):
    left = jnp.where(flags[1] > 0, 1.0, 0.0)
    right = jnp.where(flags[1] < NO - 1, 1.0, 0.0)
    j, lane = iota((8, L), 0), iota((8, L), 1)
    zc = tn(gr, jnp.where((j < 4) & (lane == j), right, 0.0), HI) + tn(
        gl, jnp.where((j < 4) & (lane == 124 + j), left, 0.0), HI
    )
    ic = tn(gr, jnp.where((j >= 4) & (lane == j - 4), right, 0.0), HI) + tn(
        gl, jnp.where((j >= 4) & (lane == 120 + j), left, 0.0), HI
    )
    return zc, ic


def edge_kernel(flags, zr, ir, got_l, got_r, volt, send_u, send_d):
    zt, it = halo_columns(flags, got_l[:, :L], got_r[:, :L])
    zb, ib = halo_columns(flags, got_l[:, T - L : T], got_r[:, T - L : T])
    low = iota((8, W), 0) < 4
    zt = jnp.concatenate([zr[0:8, :], zt[0:8]], axis=1)
    it = jnp.concatenate([ir[0:8, :], it[0:8]], axis=1)
    zb = jnp.concatenate([zr[8:16, :], zb[L - 8 :]], axis=1)
    ib = jnp.concatenate([ir[8:16, :], ib[L - 8 :]], axis=1)
    send_u[:, :W] = jnp.where(low, zt, pltpu.roll(it, 4, 0))
    send_d[:, :W] = jnp.where(low, pltpu.roll(zb, 4, 0), ib)
    send_u[:, W:] = volt[0:8, :]
    send_d[:, W:] = volt[CB - 8 :, :]


def beside(block):
    n = block.shape[0]
    rows = pltpu.roll(block, 1, 0) + pltpu.roll(block, n - 1, 0)
    return rows + (pltpu.roll(block, 1, 1) + pltpu.roll(block, W - 1, 1))


def near_tiles(ref, start, rows):
    mid = [ref[t, pl.ds(start, rows), :] for t in range(LT + 1)]
    low = [pltpu.roll(m, 1, 1) for m in mid]
    high = [pltpu.roll(m, L - 1, 1) for m in mid]
    lane = iota((rows, L), 1)
    near = []
    for t in range(LT + 1):
        rows_sum = ref[t, pl.ds(start - 1, rows), :] + ref[t, pl.ds(start + 1, rows), :]
        left = jnp.where(lane == 0, low[t - 1], low[t])
        right = jnp.where(lane == L - 1, high[(t + 1) % (LT + 1)], high[t])
        near.append(rows_sum + (left + right))
    return mid, near


def fold(p):
    return (p[:, 0:128] + p[:, 128:256]) + (p[:, 256:384] + p[:, 384:512])


def moments(z, w, n1, n2, dn3, inv):
    d = 1.0 / inv
    dz, dw, dn1, dn2 = d * z, d * w, d * n1, d * n2
    return dz * z, dz * w, dw * w, dw * n1, dn1 * n1, dn1 * n2, dn2 * n2, n2 * dn3


def basis_kernel(flags, z, invd, got_l, got_r, hist, acc_o, ie, ze, we, n1e, n2e, sem):
    zc, ic = halo_columns(flags, got_l[:, :T], got_r[:, :T])
    zero = jnp.zeros((OFF, L), F32)
    own = pl.ds(OFF, T)
    for e in (ie, ze, we, n1e, n2e):
        for t in range(LT + 1):
            e[t, 0:OFF, :] = zero
            e[t, OFF + T :, :] = zero
    for t in range(LT):
        ze[t, own, :] = z[:, lanes(t)]
        ie[t, own, :] = invd[:, lanes(t)]
    ze[LT, own, :] = zc
    ie[LT, own, :] = ic
    rows = 16

    def save(k, e):
        copy = pltpu.make_async_copy(e.at[pl.ds(0, LT), own, :], hist.at[k], sem.at[k])
        copy.start()
        return copy

    def apply_to(src, dst, minus):
        def step(i, carry):
            start = pl.multiple_of(OFF + i * rows, 8)
            mid, near = near_tiles(src, start, rows)
            for t in range(LT + 1):
                y = near[t] * ie[t, pl.ds(start, rows), :]
                dst[t, pl.ds(start, rows), :] = mid[t] - y if minus else y
            return carry

        lax.fori_loop(0, T // rows, step, 0)

    copies = [save(0, ze)]
    apply_to(ze, we, True)
    copies.append(save(1, we))
    apply_to(we, n1e, False)
    copies.append(save(2, n1e))
    apply_to(n1e, n2e, False)
    copies.append(save(3, n2e))

    def gram(i, acc):
        start = pl.multiple_of(OFF + i * 8, 8)
        n2, dn3 = near_tiles(n2e, start, 8)
        acc = list(acc)
        for t in range(LT):
            z8, w8, n18, i8 = (e[t, pl.ds(start, 8), :] for e in (ze, we, n1e, ie))
            for k, p in enumerate(moments(z8, w8, n18, n2[t], dn3[t], i8)):
                acc[k] = acc[k] + p
        return tuple(acc)

    acc = lax.fori_loop(
        1, T // 8 - 1, gram, tuple(jnp.zeros((8, L), F32) for _ in range(SUMS))
    )
    for k in range(SUMS):
        acc_o[8 * k : 8 * k + 8, :] = acc[k]
    for copy in copies:
        copy.wait()


def rim_kernel(flags, z, invd, got_l, got_r, got_u, got_d, acc_i, rims, part):
    up = jnp.where(flags[0] > 0, 1.0, 0.0)
    down = jnp.where(flags[0] < 7, 1.0, 0.0)
    low = iota((8, W), 0) < 4
    acc = [acc_i[8 * k : 8 * k + 8, :] for k in range(SUMS)]
    top, bot = got_u[:, :W], got_d[:, :W]
    for end in (0, 1):
        cols = slice(0, L) if end == 0 else slice(T - L, T)
        rows = slice(0, 16) if end == 0 else slice(T - 16, T)
        part_of = slice(0, 16) if end == 0 else slice(L - 16, L)
        zc, ic = halo_columns(flags, got_l[:, cols], got_r[:, cols])
        z16 = jnp.concatenate([z[rows, :], zc[part_of]], axis=1)
        i16 = jnp.concatenate([invd[rows, :], ic[part_of]], axis=1)
        if end == 0:
            zb = jnp.concatenate([jnp.where(low, 0.0, pltpu.roll(top, 4, 0)) * up, z16], axis=0)
            ib = jnp.concatenate([jnp.where(low, 0.0, top) * up, i16], axis=0)
            own = slice(8, 16)
        else:
            zb = jnp.concatenate([z16, jnp.where(low, bot, 0.0) * down], axis=0)
            ib = jnp.concatenate([i16, jnp.where(low, pltpu.roll(bot, 4, 0), 0.0) * down], axis=0)
            own = slice(8, 16)
        w = zb - ib * beside(zb)
        n1 = ib * beside(w)
        n2 = ib * beside(n1)
        near = beside(n2)
        zo, wo, n1o, n2o, dn3, io = (x[own, :T] for x in (zb, w, n1, n2, near, ib))
        for k, p in enumerate(moments(zo, wo, n1o, n2o, dn3, io)):
            acc[k] = acc[k] + fold(p)
        for k, x in enumerate((wo, n1o, n2o)):
            rims[16 * k + 8 * end : 16 * k + 8 * end + 8, :] = x
    rows8 = jnp.concatenate(
        [jnp.sum(a, axis=0, keepdims=True) for a in acc] + [jnp.zeros((L - SUMS, L), F32)], axis=0
    )
    sums = nt(jnp.ones((8, L), F32), rows8, HI)
    part[...] = sums


def gather_kernel(slots, hist, rims, vf, wt, g_o, x_s, slab, sem):
    copies = [pltpu.make_async_copy(hist.at[k], x_s.at[k], sem.at[k]) for k in range(4)]
    for copy in copies:
        copy.start()
    for k in range(4):
        copies[k].wait()
        if k:
            for t in range(LT):
                x_s[k, t, 0:8, :] = rims[16 * k - 16 : 16 * k - 8, lanes(t)]
                x_s[k, t, T - 8 :, :] = rims[16 * k - 8 : 16 * k, lanes(t)]

        def lay(i, carry):
            for b in range(4):
                for t in range(LT):
                    start = pl.multiple_of(i * 32 + 8 * b, 8)
                    to = (i * 32 + 8 * b) * SLAB + 4 * k + t
                    slab[pl.ds(to, 8, stride=SLAB), :] = x_s[k, t, pl.ds(start, 8), :]
            return carry

        lax.fori_loop(0, T // 32, lay, 0)
    lane, sub = iota((16, L), 1), iota((16, L), 0)

    def owner(o, carry):
        acc = jnp.zeros((16, L), F32)
        for j in range(L):
            node = slots[o, j]
            x = slab[pl.ds((node >> 9) * SLAB, 16), :]
            x = pltpu.roll(x, (j - node) & (L - 1), 1)
            acc = jnp.where(lane == j, x, acc)
        f = vf[pl.ds(o, 1), :]
        acc = jnp.where((sub & 3) == ((f >> 7) & 3), acc * wt[pl.ds(o, 1), :], 0.0)
        rows = [jnp.sum(acc[4 * k : 4 * k + 4, :], axis=0, keepdims=True) for k in range(4)]
        g_o[pl.ds(pl.multiple_of(8 * o, 8), 8), :] = jnp.concatenate(
            rows + [jnp.zeros((4, L), F32)], axis=0
        )
        return carry

    lax.fori_loop(0, NO, owner, 0)


def pack_kernel(g, rows, out):
    out[...] = g[...]
    total = jnp.sum(rows[...], axis=0, keepdims=True)
    for o in range(NO):
        out[8 * o + 4 : 8 * o + 5, :] = total


def solve(tot):
    lane = iota((1, L), 1)

    def pick(k):
        return jnp.sum(jnp.where(lane == k, tot, 0.0), axis=1, keepdims=True)

    g0, q0 = pick(0), pick(1)
    m = [pick(2 + k) for k in range(6)]
    r = [q0, q0 - m[0], q0 - m[0] - m[1]]
    h = {(0, 0): q0, **{(0, j): RHO[0] * m[j - 1] for j in (1, 2, 3)}}
    b = [g0] + r
    for k in range(3):
        h[0, 0] = h[0, 0] - Q[k] * m[k]
        b[0] = b[0] - Q[k] * r[k]
    for k in range(6):
        f = sum(Q[j] * RHO[k - j] for j in range(3) if 0 <= k - j < 4)
        h[0, 0] = h[0, 0] - f * m[k]
    for j in (1, 2, 3):
        for k in (1, 2, 3):
            h[0, j] = h[0, j] + RHO[k] * m[j - 1 + k]
            if j <= k:
                h[j, k] = m[j + k - 2] - m[j + k - 1]
    floor = [3e-7 * h[p, p] for p in range(4)]
    inv = []
    for p in range(4):
        inv.append(jnp.where(h[p, p] > floor[p], 1.0 / h[p, p], 0.0))
        for q in range(p + 1, 4):
            f = h[p, q] * inv[p]
            for r in range(q, 4):
                h[q, r] = h[q, r] - f * h[p, r]
            b[q] = b[q] - f * b[p]
    c = [None] * 4
    for p in (3, 2, 1, 0):
        s = b[p]
        for q in range(p + 1, 4):
            s = s - h[p, q] * c[q]
        c[p] = s * inv[p]
    return [c[0]] + [c[k + 1] - Q[k] * c[0] for k in range(3)]


def combine_kernel(coef, hist, rims, x_o):
    c = [coef[k : k + 1, 0:1] for k in range(4)]
    i = pl.program_id(0)
    for t in range(LT):
        x_o[:, lanes(t)] = (c[0] * hist[0, t] + c[1] * hist[1, t]) + (
            c[2] * hist[2, t] + c[3] * hist[3, t]
        )
    for end, step, rows in ((0, 0, slice(0, 8)), (1, STEPS - 1, slice(T // STEPS - 8, T // STEPS))):

        @pl.when(i == step)
        def _(end=end, rows=rows):
            for t in range(LT):
                x = c[0] * hist[0, t, rows, :]
                for k in range(3):
                    x += c[k + 1] * rims[16 * k + 8 * end : 16 * k + 8 * end + 8, lanes(t)]
                x_o[rows, lanes(t)] = x


def coarse_neighbours(flags, u, above, below, from_l, from_r):
    up = jnp.where(flags[0] > 0, 1.0, 0.0)
    down = jnp.where(flags[0] < 7, 1.0, 0.0)
    r, lane = iota((CB, CB), 0), iota((CB, CB), 1)
    g, gl = iota((8, CB), 0), iota((8, CB), 1)
    turned_l = jnp.where(g == 0, 0.0, pltpu.roll(from_l, 1, 0))
    turned_r = jnp.where(g == 7, 0.0, pltpu.roll(from_r, 7, 0))
    from_l = jnp.where(flags[1] == 0, turned_l, from_l)
    from_r = jnp.where(flags[1] == NO - 1, turned_r, from_r)
    seam_l = tn(from_l, jnp.where(gl == g * GROUP, 1.0, 0.0), HI)
    seam_r = tn(from_r, jnp.where(gl == g * GROUP + GROUP - 1, 1.0, 0.0), HI)
    near = jnp.where(r == 0, above * up, pltpu.roll(u, 1, 0))
    near += jnp.where(r == CB - 1, below * down, pltpu.roll(u, CB - 1, 0))
    near += jnp.where(lane % GROUP == 0, seam_l, pltpu.roll(u, 1, 1))
    near += jnp.where(lane % GROUP == GROUP - 1, seam_r, pltpu.roll(u, CB - 1, 1))
    return near


def base_kernel(
    flags, held, volt, cleak, got_l, got_r, got_u, got_d, cdiag, scale, base, r_o, c_o
):
    for o in range(NO):
        h = held[o : o + 1, :]
        r_o[:, lanes(o)] = onehot(h >> 7, CB)
        c_o[:, lanes(o)] = onehot(h & (CB - 1), CB)
    count = nt(r_o[...], c_o[...])
    diag = 4.0 * coarse_conductance + cleak[...] + via_conductance * count
    u = volt[...]
    near = coarse_neighbours(flags, u, got_u[7:8, W:], got_d[0:1, W:], got_l[:, T:], got_r[:, T:])
    cdiag[...] = diag
    scale[...] = relaxation / diag
    base[...] = u - relaxation * (diag * u - coarse_conductance * near) / diag


def sweep1_kernel(arrived, scale, base, r, c, coef, u_o, src_o, sl, sr, su, sd, v_s):
    tot = arrived[4:5, :]
    for o in range(1, NO):
        tot += arrived[8 * o + 4 : 8 * o + 5, :]
    d = solve(tot)
    sub = iota((8, L), 0)
    cf = jnp.zeros((8, L), F32)
    for k in range(4):
        cf = jnp.where(sub == k, d[k], cf)
    coef[...] = cf
    for o in range(NO):
        v = jnp.sum(arrived[8 * o : 8 * o + 8, :] * cf, axis=0, keepdims=True)
        hi, lo = hi_lo(v)
        on = c[:, lanes(o)]
        v_s[:, lanes(o)] = on * hi.astype(BF16)
        v_s[:, lanes(NO + o)] = on * lo.astype(BF16)
    src = nt(r[...], v_s[:, : NO * L]) + nt(r[...], v_s[:, NO * L :])
    u = base[...] + scale[...] * src
    u_o[...] = u
    src_o[...] = src
    g, gl = iota((8, CB), 0), iota((8, CB), 1)
    sl[...] = nt(jnp.where(gl == g * GROUP, 1.0, 0.0), u, HI)
    sr[...] = nt(jnp.where(gl == g * GROUP + GROUP - 1, 1.0, 0.0), u, HI)
    su[...] = u[0:8, :]
    sd[...] = u[CB - 8 :, :]


def sweep2_kernel(flags, u, src, cdiag, scale, got_l, got_r, got_u, got_d, u_o):
    near = coarse_neighbours(flags, u[...], got_u[7:8, :], got_d[0:1, :], got_l[...], got_r[...])
    u_o[...] = u[...] + scale[...] * (src[...] - (cdiag[...] * u[...] - coarse_conductance * near))


VM = pl.BlockSpec(memory_space=pltpu.VMEM)
SM = pl.BlockSpec(memory_space=pltpu.SMEM)
ANY = pl.BlockSpec(memory_space=pltpu.HBM)
vmem = pltpu.MemorySpace.VMEM
hbm = jax.ShapeDtypeStruct


def keep(*args):
    return [pltpu.with_memory_space_constraint(x, pltpu.VMEM) for x in args]


def leave(*args):
    return [pltpu.with_memory_space_constraint(x, pltpu.HBM) for x in args]


def call(body, outs, args, scratch=(), flags=None, flops=0, any_in=0, any_out=0):
    specs = ([] if flags is None else [SM]) + [ANY] * any_in + [VM] * (len(args) - any_in)
    return pl.pallas_call(
        body,
        out_shape=outs,
        in_specs=specs,
        out_specs=[ANY] * any_out + [VM] * (len(outs) - any_out),
        scratch_shapes=list(scratch),
        cost_estimate=pl.CostEstimate(flops=flops, bytes_accessed=0, transcendentals=0),
        compiler_params=pltpu.CompilerParams(vmem_limit_bytes=20 * 2**20),
    )(*([] if flags is None else [flags]), *args)


def ring(axis):
    n = lax.axis_size(axis)
    up = [(i, (i + 1) % n) for i in range(n)]
    return up, [(b, a) for a, b in up]


def swap(axis, to_low, to_high):
    up, down = ring(axis)
    return lax.ppermute(to_high, axis, up), lax.ppermute(to_low, axis, down)


def spread(x, axis=COL):
    return lax.all_to_all(x, axis, split_axis=0, concat_axis=0, tiled=True)


def per_device(load_amp, load_mask, leak, coarse_leak, coarse_init, via_fine, via_coarse, via_count):
    flags = jnp.where(
        jnp.arange(2, dtype=jnp.int32) == 0, lax.axis_index(ROW), lax.axis_index(COL)
    ).astype(jnp.int32)
    live = jnp.arange(L, dtype=jnp.int32)[None, :] < via_count.reshape(NO, 1)
    wt = jnp.where(live, via_conductance, 0.0).astype(F32)
    fine = via_fine.reshape(NO, L)
    coarse = via_coarse.reshape(NO, L)
    request = jnp.where(live, ((coarse >> 11) << 7) | (coarse & (CB - 1)), -1)
    held = spread(request)

    tile, block, slots = vmem((T, T), F32), vmem((CB, CB), F32), vmem((NO, L), F32)
    hot, chot = vmem((T, NO * L), BF16), vmem((CB, NO * L), BF16)
    hots = vmem((T, 2 * NO * L), BF16)
    rim16, side, seam = vmem((16, T), F32), vmem((8, W), F32), vmem((8, CB), F32)
    ext, packed = vmem((LT + 1, EXT, L), F32), ((L, L), F32)
    dmas = pltpu.SemaphoreType.DMA((4,))
    big = 20_000_000_000

    zl, invd, strips, irims = call(
        diag_kernel, [tile, tile, rim16, rim16],
        keep(fine, wt) + leave(load_amp, load_mask, leak), [hot, hot], flops=big,
    )
    looked = call(lookup_kernel, [slots], keep(held, coarse_init))[0]
    at_via = spread(looked)
    a, send_l, send_r = call(
        strips_kernel, [hot, side, side], keep(fine, wt, at_via, strips, coarse_init)
    )
    got_l, got_r = swap(COL, send_l, send_r)
    z, zrims = call(
        rhs_kernel, [tile, rim16], keep(fine, wt, at_via, zl, invd, a), [hots], flops=big
    )
    rim = vmem((8, W + CB), F32)
    send_u, send_d = call(
        edge_kernel, [rim, rim], keep(zrims, irims, got_l, got_r, coarse_init), flags=flags
    )
    got_u, got_d = swap(ROW, send_u, send_d)
    hist, acc = call(
        basis_kernel, [pltpu.MemorySpace.HBM((4, LT, T, L), F32), vmem((8 * SUMS, L), F32)], keep(z, invd, got_l, got_r),
        [ext] * 5 + [dmas], flags=flags, flops=big, any_out=1,
    )
    rims, part = call(
        rim_kernel, [vmem((48, T), F32), vmem((8, L), F32)],
        keep(z, invd, got_l, got_r, got_u, got_d, acc), flags=flags,
    )
    rows = spread(part, ROW)
    g = call(
        gather_kernel, [vmem(*packed)], leave(hist) + keep(rims, fine, wt),
        [vmem((4, LT, T, L), F32), vmem((T * SLAB, L), F32), dmas], flags=fine, flops=big, any_in=1,
    )[0]
    arrived = spread(call(pack_kernel, [vmem(*packed)], keep(g, rows))[0])
    cdiag, scale, base, r_hot, c_hot = call(
        base_kernel, [block, block, block, chot, chot],
        keep(held, coarse_init, coarse_leak, got_l, got_r, got_u, got_d), flags=flags, flops=big,
    )
    coef, u, src, sl, sr, su, sd = call(
        sweep1_kernel, [seam, block, block, seam, seam, seam, seam],
        keep(arrived, scale, base, r_hot, c_hot), [vmem((CB, 2 * NO * L), BF16)],
    )
    hl, hr = swap(COL, sl, sr)
    hu, hd = swap(ROW, su, sd)
    fine_drop = pl.pallas_call(
        combine_kernel,
        grid=(STEPS,),
        out_shape=hbm((T, T), F32),
        in_specs=[
            pl.BlockSpec((8, L), lambda i: (0, 0)),
            pl.BlockSpec((4, LT, T // STEPS, L), lambda i: (0, 0, i, 0)),
            pl.BlockSpec((48, T), lambda i: (0, 0)),
        ],
        out_specs=pl.BlockSpec((T // STEPS, T), lambda i: (i, 0)),
        cost_estimate=pl.CostEstimate(flops=big // 4, bytes_accessed=0, transcendentals=0),
        compiler_params=pltpu.CompilerParams(vmem_limit_bytes=20 * 2**20),
    )(*keep(coef), *leave(hist), *keep(rims))
    coarse_drop = call(
        sweep2_kernel, [hbm((CB, CB), F32)], keep(u, src, cdiag, scale, hl, hr, hu, hd), flags=flags
    )[0]
    return fine_drop, coarse_drop


def solution(mesh):
    spec = P(ROW, COL)

    return jax.shard_map(
        per_device, mesh=mesh, in_specs=(spec,) * 8, out_specs=(spec, spec), check_vma=False
    )
```

```python
import jax
import jax.numpy as jnp
from jax import lax
from jax.experimental import pallas as pl
from jax.experimental.pallas import tpu as pltpu
from jax.sharding import PartitionSpec as P


F32 = jnp.float32
BF16 = jnp.bfloat16
HI = lax.Precision.HIGHEST
ROW, COL = "row", "col"

GROUP = 16
via_conductance = 2.0
coarse_conductance = 4.0
relaxation = 0.8

T = 512
CB = 128
NO = 16
L = 128
OFF = 16
EXT = OFF + T + 16
W = T + L

Q = (1.09375, 1.765625, 1.28125)
RHO = (1.0 - Q[0], Q[0] - Q[1], Q[1] - Q[2], Q[2])
LT = T // L
SLAB = 4 * LT + 1
SUMS = 8
STEPS = 8


def iota(shape, dim):
    return lax.broadcasted_iota(jnp.int32, shape, dim)


def nt(a, b, precision=None):
    return lax.dot_general(
        a, b, (((1,), (1,)), ((), ())), precision=precision, preferred_element_type=F32
    )


def tn(a, b, precision=None):
    return lax.dot_general(
        a, b, (((0,), (0,)), ((), ())), precision=precision, preferred_element_type=F32
    )


def onehot(idx, n):
    return jnp.where(iota((n, idx.shape[1]), 0) == idx, 1.0, 0.0).astype(BF16)


def hi_lo(x):
    hi = x.astype(BF16).astype(F32)
    return hi, x - hi


def lanes(o):
    return slice(o * L, (o + 1) * L)


def diag_kernel(vf, wt, amp, mask, leak, zl, invd, strips, rims, slots, a_s, b_s):
    slots[0:NO, :] = (vf[...] >> 9) * SLAB
    slots[NO:, :] = (iota((NO, L), 1) - vf[...]) & (L - 1)
    for o in range(NO):
        f = vf[o : o + 1, :]
        a_s[:, lanes(o)] = onehot(f // T, T)
        b_s[:, lanes(o)] = jnp.where(iota((T, L), 0) == f % T, wt[o : o + 1, :], 0.0).astype(BF16)
    inv = 1.0 / (4.0 + leak[...] + nt(a_s[...], b_s[...]))
    z = amp[...] * mask[...].astype(F32) * inv
    zl[...] = z
    invd[...] = inv
    j, lane = iota((8, L), 0), iota((8, L), 1)
    first = jnp.where((j < 4) & (lane == j), 1.0, 0.0)
    last = jnp.where((j >= 4) & (lane == 120 + j), 1.0, 0.0)
    strips[0:8, :] = nt(first, z[:, :L], HI) + nt(last, z[:, T - L :], HI)
    strips[8:16, :] = nt(first, inv[:, :L], HI) + nt(last, inv[:, T - L :], HI)
    rims[0:8, :] = inv[0:8]
    rims[8:16, :] = inv[T - 8 :]


def lookup_kernel(held, volt, looked):
    v1, rest = hi_lo(volt[...].T)
    v2, v3 = hi_lo(rest)
    v = jnp.concatenate([v3, v2, v1], axis=0).astype(BF16)
    for i in range(NO // 2):
        h = jnp.concatenate([held[2 * i : 2 * i + 1, :], held[2 * i + 1 : 2 * i + 2, :]], axis=1)
        y = jnp.dot(v, onehot(h >> 7, CB), preferred_element_type=F32)
        y = y[:CB] + y[CB : 2 * CB] + y[2 * CB :]
        y = jnp.where(iota((CB, 2 * L), 0) == (h & (CB - 1)), y, 0.0)
        y = jnp.sum(y, axis=0, keepdims=True)
        looked[2 * i : 2 * i + 1, :] = y[:, :L]
        looked[2 * i + 1 : 2 * i + 2, :] = y[:, L:]


def strips_kernel(vf, wt, at_via, strips, volt, a_o, send_l, send_r):
    j = iota((8, L), 0)
    colid = jnp.where(j < 4, j, T - 8 + j)
    hs, ls = [], []
    for o in range(NO):
        f = vf[o : o + 1, :]
        a_o[:, lanes(o)] = onehot(f // T, T)
        hi, lo = hi_lo(at_via[o : o + 1, :] * wt[o : o + 1, :])
        on = colid == f % T
        hs.append(jnp.where(on, hi, 0.0))
        ls.append(jnp.where(on, lo, 0.0))
    lhs = jnp.concatenate(
        [jnp.concatenate(hs, axis=1), jnp.concatenate(ls, axis=1)], axis=0
    ).astype(BF16)
    inj = nt(lhs, a_o[...])
    inv = strips[8:16, :]
    z = strips[0:8, :] + (inj[0:8] + inj[8:16]) * inv
    low = iota((8, T), 0) < 4
    send_l[:, :T] = jnp.where(low, z, pltpu.roll(inv, 4, 0))
    send_r[:, :T] = jnp.where(low, pltpu.roll(z, 4, 0), inv)
    g, lane = iota((8, CB), 0), iota((8, CB), 1)
    send_l[:, T:] = nt(jnp.where(lane == g * GROUP, 1.0, 0.0), volt[...], HI)
    send_r[:, T:] = nt(jnp.where(lane == g * GROUP + GROUP - 1, 1.0, 0.0), volt[...], HI)


def rhs_kernel(vf, wt, at_via, zl, invd, a, z, rims, b_s):
    for o in range(NO):
        hi, lo = hi_lo(at_via[o : o + 1, :] * wt[o : o + 1, :])
        on = iota((T, L), 0) == vf[o : o + 1, :] % T
        b_s[:, lanes(o)] = jnp.where(on, hi, 0.0).astype(BF16)
        b_s[:, lanes(NO + o)] = jnp.where(on, lo, 0.0).astype(BF16)
    inj = nt(a[...], b_s[:, : NO * L]) + nt(a[...], b_s[:, NO * L :])
    zz = zl[...] + inj * invd[...]
    z[...] = zz
    rims[0:8, :] = zz[0:8]
    rims[8:16, :] = zz[T - 8 :]


def halo_columns(flags, gl, gr):
    left = jnp.where(flags[1] > 0, 1.0, 0.0)
    right = jnp.where(flags[1] < NO - 1, 1.0, 0.0)
    parts = []
    for x in (gr * right, gl * left):
        a, rest = hi_lo(x)
        b, c = hi_lo(rest)
        parts += [c, b, a]
    j, lane = iota((8, 2 * L), 0), iota((8, 2 * L), 1)
    to_r = jnp.where(lane == jnp.where(j < 4, j, L + j - 4), 1.0, 0.0)
    to_l = jnp.where(lane == jnp.where(j < 4, 124 + j, L + 120 + j), 1.0, 0.0)
    place = jnp.concatenate([to_r] * 3 + [to_l] * 3, axis=0)
    out = tn(jnp.concatenate(parts, axis=0).astype(BF16), place.astype(BF16))
    return out[:, :L], out[:, L:]


def edge_kernel(flags, zr, ir, got_l, got_r, volt, send_u, send_d, corners):
    zt, it = halo_columns(flags, got_l[:, :L], got_r[:, :L])
    zb, ib = halo_columns(flags, got_l[:, T - L : T], got_r[:, T - L : T])
    for k, x in enumerate((zt[0:16], zb[L - 16 :], it[0:16], ib[L - 16 :])):
        corners[16 * k : 16 * k + 16, :] = x
    low = iota((8, W), 0) < 4
    zt = jnp.concatenate([zr[0:8, :], zt[0:8]], axis=1)
    it = jnp.concatenate([ir[0:8, :], it[0:8]], axis=1)
    zb = jnp.concatenate([zr[8:16, :], zb[L - 8 :]], axis=1)
    ib = jnp.concatenate([ir[8:16, :], ib[L - 8 :]], axis=1)
    send_u[:, :W] = jnp.where(low, zt, pltpu.roll(it, 4, 0))
    send_d[:, :W] = jnp.where(low, pltpu.roll(zb, 4, 0), ib)
    send_u[:, W:] = volt[0:8, :]
    send_d[:, W:] = volt[CB - 8 :, :]


def beside(block):
    n = block.shape[0]
    rows = pltpu.roll(block, 1, 0) + pltpu.roll(block, n - 1, 0)
    return rows + (pltpu.roll(block, 1, 1) + pltpu.roll(block, W - 1, 1))


def near_tiles(ref, start, rows):
    mid = [ref[t, pl.ds(start, rows), :] for t in range(LT + 1)]
    low = [pltpu.roll(m, 1, 1) for m in mid]
    high = [pltpu.roll(m, L - 1, 1) for m in mid]
    lane = iota((rows, L), 1)
    near = []
    for t in range(LT + 1):
        rows_sum = ref[t, pl.ds(start - 1, rows), :] + ref[t, pl.ds(start + 1, rows), :]
        left = jnp.where(lane == 0, low[t - 1], low[t])
        right = jnp.where(lane == L - 1, high[(t + 1) % (LT + 1)], high[t])
        near.append(rows_sum + (left + right))
    return mid, near


def fold(p):
    return (p[:, 0:128] + p[:, 128:256]) + (p[:, 256:384] + p[:, 384:512])


def moments(z, w, n1, n2, dn3, inv):
    d = 1.0 / inv
    dz, dw, dn1, dn2 = d * z, d * w, d * n1, d * n2
    return dz * z, dz * w, dw * w, dw * n1, dn1 * n1, dn1 * n2, dn2 * n2, n2 * dn3


def basis_kernel(flags, z, invd, got_l, got_r, hist, acc_o, ie, ze, we, n1e, n2e, sem):
    zc, ic = halo_columns(flags, got_l[:, :T], got_r[:, :T])
    zero = jnp.zeros((OFF, L), F32)
    own = pl.ds(OFF, T)
    for e in (ie, ze, we, n1e, n2e):
        for t in range(LT + 1):
            e[t, 0:OFF, :] = zero
            e[t, OFF + T :, :] = zero
    for t in range(LT):
        ze[t, own, :] = z[:, lanes(t)]
        ie[t, own, :] = invd[:, lanes(t)]
    ze[LT, own, :] = zc
    ie[LT, own, :] = ic
    rows = 128

    def save(k, e):
        copy = pltpu.make_async_copy(e.at[pl.ds(0, LT), own, :], hist.at[k], sem.at[k])
        copy.start()
        return copy

    def apply_to(src, dst, minus):
        def step(i, carry):
            start = pl.multiple_of(OFF + i * rows, 8)
            mid, near = near_tiles(src, start, rows)
            for t in range(LT + 1):
                y = near[t] * ie[t, pl.ds(start, rows), :]
                dst[t, pl.ds(start, rows), :] = mid[t] - y if minus else y
            return carry

        lax.fori_loop(0, T // rows, step, 0)

    copies = [save(0, ze)]
    apply_to(ze, we, True)
    copies.append(save(1, we))
    apply_to(we, n1e, False)
    copies.append(save(2, n1e))
    apply_to(n1e, n2e, False)
    copies.append(save(3, n2e))

    acc = [jnp.zeros((8, L), F32) for _ in range(SUMS)]
    ends = list(range(0, T + 1, 64))
    ends[0], ends[-1] = 8, T - 8
    for low, high in zip(ends[:-1], ends[1:]):
        start, rows = OFF + low, high - low
        n2, dn3 = near_tiles(n2e, start, rows)
        for t in range(LT):
            z8, w8, n18, i8 = (e[t, pl.ds(start, rows), :] for e in (ze, we, n1e, ie))
            for k, p in enumerate(moments(z8, w8, n18, n2[t], dn3[t], i8)):
                for q in range(0, rows, 8):
                    acc[k] = acc[k] + p[q : q + 8]
    for k in range(SUMS):
        acc_o[8 * k : 8 * k + 8, :] = acc[k]
    for copy in copies:
        copy.wait()


def gram_terms(acc):
    g0, q0 = acc[0], acc[1]
    m = acc[2:]
    r = [q0, q0 - m[0], q0 - m[0] - m[1]]
    h = {(0, 0): q0, **{(0, j): RHO[0] * m[j - 1] for j in (1, 2, 3)}}
    b = [g0] + r
    for k in range(3):
        h[0, 0] = h[0, 0] - Q[k] * m[k]
        b[0] = b[0] - Q[k] * r[k]
    for k in range(6):
        f = sum(Q[j] * RHO[k - j] for j in range(3) if 0 <= k - j < 4)
        h[0, 0] = h[0, 0] - f * m[k]
    for j in (1, 2, 3):
        for k in (1, 2, 3):
            h[0, j] = h[0, j] + RHO[k] * m[j - 1 + k]
            if j <= k:
                h[j, k] = m[j + k - 2] - m[j + k - 1]
    out = []
    for p in range(4):
        out += [h[p, q] for q in range(p, 4)] + [b[p]]
    return out


def rim_kernel(flags, z, invd, corners, got_u, got_d, acc_i, rims, part):
    up = jnp.where(flags[0] > 0, 1.0, 0.0)
    down = jnp.where(flags[0] < 7, 1.0, 0.0)
    low = iota((8, W), 0) < 4
    acc = [acc_i[8 * k : 8 * k + 8, :] for k in range(SUMS)]
    top, bot = got_u[:, :W], got_d[:, :W]
    for end in (0, 1):
        rows = slice(0, 16) if end == 0 else slice(T - 16, T)
        zc, ic = corners[16 * end : 16 * end + 16, :], corners[32 + 16 * end : 48 + 16 * end, :]
        z16 = jnp.concatenate([z[rows, :], zc], axis=1)
        i16 = jnp.concatenate([invd[rows, :], ic], axis=1)
        if end == 0:
            zb = jnp.concatenate([jnp.where(low, 0.0, pltpu.roll(top, 4, 0)) * up, z16], axis=0)
            ib = jnp.concatenate([jnp.where(low, 0.0, top) * up, i16], axis=0)
            own = slice(8, 16)
        else:
            zb = jnp.concatenate([z16, jnp.where(low, bot, 0.0) * down], axis=0)
            ib = jnp.concatenate([i16, jnp.where(low, pltpu.roll(bot, 4, 0), 0.0) * down], axis=0)
            own = slice(8, 16)
        w = zb - ib * beside(zb)
        n1 = ib * beside(w)
        n2 = ib * beside(n1)
        near = beside(n2)
        zo, wo, n1o, n2o, dn3, io = (x[own, :T] for x in (zb, w, n1, n2, near, ib))
        for k, p in enumerate(moments(zo, wo, n1o, n2o, dn3, io)):
            acc[k] = acc[k] + fold(p)
        for k, x in enumerate((wo, n1o, n2o)):
            rims[16 * k + 8 * end : 16 * k + 8 * end + 8, :] = x
    terms = gram_terms(acc)
    rows14 = jnp.concatenate(
        [jnp.sum(a, axis=0, keepdims=True) for a in terms] + [jnp.zeros((2, L), F32)], axis=0
    )
    a, rest = hi_lo(rows14)
    b, c = hi_lo(rest)
    parts = jnp.concatenate([c, b, a], axis=0).astype(BF16)
    sums = nt(jnp.ones((8, L), BF16), parts)
    sums = sums[:, 0:16] + sums[:, 16:32] + sums[:, 32:48]
    sums = jnp.concatenate([sums, jnp.zeros((8, L - 16), F32)], axis=1)
    part[...] = sums


def gather_kernel(slots, hist, rims, vf, wt, g_o, x_s, slab, sem):
    copies = [pltpu.make_async_copy(hist.at[k], x_s.at[k], sem.at[k]) for k in range(4)]
    for copy in copies:
        copy.start()
    for k in range(4):
        copies[k].wait()
        if k:
            for t in range(LT):
                x_s[k, t, 0:8, :] = rims[16 * k - 16 : 16 * k - 8, lanes(t)]
                x_s[k, t, T - 8 :, :] = rims[16 * k - 8 : 16 * k, lanes(t)]

        def lay(i, carry):
            for b in range(4):
                for t in range(LT):
                    start = pl.multiple_of(i * 32 + 8 * b, 8)
                    to = (i * 32 + 8 * b) * SLAB + 4 * k + t
                    slab[pl.ds(to, 8, stride=SLAB), :] = x_s[k, t, pl.ds(start, 8), :]
            return carry

        lax.fori_loop(0, T // 32, lay, 0)
    lane, sub = iota((16, L), 1), iota((16, L), 0)

    def owner(o):
        acc = jnp.zeros((16, L), F32)
        for j in range(L):
            x = slab[pl.ds(slots[o, j], 16), :]
            x = pltpu.roll(x, slots[NO + o, j], 1)
            acc = jnp.where(lane == j, x, acc)
        f = vf[pl.ds(o, 1), :]
        acc = jnp.where((sub & 3) == ((f >> 7) & 3), acc * wt[pl.ds(o, 1), :], 0.0)
        rows = [jnp.sum(acc[4 * k : 4 * k + 4, :], axis=0, keepdims=True) for k in range(4)]
        g_o[pl.ds(pl.multiple_of(8 * o, 8), 8), :] = jnp.concatenate(
            rows + [jnp.zeros((4, L), F32)], axis=0
        )

    def owners(i, carry):
        owner(2 * i)
        owner(2 * i + 1)
        return carry

    lax.fori_loop(0, NO // 2, owners, 0)


def pack_kernel(g, rows, out):
    out[...] = g[...]
    total = jnp.sum(rows[...], axis=0, keepdims=True)
    for o in range(NO):
        out[8 * o + 4 : 8 * o + 5, :] = total


def solve(tot):
    lane = iota((1, L), 1)

    def pick(k):
        return jnp.sum(jnp.where(lane == k, tot, 0.0), axis=1, keepdims=True)

    h, b = {}, []
    k = 0
    for p in range(4):
        for q in range(p, 4):
            h[p, q] = pick(k)
            k += 1
        b.append(pick(k))
        k += 1
    floor = [3e-7 * h[p, p] for p in range(4)]
    inv = []
    for p in range(4):
        inv.append(jnp.where(h[p, p] > floor[p], 1.0 / h[p, p], 0.0))
        for q in range(p + 1, 4):
            f = h[p, q] * inv[p]
            for r in range(q, 4):
                h[q, r] = h[q, r] - f * h[p, r]
            b[q] = b[q] - f * b[p]
    c = [None] * 4
    for p in (3, 2, 1, 0):
        s = b[p]
        for q in range(p + 1, 4):
            s = s - h[p, q] * c[q]
        c[p] = s * inv[p]
    return [c[0]] + [c[k + 1] - Q[k] * c[0] for k in range(3)]


def combine_kernel(hist, coef, rims, out, h_s, x_s, sem_in, sem_out):
    n = T // STEPS
    load = [
        pltpu.make_async_copy(hist.at[:, :, pl.ds(i * n, n), :], h_s.at[i], sem_in.at[i])
        for i in range(STEPS)
    ]
    save = [
        pltpu.make_async_copy(x_s.at[pl.ds(i * n, n), :], out.at[pl.ds(i * n, n), :], sem_out.at[i])
        for i in range(STEPS)
    ]
    for copy in load:
        copy.start()
    c = [coef[k : k + 1, 0:1] for k in range(4)]
    for i in range(STEPS):
        load[i].wait()
        for t in range(LT):
            h = [h_s[i, k, t] for k in range(4)]
            x_s[i * n : (i + 1) * n, lanes(t)] = (c[0] * h[0] + c[1] * h[1]) + (
                c[2] * h[2] + c[3] * h[3]
            )
        for end, step, low in ((0, 0, 0), (1, STEPS - 1, n - 8)):
            if i == step:
                for t in range(LT):
                    x = c[0] * h_s[i, 0, t, low : low + 8, :]
                    for k in range(3):
                        x += c[k + 1] * rims[16 * k + 8 * end : 16 * k + 8 * end + 8, lanes(t)]
                    x_s[i * n + low : i * n + low + 8, lanes(t)] = x
        save[i].start()
    for copy in save:
        copy.wait()


def coarse_neighbours(flags, u, above, below, from_l, from_r):
    up = jnp.where(flags[0] > 0, 1.0, 0.0)
    down = jnp.where(flags[0] < 7, 1.0, 0.0)
    r, lane = iota((CB, CB), 0), iota((CB, CB), 1)
    g, gl = iota((8, CB), 0), iota((8, CB), 1)
    turned_l = jnp.where(g == 0, 0.0, pltpu.roll(from_l, 1, 0))
    turned_r = jnp.where(g == 7, 0.0, pltpu.roll(from_r, 7, 0))
    from_l = jnp.where(flags[1] == 0, turned_l, from_l)
    from_r = jnp.where(flags[1] == NO - 1, turned_r, from_r)
    seam_l = tn(from_l, jnp.where(gl == g * GROUP, 1.0, 0.0), HI)
    seam_r = tn(from_r, jnp.where(gl == g * GROUP + GROUP - 1, 1.0, 0.0), HI)
    near = jnp.where(r == 0, above * up, pltpu.roll(u, 1, 0))
    near += jnp.where(r == CB - 1, below * down, pltpu.roll(u, CB - 1, 0))
    near += jnp.where(lane % GROUP == 0, seam_l, pltpu.roll(u, 1, 1))
    near += jnp.where(lane % GROUP == GROUP - 1, seam_r, pltpu.roll(u, CB - 1, 1))
    return near


def base_kernel(
    flags, held, volt, cleak, got_l, got_r, got_u, got_d, cdiag, scale, base, r_o, c_o
):
    for o in range(NO):
        h = held[o : o + 1, :]
        r_o[:, lanes(o)] = onehot(h >> 7, CB)
        c_o[:, lanes(o)] = onehot(h & (CB - 1), CB)
    count = nt(r_o[...], c_o[...])
    diag = 4.0 * coarse_conductance + cleak[...] + via_conductance * count
    u = volt[...]
    near = coarse_neighbours(flags, u, got_u[7:8, W:], got_d[0:1, W:], got_l[:, T:], got_r[:, T:])
    cdiag[...] = diag
    scale[...] = relaxation / diag
    base[...] = u - relaxation * (diag * u - coarse_conductance * near) / diag


def sweep1_kernel(arrived, scale, base, r, c, coef, u_o, src_o, sl, sr, su, sd, v_s):
    tot = arrived[4:5, :]
    for o in range(1, NO):
        tot += arrived[8 * o + 4 : 8 * o + 5, :]
    d = solve(tot)
    sub = iota((8, L), 0)
    cf = jnp.zeros((8, L), F32)
    for k in range(4):
        cf = jnp.where(sub == k, d[k], cf)
    coef[...] = cf
    for o in range(NO):
        v = jnp.sum(arrived[8 * o : 8 * o + 8, :] * cf, axis=0, keepdims=True)
        hi, lo = hi_lo(v)
        on = c[:, lanes(o)]
        v_s[:, lanes(o)] = on * hi.astype(BF16)
        v_s[:, lanes(NO + o)] = on * lo.astype(BF16)
    src = nt(r[...], v_s[:, : NO * L]) + nt(r[...], v_s[:, NO * L :])
    u = base[...] + scale[...] * src
    u_o[...] = u
    src_o[...] = src
    g, gl = iota((8, CB), 0), iota((8, CB), 1)
    sl[...] = nt(jnp.where(gl == g * GROUP, 1.0, 0.0), u, HI)
    sr[...] = nt(jnp.where(gl == g * GROUP + GROUP - 1, 1.0, 0.0), u, HI)
    su[...] = u[0:8, :]
    sd[...] = u[CB - 8 :, :]


def sweep2_kernel(flags, u, src, cdiag, scale, got_l, got_r, got_u, got_d, u_o):
    near = coarse_neighbours(flags, u[...], got_u[7:8, :], got_d[0:1, :], got_l[...], got_r[...])
    u_o[...] = u[...] + scale[...] * (src[...] - (cdiag[...] * u[...] - coarse_conductance * near))


VM = pl.BlockSpec(memory_space=pltpu.VMEM)
SM = pl.BlockSpec(memory_space=pltpu.SMEM)
ANY = pl.BlockSpec(memory_space=pltpu.HBM)
vmem = pltpu.MemorySpace.VMEM
hbm = jax.ShapeDtypeStruct


def keep(*args):
    return [pltpu.with_memory_space_constraint(x, pltpu.VMEM) for x in args]


def leave(*args):
    return [pltpu.with_memory_space_constraint(x, pltpu.HBM) for x in args]


def call(body, outs, args, scratch=(), flags=None, flops=0, any_in=0, any_out=0):
    specs = ([] if flags is None else [SM]) + [ANY] * any_in + [VM] * (len(args) - any_in)
    return pl.pallas_call(
        body,
        out_shape=outs,
        in_specs=specs,
        out_specs=[ANY] * any_out + [VM] * (len(outs) - any_out),
        scratch_shapes=list(scratch),
        cost_estimate=pl.CostEstimate(flops=flops, bytes_accessed=0, transcendentals=0),
        compiler_params=pltpu.CompilerParams(vmem_limit_bytes=20 * 2**20),
    )(*([] if flags is None else [flags]), *args)


def ring(axis):
    n = lax.axis_size(axis)
    up = [(i, (i + 1) % n) for i in range(n)]
    return up, [(b, a) for a, b in up]


def swap(axis, to_low, to_high):
    up, down = ring(axis)
    return lax.ppermute(to_high, axis, up), lax.ppermute(to_low, axis, down)


def spread(x, axis=COL):
    return lax.all_to_all(x, axis, split_axis=0, concat_axis=0, tiled=True)


def per_device(load_amp, load_mask, leak, coarse_leak, coarse_init, via_fine, via_coarse, via_count):
    flags = jnp.where(
        jnp.arange(2, dtype=jnp.int32) == 0, lax.axis_index(ROW), lax.axis_index(COL)
    ).astype(jnp.int32)
    live = jnp.arange(L, dtype=jnp.int32)[None, :] < via_count.reshape(NO, 1)
    wt = jnp.where(live, via_conductance, 0.0).astype(F32)
    fine = via_fine.reshape(NO, L)
    coarse = via_coarse.reshape(NO, L)
    request = jnp.where(live, ((coarse >> 11) << 7) | (coarse & (CB - 1)), -1)
    held = spread(request)

    tile, block, slots = vmem((T, T), F32), vmem((CB, CB), F32), vmem((NO, L), F32)
    hot, chot = vmem((T, NO * L), BF16), vmem((CB, NO * L), BF16)
    hots = vmem((T, 2 * NO * L), BF16)
    rim16, side, seam = vmem((16, T), F32), vmem((8, W), F32), vmem((8, CB), F32)
    ext, packed = vmem((LT + 1, EXT, L), F32), ((L, L), F32)
    dmas = pltpu.SemaphoreType.DMA((4,))
    big = 20_000_000_000

    zl, invd, strips, irims, where = call(
        diag_kernel, [tile, tile, rim16, rim16, hbm((2 * NO, L), jnp.int32)],
        keep(fine, wt) + leave(load_amp, load_mask, leak), [hot, hot], flops=big,
    )
    looked = call(lookup_kernel, [slots], keep(held, coarse_init))[0]
    at_via = spread(looked)
    a, send_l, send_r = call(
        strips_kernel, [hot, side, side], keep(fine, wt, at_via, strips, coarse_init)
    )
    got_l, got_r = swap(COL, send_l, send_r)
    z, zrims = call(
        rhs_kernel, [tile, rim16], keep(fine, wt, at_via, zl, invd, a), [hots], flops=big
    )
    rim = vmem((8, W + CB), F32)
    send_u, send_d, corners = call(
        edge_kernel, [rim, rim, vmem((64, L), F32)], keep(zrims, irims, got_l, got_r, coarse_init), flags=flags
    )
    got_u, got_d = swap(ROW, send_u, send_d)
    hist, acc = call(
        basis_kernel, [pltpu.MemorySpace.HBM((4, LT, T, L), F32), vmem((8 * SUMS, L), F32)], keep(z, invd, got_l, got_r),
        [ext] * 5 + [dmas], flags=flags, flops=big, any_out=1,
    )
    rims, part = call(
        rim_kernel, [vmem((48, T), F32), vmem((8, L), F32)],
        keep(z, invd, corners, got_u, got_d, acc), flags=flags,
    )
    rows = spread(part, ROW)
    g = call(
        gather_kernel, [vmem(*packed)], leave(hist) + keep(rims, fine, wt),
        [vmem((4, LT, T, L), F32), vmem((T * SLAB, L), F32), dmas], flags=where, flops=big, any_in=1,
    )[0]
    arrived = spread(call(pack_kernel, [vmem(*packed)], keep(g, rows))[0])
    cdiag, scale, base, r_hot, c_hot = call(
        base_kernel, [block, block, block, chot, chot],
        keep(held, coarse_init, coarse_leak, got_l, got_r, got_u, got_d), flags=flags, flops=big,
    )
    coef, u, src, sl, sr, su, sd = call(
        sweep1_kernel, [seam, block, block, seam, seam, seam, seam],
        keep(arrived, scale, base, r_hot, c_hot), [vmem((CB, 2 * NO * L), BF16)],
    )
    hl, hr = swap(COL, sl, sr)
    hu, hd = swap(ROW, su, sd)
    fine_drop = call(
        combine_kernel, [pltpu.MemorySpace.HBM((T, T), F32)], leave(hist) + keep(coef, rims),
        [vmem((STEPS, 4, LT, T // STEPS, L), F32), tile, pltpu.SemaphoreType.DMA((STEPS,)),
         pltpu.SemaphoreType.DMA((STEPS,))], flops=big // 4, any_in=1, any_out=1,
    )[0]
    coarse_drop = call(
        sweep2_kernel, [hbm((CB, CB), F32)], keep(u, src, cdiag, scale, hl, hr, hu, hd), flags=flags
    )[0]
    return fine_drop, coarse_drop


def solution(mesh):
    spec = P(ROW, COL)

    return jax.shard_map(
        per_device, mesh=mesh, in_specs=(spec,) * 8, out_specs=(spec, spec), check_vma=False
    )
```

```python
import jax
import jax.numpy as jnp
from jax import lax
from jax.experimental import pallas as pl
from jax.experimental.pallas import tpu as pltpu
from jax.sharding import PartitionSpec as P


F32 = jnp.float32
BF16 = jnp.bfloat16
HI = lax.Precision.HIGHEST
ROW, COL = "row", "col"

GROUP = 16
via_conductance = 2.0
coarse_conductance = 4.0
relaxation = 0.8

T = 512
CB = 128
NO = 16
L = 128
OFF = 16
EXT = OFF + T + 16
W = T + L

Q = (1.09375, 1.765625, 1.28125)
RHO = (1.0 - Q[0], Q[0] - Q[1], Q[1] - Q[2], Q[2])
LT = T // L
SLAB = 4 * LT + 1
SUMS = 8
STEPS = 8


def iota(shape, dim):
    return lax.broadcasted_iota(jnp.int32, shape, dim)


def nt(a, b, precision=None):
    return lax.dot_general(
        a, b, (((1,), (1,)), ((), ())), precision=precision, preferred_element_type=F32
    )


def tn(a, b, precision=None):
    return lax.dot_general(
        a, b, (((0,), (0,)), ((), ())), precision=precision, preferred_element_type=F32
    )


def onehot(idx, n):
    return jnp.where(iota((n, idx.shape[1]), 0) == idx, 1.0, 0.0).astype(BF16)


def hi_lo(x):
    hi = x.astype(BF16).astype(F32)
    return hi, x - hi


def lanes(o):
    return slice(o * L, (o + 1) * L)


def pair_order(place, low, high):
    even = (place & 1) == 0
    return jnp.where(even, high, low), jnp.where(even, low, high)


def from_pairs(place, first, second):
    even = (place & 1) == 0
    return jnp.where(even, second, first), jnp.where(even, first, second)


def diag_kernel(vf, wt, amp, mask, leak, zl, invd, strips, rims, slots, a_s, b_s):
    slots[0:NO, :] = (vf[...] >> 9) * SLAB
    slots[NO:, :] = (iota((NO, L), 1) - vf[...]) & (L - 1)
    for o in range(NO):
        f = vf[o : o + 1, :]
        a_s[:, lanes(o)] = onehot(f // T, T)
        b_s[:, lanes(o)] = jnp.where(iota((T, L), 0) == f % T, wt[o : o + 1, :], 0.0).astype(BF16)
    inv = 1.0 / (4.0 + leak[...] + nt(a_s[...], b_s[...]))
    z = amp[...] * mask[...].astype(F32) * inv
    zl[...] = z
    invd[...] = inv
    j, lane = iota((8, L), 0), iota((8, L), 1)
    first = jnp.where((j < 4) & (lane == j), 1.0, 0.0)
    last = jnp.where((j >= 4) & (lane == 120 + j), 1.0, 0.0)
    strips[0:8, :] = nt(first, z[:, :L], HI) + nt(last, z[:, T - L :], HI)
    strips[8:16, :] = nt(first, inv[:, :L], HI) + nt(last, inv[:, T - L :], HI)
    rims[0:8, :] = inv[0:8]
    rims[8:16, :] = inv[T - 8 :]


def parts_kernel(volt, parts):
    v1, rest = hi_lo(volt[...].T)
    v2, v3 = hi_lo(rest)
    parts[...] = jnp.concatenate([v3, v2, v1], axis=0).astype(BF16)


def lookup_kernel(held, parts, looked):
    v = parts[...]
    for i in range(NO // 2):
        h = jnp.concatenate([held[2 * i : 2 * i + 1, :], held[2 * i + 1 : 2 * i + 2, :]], axis=1)
        y = jnp.dot(v, onehot(h >> 7, CB), preferred_element_type=F32)
        y = y[:CB] + y[CB : 2 * CB] + y[2 * CB :]
        y = jnp.where(iota((CB, 2 * L), 0) == (h & (CB - 1)), y, 0.0)
        y = jnp.sum(y, axis=0, keepdims=True)
        looked[2 * i : 2 * i + 1, :] = y[:, :L]
        looked[2 * i + 1 : 2 * i + 2, :] = y[:, L:]


def strips_kernel(flags, vf, wt, at_via, strips, volt, a_o, send_1, send_2):
    j = iota((8, L), 0)
    colid = jnp.where(j < 4, j, T - 8 + j)
    hs, ls = [], []
    for o in range(NO):
        f = vf[o : o + 1, :]
        a_o[:, lanes(o)] = onehot(f // T, T)
        hi, lo = hi_lo(at_via[o : o + 1, :] * wt[o : o + 1, :])
        on = colid == f % T
        hs.append(jnp.where(on, hi, 0.0))
        ls.append(jnp.where(on, lo, 0.0))
    lhs = jnp.concatenate(
        [jnp.concatenate(hs, axis=1), jnp.concatenate(ls, axis=1)], axis=0
    ).astype(BF16)
    inj = nt(lhs, a_o[...])
    inv = strips[8:16, :]
    z = strips[0:8, :] + (inj[0:8] + inj[8:16]) * inv
    low = iota((8, T), 0) < 4
    g, lane = iota((8, CB), 0), iota((8, CB), 1)
    to_l = jnp.where(low, z, pltpu.roll(inv, 4, 0))
    to_r = jnp.where(low, pltpu.roll(z, 4, 0), inv)
    send_1[:, :T], send_2[:, :T] = pair_order(flags[1], to_l, to_r)
    to_l = nt(jnp.where(lane == g * GROUP, 1.0, 0.0), volt[...], HI)
    to_r = nt(jnp.where(lane == g * GROUP + GROUP - 1, 1.0, 0.0), volt[...], HI)
    send_1[:, T:], send_2[:, T:] = pair_order(flags[1], to_l, to_r)


def rhs_kernel(vf, wt, at_via, zl, invd, a, z, rims, b_s):
    for o in range(NO):
        hi, lo = hi_lo(at_via[o : o + 1, :] * wt[o : o + 1, :])
        on = iota((T, L), 0) == vf[o : o + 1, :] % T
        b_s[:, lanes(o)] = jnp.where(on, hi, 0.0).astype(BF16)
        b_s[:, lanes(NO + o)] = jnp.where(on, lo, 0.0).astype(BF16)
    inj = nt(a[...], b_s[:, : NO * L]) + nt(a[...], b_s[:, NO * L :])
    zz = zl[...] + inj * invd[...]
    z[...] = zz
    rims[0:8, :] = zz[0:8]
    rims[8:16, :] = zz[T - 8 :]


def halo_columns(flags, gl, gr):
    left = jnp.where(flags[1] > 0, 1.0, 0.0)
    right = jnp.where(flags[1] < NO - 1, 1.0, 0.0)
    parts = []
    for x in (gr * right, gl * left):
        a, rest = hi_lo(x)
        b, c = hi_lo(rest)
        parts += [c, b, a]
    j, lane = iota((8, 2 * L), 0), iota((8, 2 * L), 1)
    to_r = jnp.where(lane == jnp.where(j < 4, j, L + j - 4), 1.0, 0.0)
    to_l = jnp.where(lane == jnp.where(j < 4, 124 + j, L + 120 + j), 1.0, 0.0)
    place = jnp.concatenate([to_r] * 3 + [to_l] * 3, axis=0)
    out = tn(jnp.concatenate(parts, axis=0).astype(BF16), place.astype(BF16))
    return out[:, :L], out[:, L:]


def edge_kernel(flags, zr, ir, col_1, col_2, volt, send_1, send_2, corners):
    got_l, got_r = from_pairs(flags[1], col_1[...], col_2[...])
    zt, it = halo_columns(flags, got_l[:, :L], got_r[:, :L])
    zb, ib = halo_columns(flags, got_l[:, T - L : T], got_r[:, T - L : T])
    for k, x in enumerate((zt[0:16], zb[L - 16 :], it[0:16], ib[L - 16 :])):
        corners[16 * k : 16 * k + 16, :] = x
    low = iota((8, W), 0) < 4
    zt = jnp.concatenate([zr[0:8, :], zt[0:8]], axis=1)
    it = jnp.concatenate([ir[0:8, :], it[0:8]], axis=1)
    zb = jnp.concatenate([zr[8:16, :], zb[L - 8 :]], axis=1)
    ib = jnp.concatenate([ir[8:16, :], ib[L - 8 :]], axis=1)
    to_u = jnp.where(low, zt, pltpu.roll(it, 4, 0))
    to_d = jnp.where(low, pltpu.roll(zb, 4, 0), ib)
    send_1[:, :W], send_2[:, :W] = pair_order(flags[0], to_u, to_d)
    send_1[:, W:], send_2[:, W:] = pair_order(flags[0], volt[0:8, :], volt[CB - 8 :, :])


def beside(block):
    n = block.shape[0]
    rows = pltpu.roll(block, 1, 0) + pltpu.roll(block, n - 1, 0)
    return rows + (pltpu.roll(block, 1, 1) + pltpu.roll(block, W - 1, 1))


def near_tiles(ref, start, rows):
    mid = [ref[t, pl.ds(start, rows), :] for t in range(LT + 1)]
    low = [pltpu.roll(m, 1, 1) for m in mid]
    high = [pltpu.roll(m, L - 1, 1) for m in mid]
    lane = iota((rows, L), 1)
    near = []
    for t in range(LT + 1):
        rows_sum = ref[t, pl.ds(start - 1, rows), :] + ref[t, pl.ds(start + 1, rows), :]
        left = jnp.where(lane == 0, low[t - 1], low[t])
        right = jnp.where(lane == L - 1, high[(t + 1) % (LT + 1)], high[t])
        near.append(rows_sum + (left + right))
    return mid, near


def fold(p):
    return (p[:, 0:128] + p[:, 128:256]) + (p[:, 256:384] + p[:, 384:512])


def moments(z, w, n1, n2, dn3, inv):
    d = 1.0 / inv
    dz, dw, dn1, dn2 = d * z, d * w, d * n1, d * n2
    return dz * z, dz * w, dw * w, dw * n1, dn1 * n1, dn1 * n2, dn2 * n2, n2 * dn3


def basis_kernel(flags, z, invd, col_1, col_2, hist, acc_o, ie, ze, we, n1e, n2e, sem):
    zc, ic = halo_columns(flags, *from_pairs(flags[1], col_1[:, :T], col_2[:, :T]))
    zero = jnp.zeros((OFF, L), F32)
    own = pl.ds(OFF, T)
    for e in (ie, ze, we, n1e, n2e):
        for t in range(LT + 1):
            e[t, 0:OFF, :] = zero
            e[t, OFF + T :, :] = zero
    for t in range(LT):
        ze[t, own, :] = z[:, lanes(t)]
        ie[t, own, :] = invd[:, lanes(t)]
    ze[LT, own, :] = zc
    ie[LT, own, :] = ic
    rows = 128

    def save(k, e):
        copy = pltpu.make_async_copy(e.at[pl.ds(0, LT), own, :], hist.at[k], sem.at[k])
        copy.start()
        return copy

    def apply_to(src, dst, minus):
        def step(i, carry):
            start = pl.multiple_of(OFF + i * rows, 8)
            mid, near = near_tiles(src, start, rows)
            for t in range(LT + 1):
                y = near[t] * ie[t, pl.ds(start, rows), :]
                dst[t, pl.ds(start, rows), :] = mid[t] - y if minus else y
            return carry

        lax.fori_loop(0, T // rows, step, 0)

    copies = [save(0, ze)]
    apply_to(ze, we, True)
    copies.append(save(1, we))
    apply_to(we, n1e, False)
    copies.append(save(2, n1e))
    apply_to(n1e, n2e, False)
    copies.append(save(3, n2e))

    acc = [jnp.zeros((8, L), F32) for _ in range(SUMS)]
    ends = list(range(0, T + 1, 64))
    ends[0], ends[-1] = 8, T - 8
    for low, high in zip(ends[:-1], ends[1:]):
        start, rows = OFF + low, high - low
        n2, dn3 = near_tiles(n2e, start, rows)
        for t in range(LT):
            z8, w8, n18, i8 = (e[t, pl.ds(start, rows), :] for e in (ze, we, n1e, ie))
            for k, p in enumerate(moments(z8, w8, n18, n2[t], dn3[t], i8)):
                for q in range(0, rows, 8):
                    acc[k] = acc[k] + p[q : q + 8]
    for k in range(SUMS):
        acc_o[8 * k : 8 * k + 8, :] = acc[k]
    for copy in copies:
        copy.wait()


def gram_terms(acc):
    g0, q0 = acc[0], acc[1]
    m = acc[2:]
    r = [q0, q0 - m[0], q0 - m[0] - m[1]]
    h = {(0, 0): q0, **{(0, j): RHO[0] * m[j - 1] for j in (1, 2, 3)}}
    b = [g0] + r
    for k in range(3):
        h[0, 0] = h[0, 0] - Q[k] * m[k]
        b[0] = b[0] - Q[k] * r[k]
    for k in range(6):
        f = sum(Q[j] * RHO[k - j] for j in range(3) if 0 <= k - j < 4)
        h[0, 0] = h[0, 0] - f * m[k]
    for j in (1, 2, 3):
        for k in (1, 2, 3):
            h[0, j] = h[0, j] + RHO[k] * m[j - 1 + k]
            if j <= k:
                h[j, k] = m[j + k - 2] - m[j + k - 1]
    out = []
    for p in range(4):
        out += [h[p, q] for q in range(p, 4)] + [b[p]]
    return out


def rim_kernel(flags, z, invd, corners, row_1, row_2, acc_i, rims, part):
    up = jnp.where(flags[0] > 0, 1.0, 0.0)
    down = jnp.where(flags[0] < 7, 1.0, 0.0)
    low = iota((8, W), 0) < 4
    acc = [acc_i[8 * k : 8 * k + 8, :] for k in range(SUMS)]
    top, bot = from_pairs(flags[0], row_1[:, :W], row_2[:, :W])
    for end in (0, 1):
        rows = slice(0, 16) if end == 0 else slice(T - 16, T)
        zc, ic = corners[16 * end : 16 * end + 16, :], corners[32 + 16 * end : 48 + 16 * end, :]
        z16 = jnp.concatenate([z[rows, :], zc], axis=1)
        i16 = jnp.concatenate([invd[rows, :], ic], axis=1)
        if end == 0:
            zb = jnp.concatenate([jnp.where(low, 0.0, pltpu.roll(top, 4, 0)) * up, z16], axis=0)
            ib = jnp.concatenate([jnp.where(low, 0.0, top) * up, i16], axis=0)
            own = slice(8, 16)
        else:
            zb = jnp.concatenate([z16, jnp.where(low, bot, 0.0) * down], axis=0)
            ib = jnp.concatenate([i16, jnp.where(low, pltpu.roll(bot, 4, 0), 0.0) * down], axis=0)
            own = slice(8, 16)
        w = zb - ib * beside(zb)
        n1 = ib * beside(w)
        n2 = ib * beside(n1)
        near = beside(n2)
        zo, wo, n1o, n2o, dn3, io = (x[own, :T] for x in (zb, w, n1, n2, near, ib))
        for k, p in enumerate(moments(zo, wo, n1o, n2o, dn3, io)):
            acc[k] = acc[k] + fold(p)
        for k, x in enumerate((wo, n1o, n2o)):
            rims[16 * k + 8 * end : 16 * k + 8 * end + 8, :] = x
    terms = gram_terms(acc)
    rows14 = jnp.concatenate(
        [jnp.sum(a, axis=0, keepdims=True) for a in terms] + [jnp.zeros((2, L), F32)], axis=0
    )
    a, rest = hi_lo(rows14)
    b, c = hi_lo(rest)
    parts = jnp.concatenate([c, b, a], axis=0).astype(BF16)
    sums = nt(jnp.ones((8, L), BF16), parts)
    sums = sums[:, 0:16] + sums[:, 16:32] + sums[:, 32:48]
    sums = jnp.concatenate([sums, jnp.zeros((8, L - 16), F32)], axis=1)
    part[...] = sums


def gather_kernel(slots, hist, rims, vf, wt, g_o, x_s, slab, sem):
    copies = [pltpu.make_async_copy(hist.at[k], x_s.at[k], sem.at[k]) for k in range(4)]
    for copy in copies:
        copy.start()
    for k in range(4):
        copies[k].wait()
        if k:
            for t in range(LT):
                x_s[k, t, 0:8, :] = rims[16 * k - 16 : 16 * k - 8, lanes(t)]
                x_s[k, t, T - 8 :, :] = rims[16 * k - 8 : 16 * k, lanes(t)]

        def lay(i, carry):
            for b in range(4):
                for t in range(LT):
                    start = pl.multiple_of(i * 32 + 8 * b, 8)
                    to = (i * 32 + 8 * b) * SLAB + 4 * k + t
                    slab[pl.ds(to, 8, stride=SLAB), :] = x_s[k, t, pl.ds(start, 8), :]
            return carry

        lax.fori_loop(0, T // 32, lay, 0)
    lane, sub = iota((16, L), 1), iota((16, L), 0)

    def owner(o):
        acc = jnp.zeros((16, L), F32)
        for j in range(L):
            x = slab[pl.ds(slots[o, j], 16), :]
            x = pltpu.roll(x, slots[NO + o, j], 1)
            acc = jnp.where(lane == j, x, acc)
        f = vf[o : o + 1, :]
        acc = jnp.where((sub & 3) == ((f >> 7) & 3), acc * wt[o : o + 1, :], 0.0)
        rows = [jnp.sum(acc[4 * k : 4 * k + 4, :], axis=0, keepdims=True) for k in range(4)]
        g_o[8 * o : 8 * o + 8, :] = jnp.concatenate(rows + [jnp.zeros((4, L), F32)], axis=0)

    for o in range(NO):
        owner(o)


def pack_kernel(g, rows, out):
    out[...] = g[...]
    total = jnp.sum(rows[...], axis=0, keepdims=True)
    for o in range(NO):
        out[8 * o + 4 : 8 * o + 5, :] = total


def solve(tot):
    lane = iota((1, L), 1)

    def pick(k):
        return jnp.sum(jnp.where(lane == k, tot, 0.0), axis=1, keepdims=True)

    h, b = {}, []
    k = 0
    for p in range(4):
        for q in range(p, 4):
            h[p, q] = pick(k)
            k += 1
        b.append(pick(k))
        k += 1
    floor = [3e-7 * h[p, p] for p in range(4)]
    inv = []
    for p in range(4):
        inv.append(jnp.where(h[p, p] > floor[p], 1.0 / h[p, p], 0.0))
        for q in range(p + 1, 4):
            f = h[p, q] * inv[p]
            for r in range(q, 4):
                h[q, r] = h[q, r] - f * h[p, r]
            b[q] = b[q] - f * b[p]
    c = [None] * 4
    for p in (3, 2, 1, 0):
        s = b[p]
        for q in range(p + 1, 4):
            s = s - h[p, q] * c[q]
        c[p] = s * inv[p]
    return [c[0]] + [c[k + 1] - Q[k] * c[0] for k in range(3)]


def combine_kernel(hist, coef, rims, out, h_s, x_s, sem_in, sem_out):
    n = T // STEPS
    load = [
        pltpu.make_async_copy(hist.at[:, :, pl.ds(i * n, n), :], h_s.at[i], sem_in.at[i])
        for i in range(STEPS)
    ]
    save = [
        pltpu.make_async_copy(x_s.at[pl.ds(i * n, n), :], out.at[pl.ds(i * n, n), :], sem_out.at[i])
        for i in range(STEPS)
    ]
    for copy in load:
        copy.start()
    c = [coef[k : k + 1, 0:1] for k in range(4)]
    for i in range(STEPS):
        load[i].wait()
        for t in range(LT):
            h = [h_s[i, k, t] for k in range(4)]
            x_s[i * n : (i + 1) * n, lanes(t)] = (c[0] * h[0] + c[1] * h[1]) + (
                c[2] * h[2] + c[3] * h[3]
            )
        for end, step, low in ((0, 0, 0), (1, STEPS - 1, n - 8)):
            if i == step:
                for t in range(LT):
                    x = c[0] * h_s[i, 0, t, low : low + 8, :]
                    for k in range(3):
                        x += c[k + 1] * rims[16 * k + 8 * end : 16 * k + 8 * end + 8, lanes(t)]
                    x_s[i * n + low : i * n + low + 8, lanes(t)] = x
        save[i].start()
    for copy in save:
        copy.wait()


def coarse_neighbours(flags, u, row_1, row_2, col_1, col_2):
    above, below = from_pairs(flags[0], row_1, row_2)
    above, below = above[7:8, :], below[0:1, :]
    from_l, from_r = from_pairs(flags[1], col_1, col_2)
    up = jnp.where(flags[0] > 0, 1.0, 0.0)
    down = jnp.where(flags[0] < 7, 1.0, 0.0)
    r, lane = iota((CB, CB), 0), iota((CB, CB), 1)
    g, gl = iota((8, CB), 0), iota((8, CB), 1)
    turned_l = jnp.where(g == 0, 0.0, pltpu.roll(from_l, 1, 0))
    turned_r = jnp.where(g == 7, 0.0, pltpu.roll(from_r, 7, 0))
    from_l = jnp.where(flags[1] == 0, turned_l, from_l)
    from_r = jnp.where(flags[1] == NO - 1, turned_r, from_r)
    seam_l = tn(from_l, jnp.where(gl == g * GROUP, 1.0, 0.0), HI)
    seam_r = tn(from_r, jnp.where(gl == g * GROUP + GROUP - 1, 1.0, 0.0), HI)
    near = jnp.where(r == 0, above * up, pltpu.roll(u, 1, 0))
    near += jnp.where(r == CB - 1, below * down, pltpu.roll(u, CB - 1, 0))
    near += jnp.where(lane % GROUP == 0, seam_l, pltpu.roll(u, 1, 1))
    near += jnp.where(lane % GROUP == GROUP - 1, seam_r, pltpu.roll(u, CB - 1, 1))
    return near


def base_kernel(
    flags, held, volt, cleak, col_1, col_2, row_1, row_2, cdiag, scale, base, r_o, c_o
):
    for o in range(NO):
        h = held[o : o + 1, :]
        r_o[:, lanes(o)] = onehot(h >> 7, CB)
        c_o[:, lanes(o)] = onehot(h & (CB - 1), CB)
    count = nt(r_o[...], c_o[...])
    diag = 4.0 * coarse_conductance + cleak[...] + via_conductance * count
    u = volt[...]
    near = coarse_neighbours(flags, u, row_1[:, W:], row_2[:, W:], col_1[:, T:], col_2[:, T:])
    cdiag[...] = diag
    scale[...] = relaxation / diag
    base[...] = u - relaxation * (diag * u - coarse_conductance * near) / diag


def sweep1_kernel(flags, arrived, scale, base, r, c, coef, u_o, src_o, c1, c2, r1, r2, v_s):
    tot = arrived[4:5, :]
    for o in range(1, NO):
        tot += arrived[8 * o + 4 : 8 * o + 5, :]
    d = solve(tot)
    sub = iota((8, L), 0)
    cf = jnp.zeros((8, L), F32)
    for k in range(4):
        cf = jnp.where(sub == k, d[k], cf)
    coef[...] = cf
    for o in range(NO):
        v = jnp.sum(arrived[8 * o : 8 * o + 8, :] * cf, axis=0, keepdims=True)
        hi, lo = hi_lo(v)
        on = c[:, lanes(o)]
        v_s[:, lanes(o)] = on * hi.astype(BF16)
        v_s[:, lanes(NO + o)] = on * lo.astype(BF16)
    src = nt(r[...], v_s[:, : NO * L]) + nt(r[...], v_s[:, NO * L :])
    u = base[...] + scale[...] * src
    u_o[...] = u
    src_o[...] = src
    g, gl = iota((8, CB), 0), iota((8, CB), 1)
    to_l = nt(jnp.where(gl == g * GROUP, 1.0, 0.0), u, HI)
    to_r = nt(jnp.where(gl == g * GROUP + GROUP - 1, 1.0, 0.0), u, HI)
    c1[...], c2[...] = pair_order(flags[1], to_l, to_r)
    r1[...], r2[...] = pair_order(flags[0], u[0:8, :], u[CB - 8 :, :])


def sweep2_kernel(flags, u, src, cdiag, scale, col_1, col_2, row_1, row_2, u_o):
    near = coarse_neighbours(flags, u[...], row_1[...], row_2[...], col_1[...], col_2[...])
    u_o[...] = u[...] + scale[...] * (src[...] - (cdiag[...] * u[...] - coarse_conductance * near))


VM = pl.BlockSpec(memory_space=pltpu.VMEM)
SM = pl.BlockSpec(memory_space=pltpu.SMEM)
ANY = pl.BlockSpec(memory_space=pltpu.HBM)
vmem = pltpu.MemorySpace.VMEM
hbm = jax.ShapeDtypeStruct


def keep(*args):
    return [pltpu.with_memory_space_constraint(x, pltpu.VMEM) for x in args]


def leave(*args):
    return [pltpu.with_memory_space_constraint(x, pltpu.HBM) for x in args]


def call(body, outs, args, scratch=(), flags=None, flops=0, any_in=0, any_out=0):
    specs = ([] if flags is None else [SM]) + [ANY] * any_in + [VM] * (len(args) - any_in)
    return pl.pallas_call(
        body,
        out_shape=outs,
        in_specs=specs,
        out_specs=[ANY] * any_out + [VM] * (len(outs) - any_out),
        scratch_shapes=list(scratch),
        cost_estimate=pl.CostEstimate(flops=flops, bytes_accessed=0, transcendentals=0),
        compiler_params=pltpu.CompilerParams(vmem_limit_bytes=20 * 2**20),
    )(*([] if flags is None else [flags]), *args)


def exchange(axis, first, second):
    n = lax.axis_size(axis)
    near = [(i, i ^ 1) for i in range(n)]
    far = [(i, ((i + 1) ^ 1) - 1 & (n - 1)) for i in range(n)]
    return lax.ppermute(first, axis, near), lax.ppermute(second, axis, far)


def spread(x, axis=COL):
    return lax.all_to_all(x, axis, split_axis=0, concat_axis=0, tiled=True)


def per_device(load_amp, load_mask, leak, coarse_leak, coarse_init, via_fine, via_coarse, via_count):
    flags = jnp.where(
        jnp.arange(2, dtype=jnp.int32) == 0, lax.axis_index(ROW), lax.axis_index(COL)
    ).astype(jnp.int32)
    live = jnp.arange(L, dtype=jnp.int32)[None, :] < via_count.reshape(NO, 1)
    wt = jnp.where(live, via_conductance, 0.0).astype(F32)
    fine = via_fine.reshape(NO, L)
    coarse = via_coarse.reshape(NO, L)
    request = jnp.where(live, ((coarse >> 11) << 7) | (coarse & (CB - 1)), -1)
    held = spread(request)

    tile, block, slots = vmem((T, T), F32), vmem((CB, CB), F32), vmem((NO, L), F32)
    hot, chot = vmem((T, NO * L), BF16), vmem((CB, NO * L), BF16)
    hots = vmem((T, 2 * NO * L), BF16)
    rim16, side, seam = vmem((16, T), F32), vmem((8, W), F32), vmem((8, CB), F32)
    ext, packed = vmem((LT + 1, EXT, L), F32), ((L, L), F32)
    dmas = pltpu.SemaphoreType.DMA((4,))
    big = 20_000_000_000

    zl, invd, strips, irims, where = call(
        diag_kernel, [tile, tile, rim16, rim16, hbm((2 * NO, L), jnp.int32)],
        keep(fine, wt) + leave(load_amp, load_mask, leak), [hot, hot], flops=big,
    )
    drops = call(parts_kernel, [vmem((3 * CB, CB), BF16)], leave(coarse_init))[0]
    looked = call(lookup_kernel, [slots], keep(held, drops))[0]
    at_via = spread(looked)
    a, send_1, send_2 = call(
        strips_kernel, [hot, side, side], keep(fine, wt, at_via, strips, coarse_init), flags=flags
    )
    col_1, col_2 = exchange(COL, send_1, send_2)
    z, zrims = call(
        rhs_kernel, [tile, rim16], keep(fine, wt, at_via, zl, invd, a), [hots], flops=big
    )
    rim = vmem((8, W + CB), F32)
    send_1, send_2, corners = call(
        edge_kernel, [rim, rim, vmem((64, L), F32)],
        keep(zrims, irims, col_1, col_2, coarse_init), flags=flags,
    )
    row_1, row_2 = exchange(ROW, send_1, send_2)
    hist, acc = call(
        basis_kernel, [pltpu.MemorySpace.HBM((4, LT, T, L), F32), vmem((8 * SUMS, L), F32)], keep(z, invd, col_1, col_2),
        [ext] * 5 + [dmas], flags=flags, flops=big, any_out=1,
    )
    rims, part = call(
        rim_kernel, [vmem((48, T), F32), vmem((8, L), F32)],
        keep(z, invd, corners, row_1, row_2, acc), flags=flags,
    )
    rows = spread(part, ROW)
    g = call(
        gather_kernel, [vmem(*packed)], leave(hist) + keep(rims, fine, wt),
        [vmem((4, LT, T, L), F32), vmem((T * SLAB, L), F32), dmas], flags=where, flops=big, any_in=1,
    )[0]
    arrived = spread(call(pack_kernel, [vmem(*packed)], keep(g, rows))[0])
    cdiag, scale, base, r_hot, c_hot = call(
        base_kernel, [block, block, block, chot, chot],
        keep(held, coarse_init, coarse_leak, col_1, col_2, row_1, row_2), flags=flags, flops=big,
    )
    coef, u, src, c1, c2, r1, r2 = call(
        sweep1_kernel, [seam, block, block, seam, seam, seam, seam],
        keep(arrived, scale, base, r_hot, c_hot), [vmem((CB, 2 * NO * L), BF16)], flags=flags,
    )
    c1, c2 = exchange(COL, c1, c2)
    r1, r2 = exchange(ROW, r1, r2)
    fine_drop = call(
        combine_kernel, [pltpu.MemorySpace.HBM((T, T), F32)], leave(hist) + keep(coef, rims),
        [vmem((STEPS, 4, LT, T // STEPS, L), F32), tile, pltpu.SemaphoreType.DMA((STEPS,)),
         pltpu.SemaphoreType.DMA((STEPS,))], flops=big // 4, any_in=1, any_out=1,
    )[0]
    coarse_drop = call(
        sweep2_kernel, [hbm((CB, CB), F32)], keep(u, src, cdiag, scale, c1, c2, r1, r2), flags=flags
    )[0]
    return fine_drop, coarse_drop


def solution(mesh):
    spec = P(ROW, COL)

    return jax.shard_map(
        per_device, mesh=mesh, in_specs=(spec,) * 8, out_specs=(spec, spec), check_vma=False
    )
```

```python
import jax
import jax.numpy as jnp
from jax import lax
from jax.experimental import pallas as pl
from jax.experimental.pallas import tpu as pltpu
from jax.sharding import PartitionSpec as P


F32 = jnp.float32
BF16 = jnp.bfloat16
HI = lax.Precision.HIGHEST
ROW, COL = "row", "col"

GROUP = 16
via_conductance = 2.0
coarse_conductance = 4.0
relaxation = 0.8

T = 512
CB = 128
NO = 16
L = 128
OFF = 16
EXT = OFF + T + 16
W = T + L

Q = (1.09375, 1.765625, 1.28125)
RHO = (1.0 - Q[0], Q[0] - Q[1], Q[1] - Q[2], Q[2])
LT = T // L
SLAB = 4 * LT + 1
SUMS = 8
STEPS = 8


def iota(shape, dim):
    return lax.broadcasted_iota(jnp.int32, shape, dim)


def nt(a, b, precision=None):
    return lax.dot_general(
        a, b, (((1,), (1,)), ((), ())), precision=precision, preferred_element_type=F32
    )


def tn(a, b, precision=None):
    return lax.dot_general(
        a, b, (((0,), (0,)), ((), ())), precision=precision, preferred_element_type=F32
    )


def onehot(idx, n):
    return jnp.where(iota((n, idx.shape[1]), 0) == idx, 1.0, 0.0).astype(BF16)


def hi_lo(x):
    hi = x.astype(BF16).astype(F32)
    return hi, x - hi


def lanes(o):
    return slice(o * L, (o + 1) * L)


def at(pos, k, like):
    return jnp.broadcast_to(pos[k : k + 1, : like.shape[1]], like.shape)


def pair_order(pos, k, low, high):
    even = (at(pos, k, low) & 1) == 0
    return jnp.where(even, high, low), jnp.where(even, low, high)


def from_pairs(pos, k, first, second):
    even = (at(pos, k, first) & 1) == 0
    return jnp.where(even, second, first), jnp.where(even, first, second)


def diag_kernel(amp, mask, leak, vf, wt, zl, invd, strips, rims, a_s, b_s, amp_s, mask_s, leak_s, sem):
    copies = [
        pltpu.make_async_copy(x, y, sem.at[k])
        for k, (x, y) in enumerate(((leak, leak_s), (amp, amp_s), (mask, mask_s)))
    ]
    for copy in copies:
        copy.start()
    for o in range(NO):
        f = vf[o : o + 1, :]
        a_s[:, lanes(o)] = onehot(f // T, T)
        b_s[:, lanes(o)] = jnp.where(iota((T, L), 0) == f % T, wt[o : o + 1, :], 0.0).astype(BF16)
    via = nt(a_s[...], b_s[...])
    for copy in copies:
        copy.wait()
    inv = 1.0 / (4.0 + leak_s[...] + via)
    z = amp_s[...] * mask_s[...].astype(F32) * inv
    zl[...] = z
    invd[...] = inv
    j, lane = iota((8, L), 0), iota((8, L), 1)
    first = jnp.where((j < 4) & (lane == j), 1.0, 0.0)
    last = jnp.where((j >= 4) & (lane == 120 + j), 1.0, 0.0)
    strips[0:8, :] = nt(first, z[:, :L], HI) + nt(last, z[:, T - L :], HI)
    strips[8:16, :] = nt(first, inv[:, :L], HI) + nt(last, inv[:, T - L :], HI)
    rims[0:8, :] = inv[0:8]
    rims[8:16, :] = inv[T - 8 :]


def parts_kernel(volt, vf, parts, slots, volt_o, vf_o):
    volt_o[...] = volt[...]
    vf_o[...] = vf[...]
    f = vf[...]
    slots[0:NO, :] = (f >> 9) * SLAB + ((f >> 7) & 3) * 4
    slots[NO:, :] = (iota((NO, L), 1) - f) & (L - 1)
    v1, rest = hi_lo(volt[...].T)
    v2, v3 = hi_lo(rest)
    parts[...] = jnp.concatenate([v3, v2, v1], axis=0).astype(BF16)


def lookup_kernel(held, parts, looked):
    v = parts[...]
    for i in range(NO // 2):
        h = jnp.concatenate([held[2 * i : 2 * i + 1, :], held[2 * i + 1 : 2 * i + 2, :]], axis=1)
        y = jnp.dot(v, onehot(h >> 7, CB), preferred_element_type=F32)
        y = y[:CB] + y[CB : 2 * CB] + y[2 * CB :]
        y = jnp.where(iota((CB, 2 * L), 0) == (h & (CB - 1)), y, 0.0)
        y = jnp.sum(y, axis=0, keepdims=True)
        looked[2 * i : 2 * i + 1, :] = y[:, :L]
        looked[2 * i + 1 : 2 * i + 2, :] = y[:, L:]


def strips_kernel(pos, vf, wt, at_via, strips, volt, a_o, send_1, send_2):
    j = iota((8, L), 0)
    colid = jnp.where(j < 4, j, T - 8 + j)
    hs, ls = [], []
    for o in range(NO):
        f = vf[o : o + 1, :]
        a_o[:, lanes(o)] = onehot(f // T, T)
        hi, lo = hi_lo(at_via[o : o + 1, :] * wt[o : o + 1, :])
        on = colid == f % T
        hs.append(jnp.where(on, hi, 0.0))
        ls.append(jnp.where(on, lo, 0.0))
    lhs = jnp.concatenate(
        [jnp.concatenate(hs, axis=1), jnp.concatenate(ls, axis=1)], axis=0
    ).astype(BF16)
    inj = nt(lhs, a_o[...])
    inv = strips[8:16, :]
    z = strips[0:8, :] + (inj[0:8] + inj[8:16]) * inv
    low = iota((8, T), 0) < 4
    g, lane = iota((8, CB), 0), iota((8, CB), 1)
    to_l = jnp.where(low, z, pltpu.roll(inv, 4, 0))
    to_r = jnp.where(low, pltpu.roll(z, 4, 0), inv)
    send_1[:, :T], send_2[:, :T] = pair_order(pos, 1, to_l, to_r)
    to_l = nt(jnp.where(lane == g * GROUP, 1.0, 0.0), volt[...], HI)
    to_r = nt(jnp.where(lane == g * GROUP + GROUP - 1, 1.0, 0.0), volt[...], HI)
    send_1[:, T:], send_2[:, T:] = pair_order(pos, 1, to_l, to_r)


def rhs_kernel(vf, wt, at_via, zl, invd, a, z, rims, b_s):
    for o in range(NO):
        hi, lo = hi_lo(at_via[o : o + 1, :] * wt[o : o + 1, :])
        on = iota((T, L), 0) == vf[o : o + 1, :] % T
        b_s[:, lanes(o)] = jnp.where(on, hi, 0.0).astype(BF16)
        b_s[:, lanes(NO + o)] = jnp.where(on, lo, 0.0).astype(BF16)
    inj = nt(a[...], b_s[:, : NO * L]) + nt(a[...], b_s[:, NO * L :])
    zz = zl[...] + inj * invd[...]
    z[...] = zz
    rims[0:8, :] = zz[0:8]
    rims[8:16, :] = zz[T - 8 :]


def halo_columns(pos, gl, gr):
    place = at(pos, 1, gl)
    parts = []
    for x in (jnp.where(place < NO - 1, gr, 0.0), jnp.where(place > 0, gl, 0.0)):
        a, rest = hi_lo(x)
        b, c = hi_lo(rest)
        parts += [c, b, a]
    j, lane = iota((8, 2 * L), 0), iota((8, 2 * L), 1)
    to_r = jnp.where(lane == jnp.where(j < 4, j, L + j - 4), 1.0, 0.0)
    to_l = jnp.where(lane == jnp.where(j < 4, 124 + j, L + 120 + j), 1.0, 0.0)
    place = jnp.concatenate([to_r] * 3 + [to_l] * 3, axis=0)
    out = tn(jnp.concatenate(parts, axis=0).astype(BF16), place.astype(BF16))
    return out[:, :L], out[:, L:]


def edge_kernel(pos, zr, ir, col_1, col_2, volt, send_1, send_2, corners):
    got_l, got_r = from_pairs(pos, 1, col_1[...], col_2[...])
    zt, it = halo_columns(pos, got_l[:, :L], got_r[:, :L])
    zb, ib = halo_columns(pos, got_l[:, T - L : T], got_r[:, T - L : T])
    for k, x in enumerate((zt[0:16], zb[L - 16 :], it[0:16], ib[L - 16 :])):
        corners[16 * k : 16 * k + 16, :] = x
    low = iota((8, W), 0) < 4
    zt = jnp.concatenate([zr[0:8, :], zt[0:8]], axis=1)
    it = jnp.concatenate([ir[0:8, :], it[0:8]], axis=1)
    zb = jnp.concatenate([zr[8:16, :], zb[L - 8 :]], axis=1)
    ib = jnp.concatenate([ir[8:16, :], ib[L - 8 :]], axis=1)
    to_u = jnp.where(low, zt, pltpu.roll(it, 4, 0))
    to_d = jnp.where(low, pltpu.roll(zb, 4, 0), ib)
    send_1[:, :W], send_2[:, :W] = pair_order(pos, 0, to_u, to_d)
    send_1[:, W:], send_2[:, W:] = pair_order(pos, 0, volt[0:8, :], volt[CB - 8 :, :])


def beside(block):
    n = block.shape[0]
    rows = pltpu.roll(block, 1, 0) + pltpu.roll(block, n - 1, 0)
    return rows + (pltpu.roll(block, 1, 1) + pltpu.roll(block, W - 1, 1))


def near_tiles(ref, start, rows):
    mid = [ref[t, pl.ds(start, rows), :] for t in range(LT + 1)]
    low = [pltpu.roll(m, 1, 1) for m in mid]
    high = [pltpu.roll(m, L - 1, 1) for m in mid]
    lane = iota((rows, L), 1)
    near = []
    for t in range(LT + 1):
        rows_sum = ref[t, pl.ds(start - 1, rows), :] + ref[t, pl.ds(start + 1, rows), :]
        left = jnp.where(lane == 0, low[t - 1], low[t])
        right = jnp.where(lane == L - 1, high[(t + 1) % (LT + 1)], high[t])
        near.append(rows_sum + (left + right))
    return mid, near


def fold(p):
    return (p[:, 0:128] + p[:, 128:256]) + (p[:, 256:384] + p[:, 384:512])


def moments(z, w, n1, n2, dn3, inv):
    d = 1.0 / inv
    dz, dw, dn1, dn2 = d * z, d * w, d * n1, d * n2
    return dz * z, dz * w, dw * w, dw * n1, dn1 * n1, dn1 * n2, dn2 * n2, n2 * dn3


def basis_kernel(pos, z, invd, col_1, col_2, hist, acc_o, ie, ze, we, n1e, n2e, sem):
    zc, ic = halo_columns(pos, *from_pairs(pos, 1, col_1[:, :T], col_2[:, :T]))
    zero = jnp.zeros((OFF, L), F32)
    own = pl.ds(OFF, T)
    for e in (ie, ze, we, n1e, n2e):
        for t in range(LT + 1):
            e[t, 0:OFF, :] = zero
            e[t, OFF + T :, :] = zero
    for t in range(LT):
        ze[t, own, :] = z[:, lanes(t)]
        ie[t, own, :] = invd[:, lanes(t)]
    ze[LT, own, :] = zc
    ie[LT, own, :] = ic
    rows = 128

    def save(k, e):
        copy = pltpu.make_async_copy(e.at[pl.ds(0, LT), own, :], hist.at[k], sem.at[k])
        copy.start()
        return copy

    def apply_to(src, dst, minus):
        def step(i, carry):
            start = pl.multiple_of(OFF + i * rows, 8)
            mid, near = near_tiles(src, start, rows)
            for t in range(LT + 1):
                y = near[t] * ie[t, pl.ds(start, rows), :]
                dst[t, pl.ds(start, rows), :] = mid[t] - y if minus else y
            return carry

        lax.fori_loop(0, T // rows, step, 0)

    copies = [save(0, ze)]
    apply_to(ze, we, True)
    copies.append(save(1, we))
    apply_to(we, n1e, False)
    copies.append(save(2, n1e))
    apply_to(n1e, n2e, False)
    copies.append(save(3, n2e))

    acc = [jnp.zeros((8, L), F32) for _ in range(SUMS)]
    ends = list(range(0, T + 1, 64))
    ends[0], ends[-1] = 8, T - 8
    for low, high in zip(ends[:-1], ends[1:]):
        start, rows = OFF + low, high - low
        n2, dn3 = near_tiles(n2e, start, rows)
        for t in range(LT):
            z8, w8, n18, i8 = (e[t, pl.ds(start, rows), :] for e in (ze, we, n1e, ie))
            for k, p in enumerate(moments(z8, w8, n18, n2[t], dn3[t], i8)):
                for q in range(0, rows, 8):
                    acc[k] = acc[k] + p[q : q + 8]
    for k in range(SUMS):
        acc_o[8 * k : 8 * k + 8, :] = acc[k]
    for copy in copies:
        copy.wait()


def gram_terms(acc):
    g0, q0 = acc[0], acc[1]
    m = acc[2:]
    r = [q0, q0 - m[0], q0 - m[0] - m[1]]
    h = {(0, 0): q0, **{(0, j): RHO[0] * m[j - 1] for j in (1, 2, 3)}}
    b = [g0] + r
    for k in range(3):
        h[0, 0] = h[0, 0] - Q[k] * m[k]
        b[0] = b[0] - Q[k] * r[k]
    for k in range(6):
        f = sum(Q[j] * RHO[k - j] for j in range(3) if 0 <= k - j < 4)
        h[0, 0] = h[0, 0] - f * m[k]
    for j in (1, 2, 3):
        for k in (1, 2, 3):
            h[0, j] = h[0, j] + RHO[k] * m[j - 1 + k]
            if j <= k:
                h[j, k] = m[j + k - 2] - m[j + k - 1]
    out = []
    for p in range(4):
        out += [h[p, q] for q in range(p, 4)] + [b[p]]
    return out


def rim_kernel(pos, z, invd, corners, row_1, row_2, acc_i, rims, part):
    sub = iota((8, W), 0)
    ours = at(pos, 0, sub)
    above, below = (sub >= 4) & (ours > 0), (sub < 4) & (ours < 7)
    top, bot = from_pairs(pos, 0, row_1[:, :W], row_2[:, :W])
    acc = [acc_i[8 * k : 8 * k + 8, :] for k in range(SUMS)]
    for end in (0, 1):
        rows = slice(0, 16) if end == 0 else slice(T - 16, T)
        zc, ic = corners[16 * end : 16 * end + 16, :], corners[32 + 16 * end : 48 + 16 * end, :]
        z16 = jnp.concatenate([z[rows, :], zc], axis=1)
        i16 = jnp.concatenate([invd[rows, :], ic], axis=1)
        if end == 0:
            zb = jnp.concatenate([jnp.where(above, pltpu.roll(top, 4, 0), 0.0), z16], axis=0)
            ib = jnp.concatenate([jnp.where(above, top, 0.0), i16], axis=0)
            own = slice(8, 16)
        else:
            zb = jnp.concatenate([z16, jnp.where(below, bot, 0.0)], axis=0)
            ib = jnp.concatenate([i16, jnp.where(below, pltpu.roll(bot, 4, 0), 0.0)], axis=0)
            own = slice(8, 16)
        w = zb - ib * beside(zb)
        n1 = ib * beside(w)
        n2 = ib * beside(n1)
        near = beside(n2)
        zo, wo, n1o, n2o, dn3, io = (x[own, :T] for x in (zb, w, n1, n2, near, ib))
        for k, p in enumerate(moments(zo, wo, n1o, n2o, dn3, io)):
            acc[k] = acc[k] + fold(p)
        for k, x in enumerate((wo, n1o, n2o)):
            rims[16 * k + 8 * end : 16 * k + 8 * end + 8, :] = x
    terms = gram_terms(acc)
    rows14 = jnp.concatenate(
        [jnp.sum(a, axis=0, keepdims=True) for a in terms] + [jnp.zeros((2, L), F32)], axis=0
    )
    a, rest = hi_lo(rows14)
    b, c = hi_lo(rest)
    parts = jnp.concatenate([c, b, a], axis=0).astype(BF16)
    sums = nt(jnp.ones((8, L), BF16), parts)
    sums = sums[:, 0:16] + sums[:, 16:32] + sums[:, 32:48]
    sums = jnp.concatenate([sums, jnp.zeros((8, L - 16), F32)], axis=1)
    part[...] = sums


def gather_kernel(hist, table, rims, wt, g_o, x_s, slab, slots, sem):
    copies = [pltpu.make_async_copy(hist.at[k], x_s.at[k], sem.at[k]) for k in range(4)]
    ready = pltpu.make_async_copy(table, slots, sem.at[4])
    ready.start()
    for copy in copies:
        copy.start()
    for k in range(4):
        copies[k].wait()
        if k:
            for t in range(LT):
                x_s[k, t, 0:8, :] = rims[16 * k - 16 : 16 * k - 8, lanes(t)]
                x_s[k, t, T - 8 :, :] = rims[16 * k - 8 : 16 * k, lanes(t)]

        def lay(i, carry):
            for b in range(4):
                for t in range(LT):
                    start = pl.multiple_of(i * 32 + 8 * b, 8)
                    to = (i * 32 + 8 * b) * SLAB + 4 * t + k
                    slab[pl.ds(to, 8, stride=SLAB), :] = x_s[k, t, pl.ds(start, 8), :]
            return carry

        lax.fori_loop(0, T // 32, lay, 0)
    lane, sub = iota((8, L), 1), iota((8, L), 0)
    ready.wait()
    for o in range(NO):
        acc = jnp.zeros((8, L), F32)
        for j in range(L):
            x = slab[pl.ds(slots[o, j], 8), :]
            acc = jnp.where(lane == j, pltpu.roll(x, slots[NO + o, j], 1), acc)
        g_o[8 * o : 8 * o + 8, :] = jnp.where(sub < 4, acc * wt[o : o + 1, :], 0.0)


def pack_kernel(g, rows, out):
    out[...] = g[...]
    total = jnp.sum(rows[...], axis=0, keepdims=True)
    for o in range(NO):
        out[8 * o + 4 : 8 * o + 5, :] = total


def solve(tot):
    lane = iota((1, L), 1)

    def pick(k):
        return jnp.sum(jnp.where(lane == k, tot, 0.0), axis=1, keepdims=True)

    h, b = {}, []
    k = 0
    for p in range(4):
        for q in range(p, 4):
            h[p, q] = pick(k)
            k += 1
        b.append(pick(k))
        k += 1
    floor = [3e-7 * h[p, p] for p in range(4)]
    inv = []
    for p in range(4):
        inv.append(jnp.where(h[p, p] > floor[p], 1.0 / h[p, p], 0.0))
        for q in range(p + 1, 4):
            f = h[p, q] * inv[p]
            for r in range(q, 4):
                h[q, r] = h[q, r] - f * h[p, r]
            b[q] = b[q] - f * b[p]
    c = [None] * 4
    for p in (3, 2, 1, 0):
        s = b[p]
        for q in range(p + 1, 4):
            s = s - h[p, q] * c[q]
        c[p] = s * inv[p]
    return [c[0]] + [c[k + 1] - Q[k] * c[0] for k in range(3)]


def combine_kernel(hist, ahead, coef, rims, out, h_s, x_s, sem_in, sem_out):
    n = T // STEPS
    load = [
        pltpu.make_async_copy(
            hist.at[pl.ds(1, 3), :, pl.ds(i * n, n), :], h_s.at[i], sem_in.at[i]
        )
        for i in range(STEPS)
    ]
    save = [
        pltpu.make_async_copy(x_s.at[pl.ds(i * n, n), :], out.at[pl.ds(i * n, n), :], sem_out.at[i])
        for i in range(STEPS)
    ]
    for copy in load:
        copy.start()
    c = [coef[k : k + 1, 0:1] for k in range(4)]
    for i in range(STEPS):
        load[i].wait()
        for t in range(LT):
            h = [ahead[0, t, i * n : (i + 1) * n, :]] + [h_s[i, k, t] for k in range(3)]
            x_s[i * n : (i + 1) * n, lanes(t)] = (c[0] * h[0] + c[1] * h[1]) + (
                c[2] * h[2] + c[3] * h[3]
            )
        for end, step, low in ((0, 0, 0), (1, STEPS - 1, n - 8)):
            if i == step:
                for t in range(LT):
                    x = c[0] * ahead[0, t, i * n + low : i * n + low + 8, :]
                    for k in range(3):
                        x += c[k + 1] * rims[16 * k + 8 * end : 16 * k + 8 * end + 8, lanes(t)]
                    x_s[i * n + low : i * n + low + 8, lanes(t)] = x
        save[i].start()
    for copy in save:
        copy.wait()


def coarse_neighbours(pos, u, row_1, row_2, col_1, col_2):
    above, below = from_pairs(pos, 0, row_1, row_2)
    above, below = above[7:8, :], below[0:1, :]
    from_l, from_r = from_pairs(pos, 1, col_1, col_2)
    above = jnp.where(at(pos, 0, above) > 0, above, 0.0)
    below = jnp.where(at(pos, 0, below) < 7, below, 0.0)
    r, lane = iota((CB, CB), 0), iota((CB, CB), 1)
    g, gl = iota((8, CB), 0), iota((8, CB), 1)
    turned_l = jnp.where(g == 0, 0.0, pltpu.roll(from_l, 1, 0))
    turned_r = jnp.where(g == 7, 0.0, pltpu.roll(from_r, 7, 0))
    place = at(pos, 1, from_l)
    from_l = jnp.where(place == 0, turned_l, from_l)
    from_r = jnp.where(place == NO - 1, turned_r, from_r)
    seam_l = tn(from_l, jnp.where(gl == g * GROUP, 1.0, 0.0), HI)
    seam_r = tn(from_r, jnp.where(gl == g * GROUP + GROUP - 1, 1.0, 0.0), HI)
    near = jnp.where(r == 0, above, pltpu.roll(u, 1, 0))
    near += jnp.where(r == CB - 1, below, pltpu.roll(u, CB - 1, 0))
    near += jnp.where(lane % GROUP == 0, seam_l, pltpu.roll(u, 1, 1))
    near += jnp.where(lane % GROUP == GROUP - 1, seam_r, pltpu.roll(u, CB - 1, 1))
    return near


def base_kernel(
    hist, pos, held, volt, cleak, col_1, col_2, row_1, row_2,
    cdiag, scale, base, r_o, c_o, ahead, sem,
):
    copy = pltpu.make_async_copy(hist.at[pl.ds(0, 1)], ahead, sem.at[0])
    copy.start()
    for o in range(NO):
        h = held[o : o + 1, :]
        r_o[:, lanes(o)] = onehot(h >> 7, CB)
        c_o[:, lanes(o)] = onehot(h & (CB - 1), CB)
    count = nt(r_o[...], c_o[...])
    diag = 4.0 * coarse_conductance + cleak[...] + via_conductance * count
    u = volt[...]
    near = coarse_neighbours(pos, u, row_1[:, W:], row_2[:, W:], col_1[:, T:], col_2[:, T:])
    cdiag[...] = diag
    scale[...] = relaxation / diag
    base[...] = u - relaxation * (diag * u - coarse_conductance * near) / diag
    copy.wait()


def sweep1_kernel(pos, arrived, scale, base, r, c, coef, u_o, src_o, c1, c2, r1, r2, v_s):
    tot = arrived[4:5, :]
    for o in range(1, NO):
        tot += arrived[8 * o + 4 : 8 * o + 5, :]
    d = solve(tot)
    sub = iota((8, L), 0)
    cf = jnp.zeros((8, L), F32)
    for k in range(4):
        cf = jnp.where(sub == k, d[k], cf)
    coef[...] = cf
    for o in range(NO):
        v = jnp.sum(arrived[8 * o : 8 * o + 8, :] * cf, axis=0, keepdims=True)
        hi, lo = hi_lo(v)
        on = c[:, lanes(o)]
        v_s[:, lanes(o)] = on * hi.astype(BF16)
        v_s[:, lanes(NO + o)] = on * lo.astype(BF16)
    src = nt(r[...], v_s[:, : NO * L]) + nt(r[...], v_s[:, NO * L :])
    u = base[...] + scale[...] * src
    u_o[...] = u
    src_o[...] = src
    g, gl = iota((8, CB), 0), iota((8, CB), 1)
    to_l = nt(jnp.where(gl == g * GROUP, 1.0, 0.0), u, HI)
    to_r = nt(jnp.where(gl == g * GROUP + GROUP - 1, 1.0, 0.0), u, HI)
    c1[...], c2[...] = pair_order(pos, 1, to_l, to_r)
    r1[...], r2[...] = pair_order(pos, 0, u[0:8, :], u[CB - 8 :, :])


def sweep2_kernel(pos, u, src, cdiag, scale, col_1, col_2, row_1, row_2, u_o):
    near = coarse_neighbours(pos, u[...], row_1[...], row_2[...], col_1[...], col_2[...])
    u_o[...] = u[...] + scale[...] * (src[...] - (cdiag[...] * u[...] - coarse_conductance * near))


VM = pl.BlockSpec(memory_space=pltpu.VMEM)
ANY = pl.BlockSpec(memory_space=pltpu.HBM)
vmem = pltpu.MemorySpace.VMEM
hbm = jax.ShapeDtypeStruct


def keep(*args):
    return [pltpu.with_memory_space_constraint(x, pltpu.VMEM) for x in args]


def leave(*args):
    return [pltpu.with_memory_space_constraint(x, pltpu.HBM) for x in args]


def call(body, outs, args, scratch=(), flops=0, any_in=0, any_out=0):
    specs = [ANY] * any_in + [VM] * (len(args) - any_in)
    return pl.pallas_call(
        body,
        out_shape=outs,
        in_specs=specs,
        out_specs=[ANY] * any_out + [VM] * (len(outs) - any_out),
        scratch_shapes=list(scratch),
        cost_estimate=pl.CostEstimate(flops=flops, bytes_accessed=0, transcendentals=0),
        compiler_params=pltpu.CompilerParams(vmem_limit_bytes=20 * 2**20),
    )(*args)


def exchange(axis, first, second):
    n = lax.axis_size(axis)
    near = [(i, i ^ 1) for i in range(n)]
    far = [(i, ((i + 1) ^ 1) - 1 & (n - 1)) for i in range(n)]
    return lax.ppermute(first, axis, near), lax.ppermute(second, axis, far)


def spread(x, axis=COL):
    return lax.all_to_all(x, axis, split_axis=0, concat_axis=0, tiled=True)


def per_device(load_amp, load_mask, leak, coarse_leak, coarse_init, via_fine, via_coarse, via_count):
    pos = jnp.where(
        lax.broadcasted_iota(jnp.int32, (8, W + CB), 0) == 0, lax.axis_index(ROW), lax.axis_index(COL)
    ).astype(jnp.int32)
    live = jnp.arange(L, dtype=jnp.int32)[None, :] < via_count.reshape(NO, 1)
    wt = jnp.where(live, via_conductance, 0.0).astype(F32)
    fine = via_fine.reshape(NO, L)
    coarse = via_coarse.reshape(NO, L)
    request = jnp.where(live, ((coarse >> 11) << 7) | (coarse & (CB - 1)), -1)
    held = spread(request)

    tile, block, slots = vmem((T, T), F32), vmem((CB, CB), F32), vmem((NO, L), F32)
    hot, chot = vmem((T, NO * L), BF16), vmem((CB, NO * L), BF16)
    hots = vmem((T, 2 * NO * L), BF16)
    rim16, side, seam = vmem((16, T), F32), vmem((8, W), F32), vmem((8, CB), F32)
    ext, packed = vmem((LT + 1, EXT, L), F32), ((L, L), F32)
    dmas = pltpu.SemaphoreType.DMA((4,))
    big = 20_000_000_000

    drops, where, volt, fine = call(
        parts_kernel,
        [vmem((3 * CB, CB), BF16), hbm((2 * NO, L), jnp.int32), block, vmem((NO, L), jnp.int32)],
        leave(coarse_init, fine),
    )
    zl, invd, strips, irims = call(
        diag_kernel, [tile, tile, rim16, rim16],
        leave(load_amp, load_mask, leak) + keep(fine, wt),
        [hot, hot, tile, vmem((T, T), jnp.int32), tile, dmas], flops=big, any_in=3,
    )
    looked = call(lookup_kernel, [slots], keep(held, drops))[0]
    at_via = spread(looked)
    a, send_1, send_2 = call(
        strips_kernel, [hot, side, side], keep(pos, fine, wt, at_via, strips, volt)    )
    col_1, col_2 = exchange(COL, send_1, send_2)
    z, zrims = call(
        rhs_kernel, [tile, rim16], keep(fine, wt, at_via, zl, invd, a), [hots], flops=big
    )
    rim = vmem((8, W + CB), F32)
    send_1, send_2, corners = call(
        edge_kernel, [rim, rim, vmem((64, L), F32)],
        keep(pos, zrims, irims, col_1, col_2, volt)    )
    row_1, row_2 = exchange(ROW, send_1, send_2)
    hist, acc = call(
        basis_kernel, [pltpu.MemorySpace.HBM((4, LT, T, L), F32), vmem((8 * SUMS, L), F32)], keep(pos, z, invd, col_1, col_2),
        [ext] * 5 + [dmas], flops=big, any_out=1,
    )
    rims, part = call(
        rim_kernel, [vmem((48, T), F32), vmem((8, L), F32)],
        keep(pos, z, invd, corners, row_1, row_2, acc)    )
    rows = spread(part, ROW)
    g = call(
        gather_kernel, [vmem(*packed)], leave(hist, where) + keep(rims, wt),
        [vmem((4, LT, T, L), F32), vmem((T * SLAB + 8, L), F32),
         pltpu.MemorySpace.SMEM((2 * NO, L), jnp.int32), pltpu.SemaphoreType.DMA((5,))],
        flops=big, any_in=2,
    )[0]
    arrived = spread(call(pack_kernel, [vmem(*packed)], keep(g, rows))[0])
    cdiag, scale, base, r_hot, c_hot, ahead = call(
        base_kernel, [block, block, block, chot, chot, vmem((1, LT, T, L), F32)],
        leave(hist) + keep(pos, held, volt, coarse_leak, col_1, col_2, row_1, row_2),
        [dmas], flops=big, any_in=1,
    )
    coef, u, src, c1, c2, r1, r2 = call(
        sweep1_kernel, [seam, block, block, seam, seam, seam, seam],
        keep(pos, arrived, scale, base, r_hot, c_hot), [vmem((CB, 2 * NO * L), BF16)]    )
    c1, c2 = exchange(COL, c1, c2)
    r1, r2 = exchange(ROW, r1, r2)
    fine_drop = call(
        combine_kernel, [pltpu.MemorySpace.HBM((T, T), F32)], leave(hist) + keep(ahead, coef, rims),
        [vmem((STEPS, 3, LT, T // STEPS, L), F32), tile, pltpu.SemaphoreType.DMA((STEPS,)),
         pltpu.SemaphoreType.DMA((STEPS,))], flops=big // 4, any_in=1, any_out=1,
    )[0]
    coarse_drop = call(
        sweep2_kernel, [hbm((CB, CB), F32)], keep(pos, u, src, cdiag, scale, c1, c2, r1, r2)    )[0]
    return fine_drop, coarse_drop


def solution(mesh):
    spec = P(ROW, COL)

    return jax.shard_map(
        per_device, mesh=mesh, in_specs=(spec,) * 8, out_specs=(spec, spec), check_vma=False
    )
```

```python
import jax
import jax.numpy as jnp
from jax import lax
from jax.experimental import pallas as pl
from jax.experimental.pallas import tpu as pltpu
from jax.sharding import PartitionSpec as P


F32 = jnp.float32
BF16 = jnp.bfloat16
HI = lax.Precision.HIGHEST
ROW, COL = "row", "col"

GROUP = 16
via_conductance = 2.0
coarse_conductance = 4.0
relaxation = 0.8

T = 512
CB = 128
NO = 16
L = 128
OFF = 16
EXT = OFF + T + 16
W = T + L

Q = (1.09375, 1.765625, 1.28125)
RHO = (1.0 - Q[0], Q[0] - Q[1], Q[1] - Q[2], Q[2])
LT = T // L
SLAB = 4 * LT + 1
SUMS = 8
STEPS = 8


def iota(shape, dim):
    return lax.broadcasted_iota(jnp.int32, shape, dim)


def nt(a, b, precision=None):
    return lax.dot_general(
        a, b, (((1,), (1,)), ((), ())), precision=precision, preferred_element_type=F32
    )


def tn(a, b, precision=None):
    return lax.dot_general(
        a, b, (((0,), (0,)), ((), ())), precision=precision, preferred_element_type=F32
    )


def onehot(idx, n):
    return jnp.where(iota((n, idx.shape[1]), 0) == idx, 1.0, 0.0).astype(BF16)


def hi_lo(x):
    hi = x.astype(BF16).astype(F32)
    return hi, x - hi


def lanes(o):
    return slice(o * L, (o + 1) * L)


def at(pos, k, like):
    return jnp.broadcast_to(pos[k : k + 1, : like.shape[1]], like.shape)


def pair_order(pos, k, low, high):
    even = (at(pos, k, low) & 1) == 0
    return jnp.where(even, high, low), jnp.where(even, low, high)


def from_pairs(pos, k, first, second):
    even = (at(pos, k, first) & 1) == 0
    return jnp.where(even, second, first), jnp.where(even, first, second)


def diag_kernel(
    amp, mask, leak, via, zl, invd, strips, rims, amp_s, mask_s, leak_s, via_s, sem
):
    copies = [
        pltpu.make_async_copy(x, y, sem.at[k])
        for k, (x, y) in enumerate(
            ((leak, leak_s), (via, via_s), (amp, amp_s), (mask, mask_s))
        )
    ]
    for copy in copies:
        copy.start()
    for copy in copies:
        copy.wait()
    inv = 1.0 / (4.0 + leak_s[...] + via_s[...])
    z = amp_s[...] * mask_s[...].astype(F32) * inv
    zl[...] = z
    invd[...] = inv
    j, lane = iota((8, 2 * L), 0), iota((8, 2 * L), 1)
    pick = jnp.where(lane == jnp.where(j < 4, j, 2 * L - 8 + j), 1.0, 0.0).astype(BF16)
    for k, x in enumerate((z, inv)):
        hi, rest = hi_lo(jnp.concatenate([x[:, :L], x[:, T - L :]], axis=1))
        mid, lo = hi_lo(rest)
        strips[8 * k : 8 * k + 8, :] = (
            nt(pick, lo.astype(BF16)) + nt(pick, mid.astype(BF16)) + nt(pick, hi.astype(BF16))
        )
    rims[0:8, :] = inv[0:8]
    rims[8:16, :] = inv[T - 8 :]


def parts_kernel(volt, vf, wt, pos, parts, slots, volt_o, vf_o, seams, round_o, via, a_s, b_s):
    u = volt[...]
    f = vf[...]
    volt_o[...] = u
    vf_o[...] = f
    slots[0:NO, :] = (f >> 9) * SLAB + ((f >> 7) & 3) * 4
    slots[NO:, :] = (iota((NO, L), 1) - f) & (L - 1)
    v1, rest = hi_lo(u.T)
    v2, v3 = hi_lo(rest)
    parts[...] = jnp.concatenate([v3, v2, v1], axis=0).astype(BF16)
    g, lane = iota((8, CB), 0), iota((8, CB), 1)
    to_l = nt(jnp.where(lane == g * GROUP, 1.0, 0.0), u, HI)
    to_r = nt(jnp.where(lane == g * GROUP + GROUP - 1, 1.0, 0.0), u, HI)
    seams[0:8, :] = to_l
    seams[8:16, :] = to_r
    round_o[...] = jnp.where(at(pos, 1, to_l) == 0, to_l, to_r)
    for o in range(NO):
        f = vf[o : o + 1, :]
        a_s[:, lanes(o)] = onehot(f // T, T)
        b_s[:, lanes(o)] = jnp.where(iota((T, L), 0) == f % T, wt[o : o + 1, :], 0.0).astype(BF16)
    via[...] = nt(a_s[...], b_s[...])


def lookup_kernel(held, parts, looked):
    v = parts[...]
    for i in range(NO // 2):
        h = jnp.concatenate([held[2 * i : 2 * i + 1, :], held[2 * i + 1 : 2 * i + 2, :]], axis=1)
        y = jnp.dot(v, onehot(h >> 7, CB), preferred_element_type=F32)
        y = y[:CB] + y[CB : 2 * CB] + y[2 * CB :]
        y = jnp.where(iota((CB, 2 * L), 0) == (h & (CB - 1)), y, 0.0)
        y = jnp.sum(y, axis=0, keepdims=True)
        looked[2 * i : 2 * i + 1, :] = y[:, :L]
        looked[2 * i + 1 : 2 * i + 2, :] = y[:, L:]


def strips_kernel(pos, vf, wt, at_via, strips, seams, a_o, send_1, send_2):
    j = iota((8, L), 0)
    colid = jnp.where(j < 4, j, T - 8 + j)
    hs, ls = [], []
    for o in range(NO):
        f = vf[o : o + 1, :]
        a_o[:, lanes(o)] = onehot(f // T, T)
        hi, lo = hi_lo(at_via[o : o + 1, :] * wt[o : o + 1, :])
        on = colid == f % T
        hs.append(jnp.where(on, hi, 0.0))
        ls.append(jnp.where(on, lo, 0.0))
    lhs = jnp.concatenate(
        [jnp.concatenate(hs, axis=1), jnp.concatenate(ls, axis=1)], axis=0
    ).astype(BF16)
    inj = nt(lhs, a_o[...])
    inv = strips[8:16, :]
    z = strips[0:8, :] + (inj[0:8] + inj[8:16]) * inv
    low = iota((8, T), 0) < 4
    to_l = jnp.where(low, z, pltpu.roll(inv, 4, 0))
    to_r = jnp.where(low, pltpu.roll(z, 4, 0), inv)
    send_1[:, :T], send_2[:, :T] = pair_order(pos, 1, to_l, to_r)
    send_1[:, T:], send_2[:, T:] = pair_order(pos, 1, seams[0:8, :], seams[8:16, :])


def rhs_kernel(vf, wt, at_via, zl, invd, a, z, rims, b_s):
    for o in range(NO):
        hi, lo = hi_lo(at_via[o : o + 1, :] * wt[o : o + 1, :])
        on = iota((T, L), 0) == vf[o : o + 1, :] % T
        b_s[:, lanes(o)] = jnp.where(on, hi, 0.0).astype(BF16)
        b_s[:, lanes(NO + o)] = jnp.where(on, lo, 0.0).astype(BF16)
    inj = nt(a[...], b_s[:, : NO * L]) + nt(a[...], b_s[:, NO * L :])
    zz = zl[...] + inj * invd[...]
    z[...] = zz
    rims[0:8, :] = zz[0:8]
    rims[8:16, :] = zz[T - 8 :]


def halo_columns(pos, gl, gr):
    place = at(pos, 1, gl)
    parts = []
    for x in (jnp.where(place < NO - 1, gr, 0.0), jnp.where(place > 0, gl, 0.0)):
        a, rest = hi_lo(x)
        b, c = hi_lo(rest)
        parts += [c, b, a]
    j, lane = iota((8, 2 * L), 0), iota((8, 2 * L), 1)
    to_r = jnp.where(lane == jnp.where(j < 4, j, L + j - 4), 1.0, 0.0)
    to_l = jnp.where(lane == jnp.where(j < 4, 124 + j, L + 120 + j), 1.0, 0.0)
    place = jnp.concatenate([to_r] * 3 + [to_l] * 3, axis=0)
    out = tn(jnp.concatenate(parts, axis=0).astype(BF16), place.astype(BF16))
    return out[:, :L], out[:, L:]


def edge_kernel(pos, zr, ir, col_1, col_2, volt, send_1, send_2, corners):
    got_l, got_r = from_pairs(pos, 1, col_1[...], col_2[...])
    zt, it = halo_columns(pos, got_l[:, :L], got_r[:, :L])
    zb, ib = halo_columns(pos, got_l[:, T - L : T], got_r[:, T - L : T])
    for k, x in enumerate((zt[0:16], zb[L - 16 :], it[0:16], ib[L - 16 :])):
        corners[16 * k : 16 * k + 16, :] = x
    low = iota((8, W), 0) < 4
    zt = jnp.concatenate([zr[0:8, :], zt[0:8]], axis=1)
    it = jnp.concatenate([ir[0:8, :], it[0:8]], axis=1)
    zb = jnp.concatenate([zr[8:16, :], zb[L - 8 :]], axis=1)
    ib = jnp.concatenate([ir[8:16, :], ib[L - 8 :]], axis=1)
    to_u = jnp.where(low, zt, pltpu.roll(it, 4, 0))
    to_d = jnp.where(low, pltpu.roll(zb, 4, 0), ib)
    send_1[:, :W], send_2[:, :W] = pair_order(pos, 0, to_u, to_d)
    send_1[:, W:], send_2[:, W:] = pair_order(pos, 0, volt[0:8, :], volt[CB - 8 :, :])


def beside(block):
    n = block.shape[0]
    rows = pltpu.roll(block, 1, 0) + pltpu.roll(block, n - 1, 0)
    return rows + (pltpu.roll(block, 1, 1) + pltpu.roll(block, W - 1, 1))


def near_tiles(ref, start, rows):
    mid = [ref[t, pl.ds(start, rows), :] for t in range(LT + 1)]
    low = [pltpu.roll(m, 1, 1) for m in mid]
    high = [pltpu.roll(m, L - 1, 1) for m in mid]
    lane = iota((rows, L), 1)
    near = []
    for t in range(LT + 1):
        rows_sum = ref[t, pl.ds(start - 1, rows), :] + ref[t, pl.ds(start + 1, rows), :]
        left = jnp.where(lane == 0, low[t - 1], low[t])
        right = jnp.where(lane == L - 1, high[(t + 1) % (LT + 1)], high[t])
        near.append(rows_sum + (left + right))
    return mid, near


def fold(p):
    return (p[:, 0:128] + p[:, 128:256]) + (p[:, 256:384] + p[:, 384:512])


def moments(z, w, n1, n2, dn3, inv):
    d = 1.0 / inv
    dz, dw, dn1, dn2 = d * z, d * w, d * n1, d * n2
    return dz * z, dz * w, dw * w, dw * n1, dn1 * n1, dn1 * n2, dn2 * n2, n2 * dn3


def basis_kernel(pos, z, invd, col_1, col_2, hist, acc_o, ie, ze, we, n1e, n2e, sem):
    zc, ic = halo_columns(pos, *from_pairs(pos, 1, col_1[:, :T], col_2[:, :T]))
    zero = jnp.zeros((OFF, L), F32)
    own = pl.ds(OFF, T)
    for e in (ie, ze, we, n1e, n2e):
        for t in range(LT + 1):
            e[t, 0:OFF, :] = zero
            e[t, OFF + T :, :] = zero
    for t in range(LT):
        ze[t, own, :] = z[:, lanes(t)]
        ie[t, own, :] = invd[:, lanes(t)]
    ze[LT, own, :] = zc
    ie[LT, own, :] = ic
    rows = 128

    def save(k, e):
        copy = pltpu.make_async_copy(e.at[pl.ds(0, LT), own, :], hist.at[k], sem.at[k])
        copy.start()
        return copy

    def apply_to(src, dst, minus):
        def step(i, carry):
            start = pl.multiple_of(OFF + i * rows, 8)
            mid, near = near_tiles(src, start, rows)
            for t in range(LT + 1):
                y = near[t] * ie[t, pl.ds(start, rows), :]
                dst[t, pl.ds(start, rows), :] = mid[t] - y if minus else y
            return carry

        lax.fori_loop(0, T // rows, step, 0)

    copies = [save(0, ze)]
    apply_to(ze, we, True)
    copies.append(save(1, we))
    apply_to(we, n1e, False)
    copies.append(save(2, n1e))
    apply_to(n1e, n2e, False)
    copies.append(save(3, n2e))

    acc = [jnp.zeros((8, L), F32) for _ in range(SUMS)]
    ends = list(range(0, T + 1, 64))
    ends[0], ends[-1] = 8, T - 8
    for low, high in zip(ends[:-1], ends[1:]):
        start, rows = OFF + low, high - low
        n2, dn3 = near_tiles(n2e, start, rows)
        for t in range(LT):
            z8, w8, n18, i8 = (e[t, pl.ds(start, rows), :] for e in (ze, we, n1e, ie))
            for k, p in enumerate(moments(z8, w8, n18, n2[t], dn3[t], i8)):
                for q in range(0, rows, 8):
                    acc[k] = acc[k] + p[q : q + 8]
    for k in range(SUMS):
        acc_o[8 * k : 8 * k + 8, :] = acc[k]
    for copy in copies:
        copy.wait()


def gram_terms(acc):
    g0, q0 = acc[0], acc[1]
    m = acc[2:]
    r = [q0, q0 - m[0], q0 - m[0] - m[1]]
    h = {(0, 0): q0, **{(0, j): RHO[0] * m[j - 1] for j in (1, 2, 3)}}
    b = [g0] + r
    for k in range(3):
        h[0, 0] = h[0, 0] - Q[k] * m[k]
        b[0] = b[0] - Q[k] * r[k]
    for k in range(6):
        f = sum(Q[j] * RHO[k - j] for j in range(3) if 0 <= k - j < 4)
        h[0, 0] = h[0, 0] - f * m[k]
    for j in (1, 2, 3):
        for k in (1, 2, 3):
            h[0, j] = h[0, j] + RHO[k] * m[j - 1 + k]
            if j <= k:
                h[j, k] = m[j + k - 2] - m[j + k - 1]
    out = []
    for p in range(4):
        out += [h[p, q] for q in range(p, 4)] + [b[p]]
    return out


def rim_kernel(pos, z, invd, corners, row_1, row_2, acc_i, rims, part):
    sub = iota((8, W), 0)
    ours = at(pos, 0, sub)
    above, below = (sub >= 4) & (ours > 0), (sub < 4) & (ours < 7)
    top, bot = from_pairs(pos, 0, row_1[:, :W], row_2[:, :W])
    acc = [acc_i[8 * k : 8 * k + 8, :] for k in range(SUMS)]
    for end in (0, 1):
        rows = slice(0, 16) if end == 0 else slice(T - 16, T)
        zc, ic = corners[16 * end : 16 * end + 16, :], corners[32 + 16 * end : 48 + 16 * end, :]
        z16 = jnp.concatenate([z[rows, :], zc], axis=1)
        i16 = jnp.concatenate([invd[rows, :], ic], axis=1)
        if end == 0:
            zb = jnp.concatenate([jnp.where(above, pltpu.roll(top, 4, 0), 0.0), z16], axis=0)
            ib = jnp.concatenate([jnp.where(above, top, 0.0), i16], axis=0)
            own = slice(8, 16)
        else:
            zb = jnp.concatenate([z16, jnp.where(below, bot, 0.0)], axis=0)
            ib = jnp.concatenate([i16, jnp.where(below, pltpu.roll(bot, 4, 0), 0.0)], axis=0)
            own = slice(8, 16)
        w = zb - ib * beside(zb)
        n1 = ib * beside(w)
        n2 = ib * beside(n1)
        near = beside(n2)
        zo, wo, n1o, n2o, dn3, io = (x[own, :T] for x in (zb, w, n1, n2, near, ib))
        for k, p in enumerate(moments(zo, wo, n1o, n2o, dn3, io)):
            acc[k] = acc[k] + fold(p)
        for k, x in enumerate((wo, n1o, n2o)):
            rims[16 * k + 8 * end : 16 * k + 8 * end + 8, :] = x
    terms = gram_terms(acc)
    rows14 = jnp.concatenate(
        [jnp.sum(a, axis=0, keepdims=True) for a in terms] + [jnp.zeros((2, L), F32)], axis=0
    )
    a, rest = hi_lo(rows14)
    b, c = hi_lo(rest)
    parts = jnp.concatenate([c, b, a], axis=0).astype(BF16)
    sums = nt(jnp.ones((8, L), BF16), parts)
    sums = sums[:, 0:16] + sums[:, 16:32] + sums[:, 32:48]
    sums = jnp.concatenate([sums, jnp.zeros((8, L - 16), F32)], axis=1)
    part[...] = sums


def gather_kernel(hist, table, rims, wt, g_o, x_s, slab, slots, sem):
    copies = [pltpu.make_async_copy(hist.at[k], x_s.at[k], sem.at[k]) for k in range(4)]
    ready = pltpu.make_async_copy(table, slots, sem.at[4])
    ready.start()
    for copy in copies:
        copy.start()
    for k in range(4):
        copies[k].wait()
        if k:
            for t in range(LT):
                x_s[k, t, 0:8, :] = rims[16 * k - 16 : 16 * k - 8, lanes(t)]
                x_s[k, t, T - 8 :, :] = rims[16 * k - 8 : 16 * k, lanes(t)]

        def lay(i, carry):
            for b in range(4):
                for t in range(LT):
                    start = pl.multiple_of(i * 32 + 8 * b, 8)
                    to = (i * 32 + 8 * b) * SLAB + 4 * t + k
                    slab[pl.ds(to, 8, stride=SLAB), :] = x_s[k, t, pl.ds(start, 8), :]
            return carry

        lax.fori_loop(0, T // 32, lay, 0)
    lane, sub = iota((8, L), 1), iota((8, L), 0)
    ready.wait()
    for o in range(NO):
        acc = jnp.zeros((8, L), F32)
        for j in range(L):
            x = slab[pl.ds(slots[o, j], 8), :]
            acc = jnp.where(lane == j, pltpu.roll(x, slots[NO + o, j], 1), acc)
        g_o[8 * o : 8 * o + 8, :] = jnp.where(sub < 4, acc * wt[o : o + 1, :], 0.0)


def pack_kernel(g, rows, out):
    out[...] = g[...]
    total = jnp.sum(rows[...], axis=0, keepdims=True)
    for o in range(NO):
        out[8 * o + 4 : 8 * o + 5, :] = total


def solve(tot):
    lane = iota((1, L), 1)

    def pick(k):
        return jnp.sum(jnp.where(lane == k, tot, 0.0), axis=1, keepdims=True)

    h, b = {}, []
    k = 0
    for p in range(4):
        for q in range(p, 4):
            h[p, q] = pick(k)
            k += 1
        b.append(pick(k))
        k += 1
    floor = [3e-7 * h[p, p] for p in range(4)]
    inv = []
    for p in range(4):
        inv.append(jnp.where(h[p, p] > floor[p], 1.0 / h[p, p], 0.0))
        for q in range(p + 1, 4):
            f = h[p, q] * inv[p]
            for r in range(q, 4):
                h[q, r] = h[q, r] - f * h[p, r]
            b[q] = b[q] - f * b[p]
    c = [None] * 4
    for p in (3, 2, 1, 0):
        s = b[p]
        for q in range(p + 1, 4):
            s = s - h[p, q] * c[q]
        c[p] = s * inv[p]
    return [c[0]] + [c[k + 1] - Q[k] * c[0] for k in range(3)]


def combine_kernel(hist, ahead, coef, rims, out, h_s, x_s, sem_in, sem_out):
    n = T // STEPS
    load = [
        pltpu.make_async_copy(
            hist.at[pl.ds(1, 3), :, pl.ds(i * n, n), :], h_s.at[i], sem_in.at[i]
        )
        for i in range(STEPS)
    ]
    save = [
        pltpu.make_async_copy(x_s.at[pl.ds(i * n, n), :], out.at[pl.ds(i * n, n), :], sem_out.at[i])
        for i in range(STEPS)
    ]
    for copy in load:
        copy.start()
    c = [coef[k : k + 1, 0:1] for k in range(4)]
    for i in range(STEPS):
        load[i].wait()
        for t in range(LT):
            h = [ahead[0, t, i * n : (i + 1) * n, :]] + [h_s[i, k, t] for k in range(3)]
            x_s[i * n : (i + 1) * n, lanes(t)] = (c[0] * h[0] + c[1] * h[1]) + (
                c[2] * h[2] + c[3] * h[3]
            )
        for end, step, low in ((0, 0, 0), (1, STEPS - 1, n - 8)):
            if i == step:
                for t in range(LT):
                    x = c[0] * ahead[0, t, i * n + low : i * n + low + 8, :]
                    for k in range(3):
                        x += c[k + 1] * rims[16 * k + 8 * end : 16 * k + 8 * end + 8, lanes(t)]
                    x_s[i * n + low : i * n + low + 8, lanes(t)] = x
        save[i].start()
    for copy in save:
        copy.wait()


def coarse_neighbours(pos, u, row_1, row_2, col_1, col_2):
    above, below = from_pairs(pos, 0, row_1, row_2)
    above, below = above[7:8, :], below[0:1, :]
    from_l, from_r = from_pairs(pos, 1, col_1, col_2)
    above = jnp.where(at(pos, 0, above) > 0, above, 0.0)
    below = jnp.where(at(pos, 0, below) < 7, below, 0.0)
    r, lane = iota((CB, CB), 0), iota((CB, CB), 1)
    g, gl = iota((8, CB), 0), iota((8, CB), 1)
    turned_l = jnp.where(g == 0, 0.0, pltpu.roll(from_l, 1, 0))
    turned_r = jnp.where(g == 7, 0.0, pltpu.roll(from_r, 7, 0))
    place = at(pos, 1, from_l)
    from_l = jnp.where(place == 0, turned_l, from_l)
    from_r = jnp.where(place == NO - 1, turned_r, from_r)
    seam_l = tn(from_l, jnp.where(gl == g * GROUP, 1.0, 0.0), HI)
    seam_r = tn(from_r, jnp.where(gl == g * GROUP + GROUP - 1, 1.0, 0.0), HI)
    near = jnp.where(r == 0, above, pltpu.roll(u, 1, 0))
    near += jnp.where(r == CB - 1, below, pltpu.roll(u, CB - 1, 0))
    near += jnp.where(lane % GROUP == 0, seam_l, pltpu.roll(u, 1, 1))
    near += jnp.where(lane % GROUP == GROUP - 1, seam_r, pltpu.roll(u, CB - 1, 1))
    return near


def base_kernel(
    hist, pos, held, volt, cleak, col_1, col_2, row_1, row_2, around,
    cdiag, scale, base, r_o, c_o, ahead, sem,
):
    copy = pltpu.make_async_copy(hist.at[pl.ds(0, 1)], ahead, sem.at[0])
    copy.start()
    for o in range(NO):
        h = held[o : o + 1, :]
        r_o[:, lanes(o)] = onehot(h >> 7, CB)
        c_o[:, lanes(o)] = onehot(h & (CB - 1), CB)
    count = nt(r_o[...], c_o[...])
    diag = 4.0 * coarse_conductance + cleak[...] + via_conductance * count
    u = volt[...]
    second = col_2[:, T:]
    place = at(pos, 1, second)
    second = jnp.where((place == 0) | (place == NO - 1), around[...], second)
    near = coarse_neighbours(pos, u, row_1[:, W:], row_2[:, W:], col_1[:, T:], second)
    cdiag[...] = diag
    scale[...] = relaxation / diag
    base[...] = u - relaxation * (diag * u - coarse_conductance * near) / diag
    copy.wait()


def sweep1_kernel(pos, arrived, scale, base, r, c, coef, u_o, src_o, c1, c2, r1, r2, v_s):
    tot = arrived[4:5, :]
    for o in range(1, NO):
        tot += arrived[8 * o + 4 : 8 * o + 5, :]
    d = solve(tot)
    sub = iota((8, L), 0)
    cf = jnp.zeros((8, L), F32)
    for k in range(4):
        cf = jnp.where(sub == k, d[k], cf)
    coef[...] = cf
    for o in range(NO):
        v = jnp.sum(arrived[8 * o : 8 * o + 8, :] * cf, axis=0, keepdims=True)
        hi, lo = hi_lo(v)
        on = c[:, lanes(o)]
        v_s[:, lanes(o)] = on * hi.astype(BF16)
        v_s[:, lanes(NO + o)] = on * lo.astype(BF16)
    src = nt(r[...], v_s[:, : NO * L]) + nt(r[...], v_s[:, NO * L :])
    u = base[...] + scale[...] * src
    u_o[...] = u
    src_o[...] = src
    g, gl = iota((8, CB), 0), iota((8, CB), 1)
    to_l = nt(jnp.where(gl == g * GROUP, 1.0, 0.0), u, HI)
    to_r = nt(jnp.where(gl == g * GROUP + GROUP - 1, 1.0, 0.0), u, HI)
    c1[...], c2[...] = pair_order(pos, 1, to_l, to_r)
    r1[...], r2[...] = pair_order(pos, 0, u[0:8, :], u[CB - 8 :, :])


def sweep2_kernel(pos, u, src, cdiag, scale, col_1, col_2, row_1, row_2, u_o):
    near = coarse_neighbours(pos, u[...], row_1[...], row_2[...], col_1[...], col_2[...])
    u_o[...] = u[...] + scale[...] * (src[...] - (cdiag[...] * u[...] - coarse_conductance * near))


VM = pl.BlockSpec(memory_space=pltpu.VMEM)
ANY = pl.BlockSpec(memory_space=pltpu.HBM)
vmem = pltpu.MemorySpace.VMEM
hbm = jax.ShapeDtypeStruct


def keep(*args):
    return [pltpu.with_memory_space_constraint(x, pltpu.VMEM) for x in args]


def leave(*args):
    return [pltpu.with_memory_space_constraint(x, pltpu.HBM) for x in args]


def call(body, outs, args, scratch=(), flops=0, any_in=0, any_out=0):
    specs = [ANY] * any_in + [VM] * (len(args) - any_in)
    return pl.pallas_call(
        body,
        out_shape=outs,
        in_specs=specs,
        out_specs=[ANY] * any_out + [VM] * (len(outs) - any_out),
        scratch_shapes=list(scratch),
        cost_estimate=pl.CostEstimate(flops=flops, bytes_accessed=0, transcendentals=0),
        compiler_params=pltpu.CompilerParams(vmem_limit_bytes=20 * 2**20),
    )(*args)


def exchange(axis, first, second, wrap=False):
    n = lax.axis_size(axis)
    near = [(i, i ^ 1) for i in range(n)]
    ends = (n - 1, 0) if wrap else (0, n - 1)
    far = [(0, ends[0])] + [(i, ((i + 1) ^ 1) - 1) for i in range(1, n - 1)] + [(n - 1, ends[1])]
    return lax.ppermute(first, axis, near), lax.ppermute(second, axis, far)


def spread(x, axis=COL):
    return lax.all_to_all(x, axis, split_axis=0, concat_axis=0, tiled=True)


def per_device(load_amp, load_mask, leak, coarse_leak, coarse_init, via_fine, via_coarse, via_count):
    pos = jnp.where(
        lax.broadcasted_iota(jnp.int32, (8, W + CB), 0) == 0, lax.axis_index(ROW), lax.axis_index(COL)
    ).astype(jnp.int32)
    live = jnp.arange(L, dtype=jnp.int32)[None, :] < via_count.reshape(NO, 1)
    wt = jnp.where(live, via_conductance, 0.0).astype(F32)
    fine = via_fine.reshape(NO, L)
    coarse = via_coarse.reshape(NO, L)
    request = jnp.where(live, ((coarse >> 11) << 7) | (coarse & (CB - 1)), -1)
    held = spread(request)

    tile, block, slots = vmem((T, T), F32), vmem((CB, CB), F32), vmem((NO, L), F32)
    hot, chot = vmem((T, NO * L), BF16), vmem((CB, NO * L), BF16)
    hots = vmem((T, 2 * NO * L), BF16)
    rim16, side, seam = vmem((16, T), F32), vmem((8, W), F32), vmem((8, CB), F32)
    ext, packed = vmem((LT + 1, EXT, L), F32), ((L, L), F32)
    dmas = pltpu.SemaphoreType.DMA((4,))
    big = 20_000_000_000

    drops, where, volt, fine, seams, around, via = call(
        parts_kernel,
        [vmem((3 * CB, CB), BF16), pltpu.MemorySpace.HBM((2 * NO, L), jnp.int32), block,
         vmem((NO, L), jnp.int32), vmem((16, CB), F32), seam,
         pltpu.MemorySpace.HBM((T, T), F32)],
        leave(coarse_init, fine) + keep(wt, pos), [hot, hot], flops=big,
    )
    last = lax.axis_size(COL) - 1
    around = lax.ppermute(around, COL, [(0, last)] + [(i, i) for i in range(1, last)] + [(last, 0)])
    zl, invd, strips, irims = call(
        diag_kernel, [tile, tile, rim16, rim16],
        leave(load_amp, load_mask, leak, via),
        [tile, vmem((T, T), jnp.int32), tile, tile, dmas], flops=big, any_in=4,
    )
    looked = call(lookup_kernel, [slots], keep(held, drops))[0]
    at_via = spread(looked)
    a, send_1, send_2 = call(
        strips_kernel, [hot, side, side], keep(pos, fine, wt, at_via, strips, seams)    )
    col_1, col_2 = exchange(COL, send_1, send_2)
    z, zrims = call(
        rhs_kernel, [tile, rim16], keep(fine, wt, at_via, zl, invd, a), [hots], flops=big
    )
    rim = vmem((8, W + CB), F32)
    send_1, send_2, corners = call(
        edge_kernel, [rim, rim, vmem((64, L), F32)],
        keep(pos, zrims, irims, col_1, col_2, volt)    )
    row_1, row_2 = exchange(ROW, send_1, send_2)
    hist, acc = call(
        basis_kernel, [pltpu.MemorySpace.HBM((4, LT, T, L), F32), vmem((8 * SUMS, L), F32)], keep(pos, z, invd, col_1, col_2),
        [ext] * 5 + [dmas], flops=big, any_out=1,
    )
    rims, part = call(
        rim_kernel, [vmem((48, T), F32), vmem((8, L), F32)],
        keep(pos, z, invd, corners, row_1, row_2, acc)    )
    rows = spread(part, ROW)
    g = call(
        gather_kernel, [vmem(*packed)], leave(hist, where) + keep(rims, wt),
        [vmem((4, LT, T, L), F32), vmem((T * SLAB + 8, L), F32),
         pltpu.MemorySpace.SMEM((2 * NO, L), jnp.int32), pltpu.SemaphoreType.DMA((5,))],
        flops=big, any_in=2,
    )[0]
    arrived = spread(call(pack_kernel, [vmem(*packed)], keep(g, rows))[0])
    cdiag, scale, base, r_hot, c_hot, ahead = call(
        base_kernel, [block, block, block, chot, chot, vmem((1, LT, T, L), F32)],
        leave(hist) + keep(pos, held, volt, coarse_leak, col_1, col_2, row_1, row_2, around),
        [dmas], flops=big, any_in=1,
    )
    coef, u, src, c1, c2, r1, r2 = call(
        sweep1_kernel, [seam, block, block, seam, seam, seam, seam],
        keep(pos, arrived, scale, base, r_hot, c_hot), [vmem((CB, 2 * NO * L), BF16)]    )
    c1, c2 = exchange(COL, c1, c2, wrap=True)
    r1, r2 = exchange(ROW, r1, r2)
    fine_drop = call(
        combine_kernel, [pltpu.MemorySpace.HBM((T, T), F32)], leave(hist) + keep(ahead, coef, rims),
        [vmem((STEPS, 3, LT, T // STEPS, L), F32), tile, pltpu.SemaphoreType.DMA((STEPS,)),
         pltpu.SemaphoreType.DMA((STEPS,))], flops=big // 4, any_in=1, any_out=1,
    )[0]
    coarse_drop = call(
        sweep2_kernel, [hbm((CB, CB), F32)], keep(pos, u, src, cdiag, scale, c1, c2, r1, r2)    )[0]
    return fine_drop, coarse_drop


def solution(mesh):
    spec = P(ROW, COL)

    return jax.shard_map(
        per_device, mesh=mesh, in_specs=(spec,) * 8, out_specs=(spec, spec), check_vma=False
    )
```

```python
import jax
import jax.numpy as jnp
from jax import lax
from jax.experimental import pallas as pl
from jax.experimental.pallas import tpu as pltpu
from jax.sharding import PartitionSpec as P


F32 = jnp.float32
BF16 = jnp.bfloat16
HI = lax.Precision.HIGHEST
ROW, COL = "row", "col"

GROUP = 16
via_conductance = 2.0
coarse_conductance = 4.0
relaxation = 0.8

T = 512
CB = 128
NO = 16
L = 128
OFF = 16
EXT = OFF + T + 16
W = T + L

Q = (1.09375, 1.765625, 1.28125)
RHO = (1.0 - Q[0], Q[0] - Q[1], Q[1] - Q[2], Q[2])
LT = T // L
SLAB = 4 * LT + 1
SUMS = 8
STEPS = 8


def iota(shape, dim):
    return lax.broadcasted_iota(jnp.int32, shape, dim)


def nt(a, b, precision=None):
    return lax.dot_general(
        a, b, (((1,), (1,)), ((), ())), precision=precision, preferred_element_type=F32
    )


def tn(a, b, precision=None):
    return lax.dot_general(
        a, b, (((0,), (0,)), ((), ())), precision=precision, preferred_element_type=F32
    )


def onehot(idx, n):
    return jnp.where(iota((n, idx.shape[1]), 0) == idx, 1.0, 0.0).astype(BF16)


def hi_lo(x):
    hi = x.astype(BF16).astype(F32)
    return hi, x - hi


def lanes(o):
    return slice(o * L, (o + 1) * L)


def at(pos, k, like):
    return jnp.broadcast_to(pos[k : k + 1, : like.shape[1]], like.shape)


def pair_order(pos, k, low, high):
    even = (at(pos, k, low) & 1) == 0
    return jnp.where(even, high, low), jnp.where(even, low, high)


def from_pairs(pos, k, first, second):
    even = (at(pos, k, first) & 1) == 0
    return jnp.where(even, second, first), jnp.where(even, first, second)


def diag_kernel(
    amp, mask, leak, via, zl, invd, strips, rims, amp_s, mask_s, leak_s, via_s, sem
):
    copies = [
        pltpu.make_async_copy(x, y, sem.at[k])
        for k, (x, y) in enumerate(
            ((leak, leak_s), (via, via_s), (amp, amp_s), (mask, mask_s))
        )
    ]
    for copy in copies:
        copy.start()
    for copy in copies:
        copy.wait()
    inv = 1.0 / (4.0 + leak_s[...] + via_s[...])
    z = amp_s[...] * mask_s[...].astype(F32) * inv
    zl[...] = z
    invd[...] = inv
    j, lane = iota((8, 2 * L), 0), iota((8, 2 * L), 1)
    pick = jnp.where(lane == jnp.where(j < 4, j, 2 * L - 8 + j), 1.0, 0.0).astype(BF16)
    for k, x in enumerate((z, inv)):
        hi, rest = hi_lo(jnp.concatenate([x[:, :L], x[:, T - L :]], axis=1))
        mid, lo = hi_lo(rest)
        strips[8 * k : 8 * k + 8, :] = (
            nt(pick, lo.astype(BF16)) + nt(pick, mid.astype(BF16)) + nt(pick, hi.astype(BF16))
        )
    rims[0:8, :] = inv[0:8]
    rims[8:16, :] = inv[T - 8 :]


def parts_kernel(volt, vf, wt, parts, slots, volt_o, vf_o, seams, via, a_s, b_s):
    u = volt[...]
    f = vf[...]
    volt_o[...] = u
    vf_o[...] = f
    slots[0:NO, :] = (f >> 9) * SLAB + ((f >> 7) & 3) * 4
    slots[NO:, :] = (iota((NO, L), 1) - f) & (L - 1)
    v1, rest = hi_lo(u.T)
    v2, v3 = hi_lo(rest)
    parts[...] = jnp.concatenate([v3, v2, v1], axis=0).astype(BF16)
    g, lane = iota((8, CB), 0), iota((8, CB), 1)
    seams[0:8, :] = nt(jnp.where(lane == g * GROUP, 1.0, 0.0), u, HI)
    seams[8:16, :] = nt(jnp.where(lane == g * GROUP + GROUP - 1, 1.0, 0.0), u, HI)
    for o in range(NO):
        f = vf[o : o + 1, :]
        a_s[:, lanes(o)] = onehot(f // T, T)
        b_s[:, lanes(o)] = jnp.where(iota((T, L), 0) == f % T, wt[o : o + 1, :], 0.0).astype(BF16)
    via[...] = nt(a_s[...], b_s[...])


def lookup_kernel(held, parts, looked):
    v = parts[...]
    for i in range(NO // 2):
        h = jnp.concatenate([held[2 * i : 2 * i + 1, :], held[2 * i + 1 : 2 * i + 2, :]], axis=1)
        y = jnp.dot(v, onehot(h >> 7, CB), preferred_element_type=F32)
        y = y[:CB] + y[CB : 2 * CB] + y[2 * CB :]
        y = jnp.where(iota((CB, 2 * L), 0) == (h & (CB - 1)), y, 0.0)
        y = jnp.sum(y, axis=0, keepdims=True)
        looked[2 * i : 2 * i + 1, :] = y[:, :L]
        looked[2 * i + 1 : 2 * i + 2, :] = y[:, L:]


def strips_kernel(pos, vf, wt, at_via, strips, seams, a_o, send_1, send_2):
    j = iota((8, L), 0)
    colid = jnp.where(j < 4, j, T - 8 + j)
    hs, ls = [], []
    for o in range(NO):
        f = vf[o : o + 1, :]
        a_o[:, lanes(o)] = onehot(f // T, T)
        hi, lo = hi_lo(at_via[o : o + 1, :] * wt[o : o + 1, :])
        on = colid == f % T
        hs.append(jnp.where(on, hi, 0.0))
        ls.append(jnp.where(on, lo, 0.0))
    lhs = jnp.concatenate(
        [jnp.concatenate(hs, axis=1), jnp.concatenate(ls, axis=1)], axis=0
    ).astype(BF16)
    inj = nt(lhs, a_o[...])
    inv = strips[8:16, :]
    z = strips[0:8, :] + (inj[0:8] + inj[8:16]) * inv
    low = iota((8, T), 0) < 4
    to_l = jnp.where(low, z, pltpu.roll(inv, 4, 0))
    to_r = jnp.where(low, pltpu.roll(z, 4, 0), inv)
    send_1[:, :T], send_2[:, :T] = pair_order(pos, 1, to_l, to_r)
    send_1[:, T:], send_2[:, T:] = pair_order(pos, 1, seams[0:8, :], seams[8:16, :])


def rhs_kernel(vf, wt, at_via, zl, invd, a, z, rims, b_s):
    for o in range(NO):
        hi, lo = hi_lo(at_via[o : o + 1, :] * wt[o : o + 1, :])
        on = iota((T, L), 0) == vf[o : o + 1, :] % T
        b_s[:, lanes(o)] = jnp.where(on, hi, 0.0).astype(BF16)
        b_s[:, lanes(NO + o)] = jnp.where(on, lo, 0.0).astype(BF16)
    inj = nt(a[...], b_s[:, : NO * L]) + nt(a[...], b_s[:, NO * L :])
    zz = zl[...] + inj * invd[...]
    z[...] = zz
    rims[0:8, :] = zz[0:8]
    rims[8:16, :] = zz[T - 8 :]


def halo_columns(pos, gl, gr):
    place = at(pos, 1, gl)
    parts = []
    for x in (jnp.where(place < NO - 1, gr, 0.0), jnp.where(place > 0, gl, 0.0)):
        a, rest = hi_lo(x)
        b, c = hi_lo(rest)
        parts += [c, b, a]
    j, lane = iota((8, 2 * L), 0), iota((8, 2 * L), 1)
    to_r = jnp.where(lane == jnp.where(j < 4, j, L + j - 4), 1.0, 0.0)
    to_l = jnp.where(lane == jnp.where(j < 4, 124 + j, L + 120 + j), 1.0, 0.0)
    place = jnp.concatenate([to_r] * 3 + [to_l] * 3, axis=0)
    out = tn(jnp.concatenate(parts, axis=0).astype(BF16), place.astype(BF16))
    return out[:, :L], out[:, L:]


def edge_kernel(pos, zr, ir, col_1, col_2, volt, send_1, send_2, corners):
    got_l, got_r = from_pairs(pos, 1, col_1[...], col_2[...])
    zt, it = halo_columns(pos, got_l[:, :L], got_r[:, :L])
    zb, ib = halo_columns(pos, got_l[:, T - L : T], got_r[:, T - L : T])
    for k, x in enumerate((zt[0:16], zb[L - 16 :], it[0:16], ib[L - 16 :])):
        corners[16 * k : 16 * k + 16, :] = x
    low = iota((8, W), 0) < 4
    zt = jnp.concatenate([zr[0:8, :], zt[0:8]], axis=1)
    it = jnp.concatenate([ir[0:8, :], it[0:8]], axis=1)
    zb = jnp.concatenate([zr[8:16, :], zb[L - 8 :]], axis=1)
    ib = jnp.concatenate([ir[8:16, :], ib[L - 8 :]], axis=1)
    to_u = jnp.where(low, zt, pltpu.roll(it, 4, 0))
    to_d = jnp.where(low, pltpu.roll(zb, 4, 0), ib)
    send_1[:, :W], send_2[:, :W] = pair_order(pos, 0, to_u, to_d)
    send_1[:, W:], send_2[:, W:] = pair_order(pos, 0, volt[0:8, :], volt[CB - 8 :, :])


def beside(block):
    n = block.shape[0]
    rows = pltpu.roll(block, 1, 0) + pltpu.roll(block, n - 1, 0)
    return rows + (pltpu.roll(block, 1, 1) + pltpu.roll(block, W - 1, 1))


def near_tiles(ref, start, rows):
    mid = [ref[t, pl.ds(start, rows), :] for t in range(LT + 1)]
    low = [pltpu.roll(m, 1, 1) for m in mid]
    high = [pltpu.roll(m, L - 1, 1) for m in mid]
    lane = iota((rows, L), 1)
    near = []
    for t in range(LT + 1):
        rows_sum = ref[t, pl.ds(start - 1, rows), :] + ref[t, pl.ds(start + 1, rows), :]
        left = jnp.where(lane == 0, low[t - 1], low[t])
        right = jnp.where(lane == L - 1, high[(t + 1) % (LT + 1)], high[t])
        near.append(rows_sum + (left + right))
    return mid, near


def fold(p):
    return (p[:, 0:128] + p[:, 128:256]) + (p[:, 256:384] + p[:, 384:512])


def moments(z, w, n1, n2, dn3, inv):
    d = 1.0 / inv
    dz, dw, dn1, dn2 = d * z, d * w, d * n1, d * n2
    return dz * z, dz * w, dw * w, dw * n1, dn1 * n1, dn1 * n2, dn2 * n2, n2 * dn3


def basis_kernel(pos, z, invd, col_1, col_2, hist, acc_o, ie, ze, we, n1e, n2e, sem):
    zc, ic = halo_columns(pos, *from_pairs(pos, 1, col_1[:, :T], col_2[:, :T]))
    zero = jnp.zeros((OFF, L), F32)
    own = pl.ds(OFF, T)
    for e in (ie, ze, we, n1e, n2e):
        for t in range(LT + 1):
            e[t, 0:OFF, :] = zero
            e[t, OFF + T :, :] = zero
    for t in range(LT):
        ze[t, own, :] = z[:, lanes(t)]
        ie[t, own, :] = invd[:, lanes(t)]
    ze[LT, own, :] = zc
    ie[LT, own, :] = ic
    rows = 128

    def save(k, e):
        copy = pltpu.make_async_copy(e.at[pl.ds(0, LT), own, :], hist.at[k], sem.at[k])
        copy.start()
        return copy

    def apply_to(src, dst, minus):
        def step(i, carry):
            start = pl.multiple_of(OFF + i * rows, 8)
            mid, near = near_tiles(src, start, rows)
            for t in range(LT + 1):
                y = near[t] * ie[t, pl.ds(start, rows), :]
                dst[t, pl.ds(start, rows), :] = mid[t] - y if minus else y
            return carry

        lax.fori_loop(0, T // rows, step, 0)

    copies = [save(0, ze)]
    apply_to(ze, we, True)
    copies.append(save(1, we))
    apply_to(we, n1e, False)
    copies.append(save(2, n1e))
    apply_to(n1e, n2e, False)
    copies.append(save(3, n2e))

    acc = [jnp.zeros((8, L), F32) for _ in range(SUMS)]
    ends = list(range(0, T + 1, 64))
    ends[0], ends[-1] = 8, T - 8
    for low, high in zip(ends[:-1], ends[1:]):
        start, rows = OFF + low, high - low
        n2, dn3 = near_tiles(n2e, start, rows)
        for t in range(LT):
            z8, w8, n18, i8 = (e[t, pl.ds(start, rows), :] for e in (ze, we, n1e, ie))
            for k, p in enumerate(moments(z8, w8, n18, n2[t], dn3[t], i8)):
                for q in range(0, rows, 8):
                    acc[k] = acc[k] + p[q : q + 8]
    for k in range(SUMS):
        acc_o[8 * k : 8 * k + 8, :] = acc[k]
    for copy in copies:
        copy.wait()


def gram_terms(acc):
    g0, q0 = acc[0], acc[1]
    m = acc[2:]
    r = [q0, q0 - m[0], q0 - m[0] - m[1]]
    h = {(0, 0): q0, **{(0, j): RHO[0] * m[j - 1] for j in (1, 2, 3)}}
    b = [g0] + r
    for k in range(3):
        h[0, 0] = h[0, 0] - Q[k] * m[k]
        b[0] = b[0] - Q[k] * r[k]
    for k in range(6):
        f = sum(Q[j] * RHO[k - j] for j in range(3) if 0 <= k - j < 4)
        h[0, 0] = h[0, 0] - f * m[k]
    for j in (1, 2, 3):
        for k in (1, 2, 3):
            h[0, j] = h[0, j] + RHO[k] * m[j - 1 + k]
            if j <= k:
                h[j, k] = m[j + k - 2] - m[j + k - 1]
    out = []
    for p in range(4):
        out += [h[p, q] for q in range(p, 4)] + [b[p]]
    return out


def rim_kernel(pos, z, invd, corners, row_1, row_2, acc_i, rims, part):
    sub = iota((8, W), 0)
    ours = at(pos, 0, sub)
    above, below = (sub >= 4) & (ours > 0), (sub < 4) & (ours < 7)
    top, bot = from_pairs(pos, 0, row_1[:, :W], row_2[:, :W])
    acc = [acc_i[8 * k : 8 * k + 8, :] for k in range(SUMS)]
    for end in (0, 1):
        rows = slice(0, 16) if end == 0 else slice(T - 16, T)
        zc, ic = corners[16 * end : 16 * end + 16, :], corners[32 + 16 * end : 48 + 16 * end, :]
        z16 = jnp.concatenate([z[rows, :], zc], axis=1)
        i16 = jnp.concatenate([invd[rows, :], ic], axis=1)
        if end == 0:
            zb = jnp.concatenate([jnp.where(above, pltpu.roll(top, 4, 0), 0.0), z16], axis=0)
            ib = jnp.concatenate([jnp.where(above, top, 0.0), i16], axis=0)
            own = slice(8, 16)
        else:
            zb = jnp.concatenate([z16, jnp.where(below, bot, 0.0)], axis=0)
            ib = jnp.concatenate([i16, jnp.where(below, pltpu.roll(bot, 4, 0), 0.0)], axis=0)
            own = slice(8, 16)
        w = zb - ib * beside(zb)
        n1 = ib * beside(w)
        n2 = ib * beside(n1)
        near = beside(n2)
        zo, wo, n1o, n2o, dn3, io = (x[own, :T] for x in (zb, w, n1, n2, near, ib))
        for k, p in enumerate(moments(zo, wo, n1o, n2o, dn3, io)):
            acc[k] = acc[k] + fold(p)
        for k, x in enumerate((wo, n1o, n2o)):
            rims[16 * k + 8 * end : 16 * k + 8 * end + 8, :] = x
    terms = gram_terms(acc)
    rows14 = jnp.concatenate(
        [jnp.sum(a, axis=0, keepdims=True) for a in terms] + [jnp.zeros((2, L), F32)], axis=0
    )
    a, rest = hi_lo(rows14)
    b, c = hi_lo(rest)
    parts = jnp.concatenate([c, b, a], axis=0).astype(BF16)
    sums = nt(jnp.ones((8, L), BF16), parts)
    sums = sums[:, 0:16] + sums[:, 16:32] + sums[:, 32:48]
    sums = jnp.concatenate([sums, jnp.zeros((8, L - 16), F32)], axis=1)
    part[...] = sums


def gather_kernel(hist, table, rims, wt, g_o, x_s, slab, slots, sem):
    copies = [pltpu.make_async_copy(hist.at[k], x_s.at[k], sem.at[k]) for k in range(4)]
    ready = pltpu.make_async_copy(table, slots, sem.at[4])
    ready.start()
    for copy in copies:
        copy.start()
    for k in range(4):
        copies[k].wait()
        if k:
            for t in range(LT):
                x_s[k, t, 0:8, :] = rims[16 * k - 16 : 16 * k - 8, lanes(t)]
                x_s[k, t, T - 8 :, :] = rims[16 * k - 8 : 16 * k, lanes(t)]

        def lay(i, carry):
            for b in range(4):
                for t in range(LT):
                    start = pl.multiple_of(i * 32 + 8 * b, 8)
                    to = (i * 32 + 8 * b) * SLAB + 4 * t + k
                    slab[pl.ds(to, 8, stride=SLAB), :] = x_s[k, t, pl.ds(start, 8), :]
            return carry

        lax.fori_loop(0, T // 32, lay, 0)
    lane, sub = iota((8, L), 1), iota((8, L), 0)
    ready.wait()
    for o in range(NO):
        acc = jnp.zeros((8, L), F32)
        for j in range(L):
            x = slab[pl.ds(slots[o, j], 8), :]
            acc = jnp.where(lane == j, pltpu.roll(x, slots[NO + o, j], 1), acc)
        g_o[8 * o : 8 * o + 8, :] = jnp.where(sub < 4, acc * wt[o : o + 1, :], 0.0)


def pack_kernel(g, rows, out):
    out[...] = g[...]
    total = jnp.sum(rows[...], axis=0, keepdims=True)
    for o in range(NO):
        out[8 * o + 4 : 8 * o + 5, :] = total


def solve(tot):
    lane = iota((1, L), 1)

    def pick(k):
        return jnp.sum(jnp.where(lane == k, tot, 0.0), axis=1, keepdims=True)

    h, b = {}, []
    k = 0
    for p in range(4):
        for q in range(p, 4):
            h[p, q] = pick(k)
            k += 1
        b.append(pick(k))
        k += 1
    floor = [3e-7 * h[p, p] for p in range(4)]
    inv = []
    for p in range(4):
        inv.append(jnp.where(h[p, p] > floor[p], 1.0 / h[p, p], 0.0))
        for q in range(p + 1, 4):
            f = h[p, q] * inv[p]
            for r in range(q, 4):
                h[q, r] = h[q, r] - f * h[p, r]
            b[q] = b[q] - f * b[p]
    c = [None] * 4
    for p in (3, 2, 1, 0):
        s = b[p]
        for q in range(p + 1, 4):
            s = s - h[p, q] * c[q]
        c[p] = s * inv[p]
    return [c[0]] + [c[k + 1] - Q[k] * c[0] for k in range(3)]


def combine_kernel(hist, ahead, coef, rims, out, h_s, x_s, sem_in, sem_out):
    n = T // STEPS
    load = [
        pltpu.make_async_copy(
            hist.at[pl.ds(1, 3), :, pl.ds(i * n, n), :], h_s.at[i], sem_in.at[i]
        )
        for i in range(STEPS)
    ]
    save = [
        pltpu.make_async_copy(x_s.at[pl.ds(i * n, n), :], out.at[pl.ds(i * n, n), :], sem_out.at[i])
        for i in range(STEPS)
    ]
    for copy in load:
        copy.start()
    c = [coef[k : k + 1, 0:1] for k in range(4)]
    for i in range(STEPS):
        load[i].wait()
        for t in range(LT):
            h = [ahead[0, t, i * n : (i + 1) * n, :]] + [h_s[i, k, t] for k in range(3)]
            x_s[i * n : (i + 1) * n, lanes(t)] = (c[0] * h[0] + c[1] * h[1]) + (
                c[2] * h[2] + c[3] * h[3]
            )
        for end, step, low in ((0, 0, 0), (1, STEPS - 1, n - 8)):
            if i == step:
                for t in range(LT):
                    x = c[0] * ahead[0, t, i * n + low : i * n + low + 8, :]
                    for k in range(3):
                        x += c[k + 1] * rims[16 * k + 8 * end : 16 * k + 8 * end + 8, lanes(t)]
                    x_s[i * n + low : i * n + low + 8, lanes(t)] = x
        save[i].start()
    for copy in save:
        copy.wait()


def coarse_neighbours(pos, u, row_1, row_2, col_1, col_2):
    above, below = from_pairs(pos, 0, row_1, row_2)
    above, below = above[7:8, :], below[0:1, :]
    from_l, from_r = from_pairs(pos, 1, col_1, col_2)
    above = jnp.where(at(pos, 0, above) > 0, above, 0.0)
    below = jnp.where(at(pos, 0, below) < 7, below, 0.0)
    r, lane = iota((CB, CB), 0), iota((CB, CB), 1)
    g, gl = iota((8, CB), 0), iota((8, CB), 1)
    turned_l = jnp.where(g == 0, 0.0, pltpu.roll(from_l, 1, 0))
    turned_r = jnp.where(g == 7, 0.0, pltpu.roll(from_r, 7, 0))
    place = at(pos, 1, from_l)
    from_l = jnp.where(place == 0, turned_l, from_l)
    from_r = jnp.where(place == NO - 1, turned_r, from_r)
    seam_l = tn(from_l, jnp.where(gl == g * GROUP, 1.0, 0.0), HI)
    seam_r = tn(from_r, jnp.where(gl == g * GROUP + GROUP - 1, 1.0, 0.0), HI)
    near = jnp.where(r == 0, above, pltpu.roll(u, 1, 0))
    near += jnp.where(r == CB - 1, below, pltpu.roll(u, CB - 1, 0))
    near += jnp.where(lane % GROUP == 0, seam_l, pltpu.roll(u, 1, 1))
    near += jnp.where(lane % GROUP == GROUP - 1, seam_r, pltpu.roll(u, CB - 1, 1))
    return near


def base_kernel(
    hist, pos, held, volt, cleak, col_1, col_2, row_1, row_2,
    cdiag, scale, base, r_o, c_o, ahead, sem,
):
    copy = pltpu.make_async_copy(hist.at[pl.ds(0, 1)], ahead, sem.at[0])
    copy.start()
    for o in range(NO):
        h = held[o : o + 1, :]
        r_o[:, lanes(o)] = onehot(h >> 7, CB)
        c_o[:, lanes(o)] = onehot(h & (CB - 1), CB)
    count = nt(r_o[...], c_o[...])
    diag = 4.0 * coarse_conductance + cleak[...] + via_conductance * count
    u = volt[...]
    near = coarse_neighbours(pos, u, row_1[:, W:], row_2[:, W:], col_1[:, T:], col_2[:, T:])
    cdiag[...] = diag
    scale[...] = relaxation / diag
    base[...] = u - relaxation * (diag * u - coarse_conductance * near) / diag
    copy.wait()


def sweep1_kernel(pos, arrived, scale, base, r, c, coef, u_o, src_o, c1, c2, r1, r2, v_s):
    tot = arrived[4:5, :]
    for o in range(1, NO):
        tot += arrived[8 * o + 4 : 8 * o + 5, :]
    d = solve(tot)
    sub = iota((8, L), 0)
    cf = jnp.zeros((8, L), F32)
    for k in range(4):
        cf = jnp.where(sub == k, d[k], cf)
    coef[...] = cf
    for o in range(NO):
        v = jnp.sum(arrived[8 * o : 8 * o + 8, :] * cf, axis=0, keepdims=True)
        hi, lo = hi_lo(v)
        on = c[:, lanes(o)]
        v_s[:, lanes(o)] = on * hi.astype(BF16)
        v_s[:, lanes(NO + o)] = on * lo.astype(BF16)
    src = nt(r[...], v_s[:, : NO * L]) + nt(r[...], v_s[:, NO * L :])
    u = base[...] + scale[...] * src
    u_o[...] = u
    src_o[...] = src
    g, gl = iota((8, CB), 0), iota((8, CB), 1)
    to_l = nt(jnp.where(gl == g * GROUP, 1.0, 0.0), u, HI)
    to_r = nt(jnp.where(gl == g * GROUP + GROUP - 1, 1.0, 0.0), u, HI)
    c1[...], c2[...] = pair_order(pos, 1, to_l, to_r)
    r1[...], r2[...] = pair_order(pos, 0, u[0:8, :], u[CB - 8 :, :])


def sweep2_kernel(pos, u, src, cdiag, scale, col_1, col_2, row_1, row_2, u_o):
    near = coarse_neighbours(pos, u[...], row_1[...], row_2[...], col_1[...], col_2[...])
    u_o[...] = u[...] + scale[...] * (src[...] - (cdiag[...] * u[...] - coarse_conductance * near))


VM = pl.BlockSpec(memory_space=pltpu.VMEM)
ANY = pl.BlockSpec(memory_space=pltpu.HBM)
vmem = pltpu.MemorySpace.VMEM
hbm = jax.ShapeDtypeStruct


def keep(*args):
    return [pltpu.with_memory_space_constraint(x, pltpu.VMEM) for x in args]


def leave(*args):
    return [pltpu.with_memory_space_constraint(x, pltpu.HBM) for x in args]


def call(body, outs, args, scratch=(), flops=0, any_in=0, any_out=0):
    specs = [ANY] * any_in + [VM] * (len(args) - any_in)
    return pl.pallas_call(
        body,
        out_shape=outs,
        in_specs=specs,
        out_specs=[ANY] * any_out + [VM] * (len(outs) - any_out),
        scratch_shapes=list(scratch),
        cost_estimate=pl.CostEstimate(flops=flops, bytes_accessed=0, transcendentals=0),
        compiler_params=pltpu.CompilerParams(vmem_limit_bytes=20 * 2**20),
    )(*args)


def exchange_columns(first, second):
    n = lax.axis_size(COL)
    near = [(i, i ^ 1) for i in range(n)]
    far = [(i, ((i + 1) ^ 1) - 1 & (n - 1)) for i in range(n)]
    return lax.ppermute(first, COL, near), lax.ppermute(second, COL, far)


def exchange_rows(first, second):
    n, m = lax.axis_size(ROW), lax.axis_size(COL)
    near = [(i, i ^ 1) for i in range(n)]
    far = []
    for i in range(n):
        for k in range(m):
            to = (i, k ^ 1) if i in (0, n - 1) else (((i + 1) ^ 1) - 1, k)
            far.append((i * m + k, to[0] * m + to[1]))
    return lax.ppermute(first, ROW, near), lax.ppermute(second, (ROW, COL), far)


def spread(x, axis=COL):
    return lax.all_to_all(x, axis, split_axis=0, concat_axis=0, tiled=True)


def per_device(load_amp, load_mask, leak, coarse_leak, coarse_init, via_fine, via_coarse, via_count):
    pos = jnp.where(
        lax.broadcasted_iota(jnp.int32, (8, W + CB), 0) == 0, lax.axis_index(ROW), lax.axis_index(COL)
    ).astype(jnp.int32)
    live = jnp.arange(L, dtype=jnp.int32)[None, :] < via_count.reshape(NO, 1)
    wt = jnp.where(live, via_conductance, 0.0).astype(F32)
    fine = via_fine.reshape(NO, L)
    coarse = via_coarse.reshape(NO, L)
    request = jnp.where(live, ((coarse >> 11) << 7) | (coarse & (CB - 1)), -1)
    held = spread(request)

    tile, block, slots = vmem((T, T), F32), vmem((CB, CB), F32), vmem((NO, L), F32)
    hot, chot = vmem((T, NO * L), BF16), vmem((CB, NO * L), BF16)
    hots = vmem((T, 2 * NO * L), BF16)
    rim16, side, seam = vmem((16, T), F32), vmem((8, W), F32), vmem((8, CB), F32)
    ext, packed = vmem((LT + 1, EXT, L), F32), ((L, L), F32)
    dmas = pltpu.SemaphoreType.DMA((4,))
    big = 20_000_000_000

    drops, where, volt, fine, seams, via = call(
        parts_kernel,
        [vmem((3 * CB, CB), BF16), pltpu.MemorySpace.HBM((2 * NO, L), jnp.int32), block,
         vmem((NO, L), jnp.int32), vmem((16, CB), F32),
         pltpu.MemorySpace.HBM((T, T), F32)],
        leave(coarse_init, fine) + keep(wt), [hot, hot], flops=big,
    )
    zl, invd, strips, irims = call(
        diag_kernel, [tile, tile, rim16, rim16],
        leave(load_amp, load_mask, leak, via),
        [tile, vmem((T, T), jnp.int32), tile, tile, dmas], flops=big, any_in=4,
    )
    looked = call(lookup_kernel, [slots], keep(held, drops))[0]
    at_via = spread(looked)
    a, send_1, send_2 = call(
        strips_kernel, [hot, side, side], keep(pos, fine, wt, at_via, strips, seams)    )
    col_1, col_2 = exchange_columns(send_1, send_2)
    z, zrims = call(
        rhs_kernel, [tile, rim16], keep(fine, wt, at_via, zl, invd, a), [hots], flops=big
    )
    rim = vmem((8, W + CB), F32)
    send_1, send_2, corners = call(
        edge_kernel, [rim, rim, vmem((64, L), F32)],
        keep(pos, zrims, irims, col_1, col_2, volt)    )
    row_1, row_2 = exchange_rows(send_1, send_2)
    hist, acc = call(
        basis_kernel, [pltpu.MemorySpace.HBM((4, LT, T, L), F32), vmem((8 * SUMS, L), F32)], keep(pos, z, invd, col_1, col_2),
        [ext] * 5 + [dmas], flops=big, any_out=1,
    )
    rims, part = call(
        rim_kernel, [vmem((48, T), F32), vmem((8, L), F32)],
        keep(pos, z, invd, corners, row_1, row_2, acc)    )
    rows = spread(part, ROW)
    g = call(
        gather_kernel, [vmem(*packed)], leave(hist, where) + keep(rims, wt),
        [vmem((4, LT, T, L), F32), vmem((T * SLAB + 8, L), F32),
         pltpu.MemorySpace.SMEM((2 * NO, L), jnp.int32), pltpu.SemaphoreType.DMA((5,))],
        flops=big, any_in=2,
    )[0]
    arrived = spread(call(pack_kernel, [vmem(*packed)], keep(g, rows))[0])
    cdiag, scale, base, r_hot, c_hot, ahead = call(
        base_kernel, [block, block, block, chot, chot, vmem((1, LT, T, L), F32)],
        leave(hist) + keep(pos, held, volt, coarse_leak, col_1, col_2, row_1, row_2),
        [dmas], flops=big, any_in=1,
    )
    coef, u, src, c1, c2, r1, r2 = call(
        sweep1_kernel, [seam, block, block, seam, seam, seam, seam],
        keep(pos, arrived, scale, base, r_hot, c_hot), [vmem((CB, 2 * NO * L), BF16)]    )
    c1, c2 = exchange_columns(c1, c2)
    r1, r2 = exchange_rows(r1, r2)
    fine_drop = call(
        combine_kernel, [pltpu.MemorySpace.HBM((T, T), F32)], leave(hist) + keep(ahead, coef, rims),
        [vmem((STEPS, 3, LT, T // STEPS, L), F32), tile, pltpu.SemaphoreType.DMA((STEPS,)),
         pltpu.SemaphoreType.DMA((STEPS,))], flops=big // 4, any_in=1, any_out=1,
    )[0]
    coarse_drop = call(
        sweep2_kernel, [hbm((CB, CB), F32)], keep(pos, u, src, cdiag, scale, c1, c2, r1, r2)    )[0]
    return fine_drop, coarse_drop


def solution(mesh):
    spec = P(ROW, COL)

    return jax.shard_map(
        per_device, mesh=mesh, in_specs=(spec,) * 8, out_specs=(spec, spec), check_vma=False
    )
```

```python
import jax
import jax.numpy as jnp
from jax import lax
from jax.experimental import pallas as pl
from jax.experimental.pallas import tpu as pltpu
from jax.sharding import PartitionSpec as P


F32 = jnp.float32
BF16 = jnp.bfloat16
HI = lax.Precision.HIGHEST
ROW, COL = "row", "col"

GROUP = 16
via_conductance = 2.0
coarse_conductance = 4.0
relaxation = 0.8

T = 512
CB = 128
NO = 16
L = 128
OFF = 16
EXT = OFF + T + 16
W = T + L

Q = (1.09375, 1.765625, 1.28125)
RHO = (1.0 - Q[0], Q[0] - Q[1], Q[1] - Q[2], Q[2])
LT = T // L
SLAB = 4 * LT + 1
SUMS = 8
STEPS = 8


def iota(shape, dim):
    return lax.broadcasted_iota(jnp.int32, shape, dim)


def nt(a, b, precision=None):
    return lax.dot_general(
        a, b, (((1,), (1,)), ((), ())), precision=precision, preferred_element_type=F32
    )


def tn(a, b, precision=None):
    return lax.dot_general(
        a, b, (((0,), (0,)), ((), ())), precision=precision, preferred_element_type=F32
    )


def onehot(idx, n):
    return jnp.where(iota((n, idx.shape[1]), 0) == idx, 1.0, 0.0).astype(BF16)


def hi_lo(x):
    hi = x.astype(BF16).astype(F32)
    return hi, x - hi


def lanes(o):
    return slice(o * L, (o + 1) * L)


def at(pos, k, like):
    return jnp.broadcast_to(pos[k : k + 1, : like.shape[1]], like.shape)


def pair_order(pos, k, low, high):
    even = (at(pos, k, low) & 1) == 0
    return jnp.where(even, high, low), jnp.where(even, low, high)


def from_pairs(pos, k, first, second):
    even = (at(pos, k, first) & 1) == 0
    return jnp.where(even, second, first), jnp.where(even, first, second)


def diag_kernel(
    amp, mask, leak, via, zl, invd, strips, rims, amp_s, mask_s, leak_s, via_s, sem
):
    copies = [
        pltpu.make_async_copy(x, y, sem.at[k])
        for k, (x, y) in enumerate(
            ((leak, leak_s), (via, via_s), (amp, amp_s), (mask, mask_s))
        )
    ]
    for copy in copies:
        copy.start()
    for copy in copies:
        copy.wait()
    inv = 1.0 / (4.0 + leak_s[...] + via_s[...])
    z = amp_s[...] * mask_s[...].astype(F32) * inv
    zl[...] = z
    invd[...] = inv
    j, lane = iota((8, 2 * L), 0), iota((8, 2 * L), 1)
    pick = jnp.where(lane == jnp.where(j < 4, j, 2 * L - 8 + j), 1.0, 0.0).astype(BF16)
    for k, x in enumerate((z, inv)):
        hi, rest = hi_lo(jnp.concatenate([x[:, :L], x[:, T - L :]], axis=1))
        mid, lo = hi_lo(rest)
        strips[8 * k : 8 * k + 8, :] = (
            nt(pick, lo.astype(BF16)) + nt(pick, mid.astype(BF16)) + nt(pick, hi.astype(BF16))
        )
    rims[0:8, :] = inv[0:8]
    rims[8:16, :] = inv[T - 8 :]


def parts_kernel(volt, vf, vc, wt, node, slots, volt_o, vf_o, seams, via, a_s, b_s):
    u = volt[...]
    f = vf[...]
    volt_o[...] = u
    vf_o[...] = f
    slots[0:NO, :] = (f >> 9) * SLAB + ((f >> 7) & 3) * 4
    slots[NO:, :] = (iota((NO, L), 1) - f) & (L - 1)
    place = ((vc[...] >> 11) << 7) | (vc[...] & (CB - 1))
    node[...] = jnp.where(wt[...] > 0.0, place.astype(F32), -1.0)
    g, lane = iota((8, CB), 0), iota((8, CB), 1)
    seams[0:8, :] = nt(jnp.where(lane == g * GROUP, 1.0, 0.0), u, HI)
    seams[8:16, :] = nt(jnp.where(lane == g * GROUP + GROUP - 1, 1.0, 0.0), u, HI)
    for o in range(NO):
        f = vf[o : o + 1, :]
        a_s[:, lanes(o)] = onehot(f // T, T)
        b_s[:, lanes(o)] = jnp.where(iota((T, L), 0) == f % T, wt[o : o + 1, :], 0.0).astype(BF16)
    via[...] = nt(a_s[...], b_s[...])


def strips_kernel(pos, blocks, node, vf, wt, strips, seams, a_o, send_1, send_2, inj_o):
    for o in range(NO):
        at_node = node[o : o + 1, :].astype(jnp.int32)
        v1, rest = hi_lo(blocks[o * CB : (o + 1) * CB, :])
        v2, v3 = hi_lo(rest)
        v = jnp.concatenate([v3, v2, v1], axis=0).astype(BF16)
        y = jnp.dot(v, onehot(at_node & (CB - 1), CB), preferred_element_type=F32)
        y = y[:CB] + y[CB : 2 * CB] + y[2 * CB :]
        y = jnp.where(iota((CB, L), 0) == (at_node >> 7), y, 0.0)
        inj_o[o : o + 1, :] = jnp.sum(y, axis=0, keepdims=True) * wt[o : o + 1, :]
    j = iota((8, L), 0)
    colid = jnp.where(j < 4, j, T - 8 + j)
    hs, ls = [], []
    for o in range(NO):
        f = vf[o : o + 1, :]
        a_o[:, lanes(o)] = onehot(f // T, T)
        hi, lo = hi_lo(inj_o[o : o + 1, :])
        on = colid == f % T
        hs.append(jnp.where(on, hi, 0.0))
        ls.append(jnp.where(on, lo, 0.0))
    lhs = jnp.concatenate(
        [jnp.concatenate(hs, axis=1), jnp.concatenate(ls, axis=1)], axis=0
    ).astype(BF16)
    inj = nt(lhs, a_o[...])
    inv = strips[8:16, :]
    z = strips[0:8, :] + (inj[0:8] + inj[8:16]) * inv
    low = iota((8, T), 0) < 4
    to_l = jnp.where(low, z, pltpu.roll(inv, 4, 0))
    to_r = jnp.where(low, pltpu.roll(z, 4, 0), inv)
    send_1[:, :T], send_2[:, :T] = pair_order(pos, 1, to_l, to_r)
    send_1[:, T:], send_2[:, T:] = pair_order(pos, 1, seams[0:8, :], seams[8:16, :])


def rhs_kernel(vf, injected, zl, invd, a, z, rims, b_s):
    for o in range(NO):
        hi, lo = hi_lo(injected[o : o + 1, :])
        on = iota((T, L), 0) == vf[o : o + 1, :] % T
        b_s[:, lanes(o)] = jnp.where(on, hi, 0.0).astype(BF16)
        b_s[:, lanes(NO + o)] = jnp.where(on, lo, 0.0).astype(BF16)
    inj = nt(a[...], b_s[:, : NO * L]) + nt(a[...], b_s[:, NO * L :])
    zz = zl[...] + inj * invd[...]
    z[...] = zz
    rims[0:8, :] = zz[0:8]
    rims[8:16, :] = zz[T - 8 :]


def halo_columns(pos, gl, gr):
    place = at(pos, 1, gl)
    parts = []
    for x in (jnp.where(place < NO - 1, gr, 0.0), jnp.where(place > 0, gl, 0.0)):
        a, rest = hi_lo(x)
        b, c = hi_lo(rest)
        parts += [c, b, a]
    j, lane = iota((8, 2 * L), 0), iota((8, 2 * L), 1)
    to_r = jnp.where(lane == jnp.where(j < 4, j, L + j - 4), 1.0, 0.0)
    to_l = jnp.where(lane == jnp.where(j < 4, 124 + j, L + 120 + j), 1.0, 0.0)
    place = jnp.concatenate([to_r] * 3 + [to_l] * 3, axis=0)
    out = tn(jnp.concatenate(parts, axis=0).astype(BF16), place.astype(BF16))
    return out[:, :L], out[:, L:]


def edge_kernel(pos, zr, ir, col_1, col_2, volt, send_1, send_2, corners):
    got_l, got_r = from_pairs(pos, 1, col_1[...], col_2[...])
    zt, it = halo_columns(pos, got_l[:, :L], got_r[:, :L])
    zb, ib = halo_columns(pos, got_l[:, T - L : T], got_r[:, T - L : T])
    for k, x in enumerate((zt[0:16], zb[L - 16 :], it[0:16], ib[L - 16 :])):
        corners[16 * k : 16 * k + 16, :] = x
    low = iota((8, W), 0) < 4
    zt = jnp.concatenate([zr[0:8, :], zt[0:8]], axis=1)
    it = jnp.concatenate([ir[0:8, :], it[0:8]], axis=1)
    zb = jnp.concatenate([zr[8:16, :], zb[L - 8 :]], axis=1)
    ib = jnp.concatenate([ir[8:16, :], ib[L - 8 :]], axis=1)
    to_u = jnp.where(low, zt, pltpu.roll(it, 4, 0))
    to_d = jnp.where(low, pltpu.roll(zb, 4, 0), ib)
    send_1[:, :W], send_2[:, :W] = pair_order(pos, 0, to_u, to_d)
    send_1[:, W:], send_2[:, W:] = pair_order(pos, 0, volt[0:8, :], volt[CB - 8 :, :])


def beside(block):
    n = block.shape[0]
    rows = pltpu.roll(block, 1, 0) + pltpu.roll(block, n - 1, 0)
    return rows + (pltpu.roll(block, 1, 1) + pltpu.roll(block, W - 1, 1))


def near_tiles(ref, start, rows):
    mid = [ref[t, pl.ds(start, rows), :] for t in range(LT + 1)]
    low = [pltpu.roll(m, 1, 1) for m in mid]
    high = [pltpu.roll(m, L - 1, 1) for m in mid]
    lane = iota((rows, L), 1)
    near = []
    for t in range(LT + 1):
        rows_sum = ref[t, pl.ds(start - 1, rows), :] + ref[t, pl.ds(start + 1, rows), :]
        left = jnp.where(lane == 0, low[t - 1], low[t])
        right = jnp.where(lane == L - 1, high[(t + 1) % (LT + 1)], high[t])
        near.append(rows_sum + (left + right))
    return mid, near


def fold(p):
    return (p[:, 0:128] + p[:, 128:256]) + (p[:, 256:384] + p[:, 384:512])


def moments(z, w, n1, n2, dn3, inv):
    d = 1.0 / inv
    dz, dw, dn1, dn2 = d * z, d * w, d * n1, d * n2
    return dz * z, dz * w, dw * w, dw * n1, dn1 * n1, dn1 * n2, dn2 * n2, n2 * dn3


def basis_kernel(pos, z, invd, col_1, col_2, hist, acc_o, ie, ze, we, n1e, n2e, sem):
    zc, ic = halo_columns(pos, *from_pairs(pos, 1, col_1[:, :T], col_2[:, :T]))
    zero = jnp.zeros((OFF, L), F32)
    own = pl.ds(OFF, T)
    for e in (ie, ze, we, n1e, n2e):
        for t in range(LT + 1):
            e[t, 0:OFF, :] = zero
            e[t, OFF + T :, :] = zero
    for t in range(LT):
        ze[t, own, :] = z[:, lanes(t)]
        ie[t, own, :] = invd[:, lanes(t)]
    ze[LT, own, :] = zc
    ie[LT, own, :] = ic
    rows = 128

    def save(k, e):
        copy = pltpu.make_async_copy(e.at[pl.ds(0, LT), own, :], hist.at[k], sem.at[k])
        copy.start()
        return copy

    def apply_to(src, dst, minus):
        def step(i, carry):
            start = pl.multiple_of(OFF + i * rows, 8)
            mid, near = near_tiles(src, start, rows)
            for t in range(LT + 1):
                y = near[t] * ie[t, pl.ds(start, rows), :]
                dst[t, pl.ds(start, rows), :] = mid[t] - y if minus else y
            return carry

        lax.fori_loop(0, T // rows, step, 0)

    copies = [save(0, ze)]
    apply_to(ze, we, True)
    copies.append(save(1, we))
    apply_to(we, n1e, False)
    copies.append(save(2, n1e))
    apply_to(n1e, n2e, False)
    copies.append(save(3, n2e))

    acc = [jnp.zeros((8, L), F32) for _ in range(SUMS)]
    ends = list(range(0, T + 1, 64))
    ends[0], ends[-1] = 8, T - 8
    for low, high in zip(ends[:-1], ends[1:]):
        start, rows = OFF + low, high - low
        n2, dn3 = near_tiles(n2e, start, rows)
        for t in range(LT):
            z8, w8, n18, i8 = (e[t, pl.ds(start, rows), :] for e in (ze, we, n1e, ie))
            for k, p in enumerate(moments(z8, w8, n18, n2[t], dn3[t], i8)):
                for q in range(0, rows, 8):
                    acc[k] = acc[k] + p[q : q + 8]
    for k in range(SUMS):
        acc_o[8 * k : 8 * k + 8, :] = acc[k]
    for copy in copies:
        copy.wait()


def gram_terms(acc):
    g0, q0 = acc[0], acc[1]
    m = acc[2:]
    r = [q0, q0 - m[0], q0 - m[0] - m[1]]
    h = {(0, 0): q0, **{(0, j): RHO[0] * m[j - 1] for j in (1, 2, 3)}}
    b = [g0] + r
    for k in range(3):
        h[0, 0] = h[0, 0] - Q[k] * m[k]
        b[0] = b[0] - Q[k] * r[k]
    for k in range(6):
        f = sum(Q[j] * RHO[k - j] for j in range(3) if 0 <= k - j < 4)
        h[0, 0] = h[0, 0] - f * m[k]
    for j in (1, 2, 3):
        for k in (1, 2, 3):
            h[0, j] = h[0, j] + RHO[k] * m[j - 1 + k]
            if j <= k:
                h[j, k] = m[j + k - 2] - m[j + k - 1]
    out = []
    for p in range(4):
        out += [h[p, q] for q in range(p, 4)] + [b[p]]
    return out


def rim_kernel(pos, z, invd, corners, row_1, row_2, acc_i, rims, part):
    sub = iota((8, W), 0)
    ours = at(pos, 0, sub)
    above, below = (sub >= 4) & (ours > 0), (sub < 4) & (ours < 7)
    top, bot = from_pairs(pos, 0, row_1[:, :W], row_2[:, :W])
    acc = [acc_i[8 * k : 8 * k + 8, :] for k in range(SUMS)]
    for end in (0, 1):
        rows = slice(0, 16) if end == 0 else slice(T - 16, T)
        zc, ic = corners[16 * end : 16 * end + 16, :], corners[32 + 16 * end : 48 + 16 * end, :]
        z16 = jnp.concatenate([z[rows, :], zc], axis=1)
        i16 = jnp.concatenate([invd[rows, :], ic], axis=1)
        if end == 0:
            zb = jnp.concatenate([jnp.where(above, pltpu.roll(top, 4, 0), 0.0), z16], axis=0)
            ib = jnp.concatenate([jnp.where(above, top, 0.0), i16], axis=0)
            own = slice(8, 16)
        else:
            zb = jnp.concatenate([z16, jnp.where(below, bot, 0.0)], axis=0)
            ib = jnp.concatenate([i16, jnp.where(below, pltpu.roll(bot, 4, 0), 0.0)], axis=0)
            own = slice(8, 16)
        w = zb - ib * beside(zb)
        n1 = ib * beside(w)
        n2 = ib * beside(n1)
        near = beside(n2)
        zo, wo, n1o, n2o, dn3, io = (x[own, :T] for x in (zb, w, n1, n2, near, ib))
        for k, p in enumerate(moments(zo, wo, n1o, n2o, dn3, io)):
            acc[k] = acc[k] + fold(p)
        for k, x in enumerate((wo, n1o, n2o)):
            rims[16 * k + 8 * end : 16 * k + 8 * end + 8, :] = x
    terms = gram_terms(acc)
    rows14 = jnp.concatenate(
        [jnp.sum(a, axis=0, keepdims=True) for a in terms] + [jnp.zeros((2, L), F32)], axis=0
    )
    a, rest = hi_lo(rows14)
    b, c = hi_lo(rest)
    parts = jnp.concatenate([c, b, a], axis=0).astype(BF16)
    sums = nt(jnp.ones((8, L), BF16), parts)
    sums = sums[:, 0:16] + sums[:, 16:32] + sums[:, 32:48]
    sums = jnp.concatenate([sums, jnp.zeros((8, L - 16), F32)], axis=1)
    part[...] = sums


def gather_kernel(hist, table, rims, wt, g_o, x_s, slab, slots, sem):
    copies = [pltpu.make_async_copy(hist.at[k], x_s.at[k], sem.at[k]) for k in range(4)]
    ready = pltpu.make_async_copy(table, slots, sem.at[4])
    ready.start()
    for copy in copies:
        copy.start()
    for k in range(4):
        copies[k].wait()
        if k:
            for t in range(LT):
                x_s[k, t, 0:8, :] = rims[16 * k - 16 : 16 * k - 8, lanes(t)]
                x_s[k, t, T - 8 :, :] = rims[16 * k - 8 : 16 * k, lanes(t)]

        def lay(i, carry):
            for b in range(4):
                for t in range(LT):
                    start = pl.multiple_of(i * 32 + 8 * b, 8)
                    to = (i * 32 + 8 * b) * SLAB + 4 * t + k
                    slab[pl.ds(to, 8, stride=SLAB), :] = x_s[k, t, pl.ds(start, 8), :]
            return carry

        lax.fori_loop(0, T // 32, lay, 0)
    lane, sub = iota((8, L), 1), iota((8, L), 0)
    ready.wait()
    for o in range(NO):
        acc = jnp.zeros((8, L), F32)
        for j in range(L):
            x = slab[pl.ds(slots[o, j], 8), :]
            acc = jnp.where(lane == j, pltpu.roll(x, slots[NO + o, j], 1), acc)
        g_o[8 * o : 8 * o + 8, :] = jnp.where(sub < 4, acc * wt[o : o + 1, :], 0.0)


def pack_kernel(g, rows, node, out):
    out[...] = g[...]
    total = jnp.sum(rows[...], axis=0, keepdims=True)
    for o in range(NO):
        out[8 * o + 4 : 8 * o + 5, :] = total
        out[8 * o + 5 : 8 * o + 6, :] = node[o : o + 1, :]


def solve(tot):
    lane = iota((1, L), 1)

    def pick(k):
        return jnp.sum(jnp.where(lane == k, tot, 0.0), axis=1, keepdims=True)

    h, b = {}, []
    k = 0
    for p in range(4):
        for q in range(p, 4):
            h[p, q] = pick(k)
            k += 1
        b.append(pick(k))
        k += 1
    floor = [3e-7 * h[p, p] for p in range(4)]
    inv = []
    for p in range(4):
        inv.append(jnp.where(h[p, p] > floor[p], 1.0 / h[p, p], 0.0))
        for q in range(p + 1, 4):
            f = h[p, q] * inv[p]
            for r in range(q, 4):
                h[q, r] = h[q, r] - f * h[p, r]
            b[q] = b[q] - f * b[p]
    c = [None] * 4
    for p in (3, 2, 1, 0):
        s = b[p]
        for q in range(p + 1, 4):
            s = s - h[p, q] * c[q]
        c[p] = s * inv[p]
    return [c[0]] + [c[k + 1] - Q[k] * c[0] for k in range(3)]


def combine_kernel(hist, ahead, coef, rims, out, h_s, x_s, sem_in, sem_out):
    n = T // STEPS
    load = [
        pltpu.make_async_copy(
            hist.at[pl.ds(1, 3), :, pl.ds(i * n, n), :], h_s.at[i], sem_in.at[i]
        )
        for i in range(STEPS)
    ]
    save = [
        pltpu.make_async_copy(x_s.at[pl.ds(i * n, n), :], out.at[pl.ds(i * n, n), :], sem_out.at[i])
        for i in range(STEPS)
    ]
    for copy in load:
        copy.start()
    c = [coef[k : k + 1, 0:1] for k in range(4)]
    for i in range(STEPS):
        load[i].wait()
        for t in range(LT):
            h = [ahead[0, t, i * n : (i + 1) * n, :]] + [h_s[i, k, t] for k in range(3)]
            x_s[i * n : (i + 1) * n, lanes(t)] = (c[0] * h[0] + c[1] * h[1]) + (
                c[2] * h[2] + c[3] * h[3]
            )
        for end, step, low in ((0, 0, 0), (1, STEPS - 1, n - 8)):
            if i == step:
                for t in range(LT):
                    x = c[0] * ahead[0, t, i * n + low : i * n + low + 8, :]
                    for k in range(3):
                        x += c[k + 1] * rims[16 * k + 8 * end : 16 * k + 8 * end + 8, lanes(t)]
                    x_s[i * n + low : i * n + low + 8, lanes(t)] = x
        save[i].start()
    for copy in save:
        copy.wait()


def coarse_neighbours(pos, u, row_1, row_2, col_1, col_2):
    above, below = from_pairs(pos, 0, row_1, row_2)
    above, below = above[7:8, :], below[0:1, :]
    from_l, from_r = from_pairs(pos, 1, col_1, col_2)
    above = jnp.where(at(pos, 0, above) > 0, above, 0.0)
    below = jnp.where(at(pos, 0, below) < 7, below, 0.0)
    r, lane = iota((CB, CB), 0), iota((CB, CB), 1)
    g, gl = iota((8, CB), 0), iota((8, CB), 1)
    turned_l = jnp.where(g == 0, 0.0, pltpu.roll(from_l, 1, 0))
    turned_r = jnp.where(g == 7, 0.0, pltpu.roll(from_r, 7, 0))
    place = at(pos, 1, from_l)
    from_l = jnp.where(place == 0, turned_l, from_l)
    from_r = jnp.where(place == NO - 1, turned_r, from_r)
    seam_l = tn(from_l, jnp.where(gl == g * GROUP, 1.0, 0.0), HI)
    seam_r = tn(from_r, jnp.where(gl == g * GROUP + GROUP - 1, 1.0, 0.0), HI)
    near = jnp.where(r == 0, above, pltpu.roll(u, 1, 0))
    near += jnp.where(r == CB - 1, below, pltpu.roll(u, CB - 1, 0))
    near += jnp.where(lane % GROUP == 0, seam_l, pltpu.roll(u, 1, 1))
    near += jnp.where(lane % GROUP == GROUP - 1, seam_r, pltpu.roll(u, CB - 1, 1))
    return near


def sweep(u, src, diag, near):
    return u + relaxation * (src - (diag * u - coarse_conductance * near)) / diag


def base_kernel(hist, pos, volt, col_1, col_2, row_1, row_2, near, ahead, sem):
    copy = pltpu.make_async_copy(hist.at[pl.ds(0, 1)], ahead, sem.at[0])
    copy.start()
    near[...] = coarse_neighbours(
        pos, volt[...], row_1[:, W:], row_2[:, W:], col_1[:, T:], col_2[:, T:]
    )
    copy.wait()


def sweep1_kernel(
    pos, arrived, volt, cleak, near, coef, u_o, src_o, cdiag, scale, c1, c2, r1, r2, r_s, c_s, v_s
):
    for o in range(NO):
        h = arrived[8 * o + 5 : 8 * o + 6, :].astype(jnp.int32)
        r_s[:, lanes(o)] = onehot(h >> 7, CB)
        c_s[:, lanes(o)] = onehot(h & (CB - 1), CB)
    diag = 4.0 * coarse_conductance + cleak[...] + via_conductance * nt(r_s[...], c_s[...])
    cdiag[...] = diag
    scale[...] = relaxation / diag
    tot = arrived[4:5, :]
    for o in range(1, NO):
        tot += arrived[8 * o + 4 : 8 * o + 5, :]
    d = solve(tot)
    sub = iota((8, L), 0)
    cf = jnp.zeros((8, L), F32)
    for k in range(4):
        cf = jnp.where(sub == k, d[k], cf)
    coef[...] = cf
    for o in range(NO):
        v = jnp.sum(arrived[8 * o : 8 * o + 8, :] * cf, axis=0, keepdims=True)
        hi, lo = hi_lo(v)
        on = c_s[:, lanes(o)]
        v_s[:, lanes(o)] = on * hi.astype(BF16)
        v_s[:, lanes(NO + o)] = on * lo.astype(BF16)
    src = nt(r_s[...], v_s[:, : NO * L]) + nt(r_s[...], v_s[:, NO * L :])
    u = sweep(volt[...], src, diag, near[...])
    u_o[...] = u
    src_o[...] = src
    g, gl = iota((8, CB), 0), iota((8, CB), 1)
    to_l = nt(jnp.where(gl == g * GROUP, 1.0, 0.0), u, HI)
    to_r = nt(jnp.where(gl == g * GROUP + GROUP - 1, 1.0, 0.0), u, HI)
    c1[...], c2[...] = pair_order(pos, 1, to_l, to_r)
    r1[...], r2[...] = pair_order(pos, 0, u[0:8, :], u[CB - 8 :, :])


def sweep2_kernel(pos, u, src, cdiag, scale, col_1, col_2, row_1, row_2, u_o):
    near = coarse_neighbours(pos, u[...], row_1[...], row_2[...], col_1[...], col_2[...])
    u_o[...] = u[...] + scale[...] * (src[...] - (cdiag[...] * u[...] - coarse_conductance * near))


VM = pl.BlockSpec(memory_space=pltpu.VMEM)
ANY = pl.BlockSpec(memory_space=pltpu.HBM)
vmem = pltpu.MemorySpace.VMEM
hbm = jax.ShapeDtypeStruct


def keep(*args):
    return [pltpu.with_memory_space_constraint(x, pltpu.VMEM) for x in args]


def leave(*args):
    return [pltpu.with_memory_space_constraint(x, pltpu.HBM) for x in args]


def call(body, outs, args, scratch=(), flops=0, any_in=0, any_out=0):
    specs = [ANY] * any_in + [VM] * (len(args) - any_in)
    return pl.pallas_call(
        body,
        out_shape=outs,
        in_specs=specs,
        out_specs=[ANY] * any_out + [VM] * (len(outs) - any_out),
        scratch_shapes=list(scratch),
        cost_estimate=pl.CostEstimate(flops=flops, bytes_accessed=0, transcendentals=0),
        compiler_params=pltpu.CompilerParams(vmem_limit_bytes=20 * 2**20),
    )(*args)


def exchange_columns(first, second):
    n = lax.axis_size(COL)
    near = [(i, i ^ 1) for i in range(n)]
    far = [(i, ((i + 1) ^ 1) - 1 & (n - 1)) for i in range(n)]
    return lax.ppermute(first, COL, near), lax.ppermute(second, COL, far)


def exchange_rows(first, second):
    n, m = lax.axis_size(ROW), lax.axis_size(COL)
    near = [(i, i ^ 1) for i in range(n)]
    far = []
    for i in range(n):
        for k in range(m):
            to = (i, k ^ 1) if i in (0, n - 1) else (((i + 1) ^ 1) - 1, k)
            far.append((i * m + k, to[0] * m + to[1]))
    return lax.ppermute(first, ROW, near), lax.ppermute(second, (ROW, COL), far)


def spread(x, axis=COL):
    return lax.all_to_all(x, axis, split_axis=0, concat_axis=0, tiled=True)


def per_device(load_amp, load_mask, leak, coarse_leak, coarse_init, via_fine, via_coarse, via_count):
    pos = jnp.where(
        lax.broadcasted_iota(jnp.int32, (8, W + CB), 0) == 0, lax.axis_index(ROW), lax.axis_index(COL)
    ).astype(jnp.int32)
    live = jnp.arange(L, dtype=jnp.int32)[None, :] < via_count.reshape(NO, 1)
    wt = jnp.where(live, via_conductance, 0.0).astype(F32)
    fine = via_fine.reshape(NO, L)
    coarse = via_coarse.reshape(NO, L)
    tile, block, slots = vmem((T, T), F32), vmem((CB, CB), F32), vmem((NO, L), F32)
    hot, chot = vmem((T, NO * L), BF16), vmem((CB, NO * L), BF16)
    hots = vmem((T, 2 * NO * L), BF16)
    rim16, side, seam = vmem((16, T), F32), vmem((8, W), F32), vmem((8, CB), F32)
    ext, packed = vmem((LT + 1, EXT, L), F32), ((L, L), F32)
    dmas = pltpu.SemaphoreType.DMA((4,))
    big = 20_000_000_000

    blocks = jnp.broadcast_to(coarse_init[None], (NO, CB, CB)).reshape(NO * CB, CB)
    blocks = spread(blocks)
    node, where, volt, fine, seams, via = call(
        parts_kernel,
        [slots, pltpu.MemorySpace.HBM((2 * NO, L), jnp.int32), block,
         vmem((NO, L), jnp.int32), vmem((16, CB), F32), pltpu.MemorySpace.HBM((T, T), F32)],
        leave(coarse_init, fine, coarse) + keep(wt), [hot, hot], flops=big,
    )
    zl, invd, strips, irims = call(
        diag_kernel, [tile, tile, rim16, rim16],
        leave(load_amp, load_mask, leak, via),
        [tile, vmem((T, T), jnp.int32), tile, tile, dmas], flops=big, any_in=4,
    )
    a, send_1, send_2, injected = call(
        strips_kernel, [hot, side, side, slots],
        keep(pos, blocks, node, fine, wt, strips, seams),
    )
    col_1, col_2 = exchange_columns(send_1, send_2)
    z, zrims = call(
        rhs_kernel, [tile, rim16], keep(fine, injected, zl, invd, a), [hots], flops=big
    )
    rim = vmem((8, W + CB), F32)
    send_1, send_2, corners = call(
        edge_kernel, [rim, rim, vmem((64, L), F32)],
        keep(pos, zrims, irims, col_1, col_2, volt)    )
    row_1, row_2 = exchange_rows(send_1, send_2)
    hist, acc = call(
        basis_kernel, [pltpu.MemorySpace.HBM((4, LT, T, L), F32), vmem((8 * SUMS, L), F32)], keep(pos, z, invd, col_1, col_2),
        [ext] * 5 + [dmas], flops=big, any_out=1,
    )
    rims, part = call(
        rim_kernel, [vmem((48, T), F32), vmem((8, L), F32)],
        keep(pos, z, invd, corners, row_1, row_2, acc)    )
    rows = spread(part, ROW)
    g = call(
        gather_kernel, [vmem(*packed)], leave(hist, where) + keep(rims, wt),
        [vmem((4, LT, T, L), F32), vmem((T * SLAB + 8, L), F32),
         pltpu.MemorySpace.SMEM((2 * NO, L), jnp.int32), pltpu.SemaphoreType.DMA((5,))],
        flops=big, any_in=2,
    )[0]
    arrived = spread(call(pack_kernel, [vmem(*packed)], keep(g, rows, node))[0])
    near, ahead = call(
        base_kernel, [block, vmem((1, LT, T, L), F32)],
        leave(hist) + keep(pos, volt, col_1, col_2, row_1, row_2), [dmas], flops=big, any_in=1,
    )
    coef, u, src, cdiag, scale, c1, c2, r1, r2 = call(
        sweep1_kernel, [seam, block, block, block, block, seam, seam, seam, seam],
        keep(pos, arrived, volt, coarse_leak, near),
        [chot, chot, vmem((CB, 2 * NO * L), BF16)],
    )
    c1, c2 = exchange_columns(c1, c2)
    r1, r2 = exchange_rows(r1, r2)
    fine_drop = call(
        combine_kernel, [pltpu.MemorySpace.HBM((T, T), F32)], leave(hist) + keep(ahead, coef, rims),
        [vmem((STEPS, 3, LT, T // STEPS, L), F32), tile, pltpu.SemaphoreType.DMA((STEPS,)),
         pltpu.SemaphoreType.DMA((STEPS,))], flops=big // 4, any_in=1, any_out=1,
    )[0]
    coarse_drop = call(
        sweep2_kernel, [hbm((CB, CB), F32)], keep(pos, u, src, cdiag, scale, c1, c2, r1, r2)    )[0]
    return fine_drop, coarse_drop


def solution(mesh):
    spec = P(ROW, COL)

    return jax.shard_map(
        per_device, mesh=mesh, in_specs=(spec,) * 8, out_specs=(spec, spec), check_vma=False
    )
```

```python
import jax
import jax.numpy as jnp
from jax import lax
from jax.experimental import pallas as pl
from jax.experimental.pallas import tpu as pltpu
from jax.sharding import PartitionSpec as P


F32 = jnp.float32
BF16 = jnp.bfloat16
HI = lax.Precision.HIGHEST
ROW, COL = "row", "col"

GROUP = 16
via_conductance = 2.0
coarse_conductance = 4.0
relaxation = 0.8

T = 512
CB = 128
NO = 16
L = 128
OFF = 16
EXT = OFF + T + 16
W = T + L

Q = (1.09375, 1.765625, 1.28125)
RHO = (1.0 - Q[0], Q[0] - Q[1], Q[1] - Q[2], Q[2])
LT = T // L
SLAB = 4 * LT + 1
SUMS = 8
AHEAD = 1
STEPS = 8


def iota(shape, dim):
    return lax.broadcasted_iota(jnp.int32, shape, dim)


def nt(a, b, precision=None):
    return lax.dot_general(
        a, b, (((1,), (1,)), ((), ())), precision=precision, preferred_element_type=F32
    )


def tn(a, b, precision=None):
    return lax.dot_general(
        a, b, (((0,), (0,)), ((), ())), precision=precision, preferred_element_type=F32
    )


def onehot(idx, n):
    return jnp.where(iota((n, idx.shape[1]), 0) == idx, 1.0, 0.0).astype(BF16)


def hi_lo(x):
    hi = x.astype(BF16).astype(F32)
    return hi, x - hi


def lanes(o):
    return slice(o * L, (o + 1) * L)


def at(pos, k, like):
    return jnp.broadcast_to(pos[k : k + 1, : like.shape[1]], like.shape)


def pair_order(pos, k, low, high):
    even = (at(pos, k, low) & 1) == 0
    return jnp.where(even, high, low), jnp.where(even, low, high)


def from_pairs(pos, k, first, second):
    even = (at(pos, k, first) & 1) == 0
    return jnp.where(even, second, first), jnp.where(even, first, second)


def diag_kernel(
    amp, mask, leak, via, zl, invd, strips, rims, amp_s, mask_s, leak_s, via_s, sem
):
    copies = [
        pltpu.make_async_copy(x, y, sem.at[k])
        for k, (x, y) in enumerate(
            ((leak, leak_s), (via, via_s), (amp, amp_s), (mask, mask_s))
        )
    ]
    for copy in copies:
        copy.start()
    for copy in copies:
        copy.wait()
    inv = 1.0 / (4.0 + leak_s[...] + via_s[...])
    z = amp_s[...] * mask_s[...].astype(F32) * inv
    zl[...] = z
    invd[...] = inv
    j, lane = iota((8, 2 * L), 0), iota((8, 2 * L), 1)
    pick = jnp.where(lane == jnp.where(j < 4, j, 2 * L - 8 + j), 1.0, 0.0).astype(BF16)
    for k, x in enumerate((z, inv)):
        hi, rest = hi_lo(jnp.concatenate([x[:, :L], x[:, T - L :]], axis=1))
        mid, lo = hi_lo(rest)
        strips[8 * k : 8 * k + 8, :] = (
            nt(pick, lo.astype(BF16)) + nt(pick, mid.astype(BF16)) + nt(pick, hi.astype(BF16))
        )
    rims[0:8, :] = inv[0:8]
    rims[8:16, :] = inv[T - 8 :]


def copies_kernel(volt, out, sem):
    copies = [
        pltpu.make_async_copy(volt, out.at[pl.ds(o * CB, CB), :], sem.at[o]) for o in range(NO)
    ]
    for copy in copies:
        copy.start()
    for copy in copies:
        copy.wait()


def parts_kernel(vf, vc, wt, node, slots, vf_o, via, a_s, b_s):
    f = vf[...]
    vf_o[...] = f
    slots[0:NO, :] = (f >> 9) * SLAB + ((f >> 7) & 3) * 4
    slots[NO:, :] = (iota((NO, L), 1) - f) & (L - 1)
    place = ((vc[...] >> 11) << 7) | (vc[...] & (CB - 1))
    node[...] = jnp.where(wt[...] > 0.0, place.astype(F32), -1.0)
    for o in range(NO):
        f = vf[o : o + 1, :]
        a_s[:, lanes(o)] = onehot(f // T, T)
        b_s[:, lanes(o)] = jnp.where(iota((T, L), 0) == f % T, wt[o : o + 1, :], 0.0).astype(BF16)
    via[...] = nt(a_s[...], b_s[...])


def strips_kernel(pos, blocks, node, vf, wt, strips, a_o, send_1, send_2, inj_o):
    for o in range(NO):
        at_node = node[o : o + 1, :].astype(jnp.int32)
        v1, rest = hi_lo(blocks[o * CB : (o + 1) * CB, :])
        v2, v3 = hi_lo(rest)
        v = jnp.concatenate([v3, v2, v1], axis=0).astype(BF16)
        y = jnp.dot(v, onehot(at_node & (CB - 1), CB), preferred_element_type=F32)
        y = y[:CB] + y[CB : 2 * CB] + y[2 * CB :]
        y = jnp.where(iota((CB, L), 0) == (at_node >> 7), y, 0.0)
        inj_o[o : o + 1, :] = jnp.sum(y, axis=0, keepdims=True) * wt[o : o + 1, :]
    j = iota((8, L), 0)
    colid = jnp.where(j < 4, j, T - 8 + j)
    hs, ls = [], []
    for o in range(NO):
        f = vf[o : o + 1, :]
        a_o[:, lanes(o)] = onehot(f // T, T)
        hi, lo = hi_lo(inj_o[o : o + 1, :])
        on = colid == f % T
        hs.append(jnp.where(on, hi, 0.0))
        ls.append(jnp.where(on, lo, 0.0))
    lhs = jnp.concatenate(
        [jnp.concatenate(hs, axis=1), jnp.concatenate(ls, axis=1)], axis=0
    ).astype(BF16)
    inj = nt(lhs, a_o[...])
    inv = strips[8:16, :]
    z = strips[0:8, :] + (inj[0:8] + inj[8:16]) * inv
    low = iota((8, T), 0) < 4
    to_l = jnp.where(low, z, pltpu.roll(inv, 4, 0))
    to_r = jnp.where(low, pltpu.roll(z, 4, 0), inv)
    send_1[...], send_2[...] = pair_order(pos, 1, to_l, to_r)


def rhs_kernel(vf, injected, zl, invd, a, z, rims, b_s):
    for o in range(NO):
        hi, lo = hi_lo(injected[o : o + 1, :])
        on = iota((T, L), 0) == vf[o : o + 1, :] % T
        b_s[:, lanes(o)] = jnp.where(on, hi, 0.0).astype(BF16)
        b_s[:, lanes(NO + o)] = jnp.where(on, lo, 0.0).astype(BF16)
    inj = nt(a[...], b_s[:, : NO * L]) + nt(a[...], b_s[:, NO * L :])
    zz = zl[...] + inj * invd[...]
    z[...] = zz
    rims[0:8, :] = zz[0:8]
    rims[8:16, :] = zz[T - 8 :]


def halo_columns(pos, gl, gr):
    place = at(pos, 1, gl)
    parts = []
    for x in (jnp.where(place < NO - 1, gr, 0.0), jnp.where(place > 0, gl, 0.0)):
        a, rest = hi_lo(x)
        b, c = hi_lo(rest)
        parts += [c, b, a]
    j, lane = iota((8, 2 * L), 0), iota((8, 2 * L), 1)
    to_r = jnp.where(lane == jnp.where(j < 4, j, L + j - 4), 1.0, 0.0)
    to_l = jnp.where(lane == jnp.where(j < 4, 124 + j, L + 120 + j), 1.0, 0.0)
    place = jnp.concatenate([to_r] * 3 + [to_l] * 3, axis=0)
    out = tn(jnp.concatenate(parts, axis=0).astype(BF16), place.astype(BF16))
    return out[:, :L], out[:, L:]


def edge_kernel(pos, zr, ir, col_1, col_2, volt, send_1, send_2, corners):
    got_l, got_r = from_pairs(pos, 1, col_1[...], col_2[...])
    zt, it = halo_columns(pos, got_l[:, :L], got_r[:, :L])
    zb, ib = halo_columns(pos, got_l[:, T - L : T], got_r[:, T - L : T])
    for k, x in enumerate((zt[0:16], zb[L - 16 :], it[0:16], ib[L - 16 :])):
        corners[16 * k : 16 * k + 16, :] = x
    low = iota((8, W), 0) < 4
    zt = jnp.concatenate([zr[0:8, :], zt[0:8]], axis=1)
    it = jnp.concatenate([ir[0:8, :], it[0:8]], axis=1)
    zb = jnp.concatenate([zr[8:16, :], zb[L - 8 :]], axis=1)
    ib = jnp.concatenate([ir[8:16, :], ib[L - 8 :]], axis=1)
    to_u = jnp.where(low, zt, pltpu.roll(it, 4, 0))
    to_d = jnp.where(low, pltpu.roll(zb, 4, 0), ib)
    send_1[:, :W], send_2[:, :W] = pair_order(pos, 0, to_u, to_d)
    send_1[:, W:], send_2[:, W:] = pair_order(pos, 0, volt[0:8, :], volt[CB - 8 :, :])


def beside(block):
    n = block.shape[0]
    rows = pltpu.roll(block, 1, 0) + pltpu.roll(block, n - 1, 0)
    return rows + (pltpu.roll(block, 1, 1) + pltpu.roll(block, W - 1, 1))


def near_tiles(ref, start, rows):
    mid = [ref[t, pl.ds(start, rows), :] for t in range(LT + 1)]
    low = [pltpu.roll(m, 1, 1) for m in mid]
    high = [pltpu.roll(m, L - 1, 1) for m in mid]
    lane = iota((rows, L), 1)
    near = []
    for t in range(LT + 1):
        rows_sum = ref[t, pl.ds(start - 1, rows), :] + ref[t, pl.ds(start + 1, rows), :]
        left = jnp.where(lane == 0, low[t - 1], low[t])
        right = jnp.where(lane == L - 1, high[(t + 1) % (LT + 1)], high[t])
        near.append(rows_sum + (left + right))
    return mid, near


def fold(p):
    return (p[:, 0:128] + p[:, 128:256]) + (p[:, 256:384] + p[:, 384:512])


def moments(z, w, n1, n2, dn3, inv):
    d = 1.0 / inv
    dz, dw, dn1, dn2 = d * z, d * w, d * n1, d * n2
    return dz * z, dz * w, dw * w, dw * n1, dn1 * n1, dn1 * n2, dn2 * n2, n2 * dn3


def basis_kernel(pos, z, invd, col_1, col_2, hist, acc_o, ie, ze, we, n1e, n2e, sem):
    zc, ic = halo_columns(pos, *from_pairs(pos, 1, col_1[:, :T], col_2[:, :T]))
    zero = jnp.zeros((OFF, L), F32)
    own = pl.ds(OFF, T)
    for e in (ie, ze, we, n1e, n2e):
        for t in range(LT + 1):
            e[t, 0:OFF, :] = zero
            e[t, OFF + T :, :] = zero
    for t in range(LT):
        ze[t, own, :] = z[:, lanes(t)]
        ie[t, own, :] = invd[:, lanes(t)]
    ze[LT, own, :] = zc
    ie[LT, own, :] = ic
    rows = 128

    def save(k, e):
        copy = pltpu.make_async_copy(e.at[pl.ds(0, LT), own, :], hist.at[k], sem.at[k])
        copy.start()
        return copy

    def apply_to(src, dst, minus):
        def step(i, carry):
            start = pl.multiple_of(OFF + i * rows, 8)
            mid, near = near_tiles(src, start, rows)
            for t in range(LT + 1):
                y = near[t] * ie[t, pl.ds(start, rows), :]
                dst[t, pl.ds(start, rows), :] = mid[t] - y if minus else y
            return carry

        lax.fori_loop(0, T // rows, step, 0)

    copies = [save(0, ze)]
    apply_to(ze, we, True)
    copies.append(save(1, we))
    apply_to(we, n1e, False)
    copies.append(save(2, n1e))
    apply_to(n1e, n2e, False)
    copies.append(save(3, n2e))

    acc = [jnp.zeros((8, L), F32) for _ in range(SUMS)]
    ends = list(range(0, T + 1, 64))
    ends[0], ends[-1] = 8, T - 8
    for low, high in zip(ends[:-1], ends[1:]):
        start, rows = OFF + low, high - low
        n2, dn3 = near_tiles(n2e, start, rows)
        for t in range(LT):
            z8, w8, n18, i8 = (e[t, pl.ds(start, rows), :] for e in (ze, we, n1e, ie))
            for k, p in enumerate(moments(z8, w8, n18, n2[t], dn3[t], i8)):
                for q in range(0, rows, 8):
                    acc[k] = acc[k] + p[q : q + 8]
    for k in range(SUMS):
        acc_o[8 * k : 8 * k + 8, :] = acc[k]
    for copy in copies:
        copy.wait()


def gram_terms(acc):
    g0, q0 = acc[0], acc[1]
    m = acc[2:]
    r = [q0, q0 - m[0], q0 - m[0] - m[1]]
    h = {(0, 0): q0, **{(0, j): RHO[0] * m[j - 1] for j in (1, 2, 3)}}
    b = [g0] + r
    for k in range(3):
        h[0, 0] = h[0, 0] - Q[k] * m[k]
        b[0] = b[0] - Q[k] * r[k]
    for k in range(6):
        f = sum(Q[j] * RHO[k - j] for j in range(3) if 0 <= k - j < 4)
        h[0, 0] = h[0, 0] - f * m[k]
    for j in (1, 2, 3):
        for k in (1, 2, 3):
            h[0, j] = h[0, j] + RHO[k] * m[j - 1 + k]
            if j <= k:
                h[j, k] = m[j + k - 2] - m[j + k - 1]
    out = []
    for p in range(4):
        out += [h[p, q] for q in range(p, 4)] + [b[p]]
    return out


def rim_kernel(pos, z, invd, corners, row_1, row_2, acc_i, rims, part):
    sub = iota((8, W), 0)
    ours = at(pos, 0, sub)
    above, below = (sub >= 4) & (ours > 0), (sub < 4) & (ours < 7)
    top, bot = from_pairs(pos, 0, row_1[:, :W], row_2[:, :W])
    acc = [acc_i[8 * k : 8 * k + 8, :] for k in range(SUMS)]
    for end in (0, 1):
        rows = slice(0, 16) if end == 0 else slice(T - 16, T)
        zc, ic = corners[16 * end : 16 * end + 16, :], corners[32 + 16 * end : 48 + 16 * end, :]
        z16 = jnp.concatenate([z[rows, :], zc], axis=1)
        i16 = jnp.concatenate([invd[rows, :], ic], axis=1)
        if end == 0:
            zb = jnp.concatenate([jnp.where(above, pltpu.roll(top, 4, 0), 0.0), z16], axis=0)
            ib = jnp.concatenate([jnp.where(above, top, 0.0), i16], axis=0)
            own = slice(8, 16)
        else:
            zb = jnp.concatenate([z16, jnp.where(below, bot, 0.0)], axis=0)
            ib = jnp.concatenate([i16, jnp.where(below, pltpu.roll(bot, 4, 0), 0.0)], axis=0)
            own = slice(8, 16)
        w = zb - ib * beside(zb)
        n1 = ib * beside(w)
        n2 = ib * beside(n1)
        near = beside(n2)
        zo, wo, n1o, n2o, dn3, io = (x[own, :T] for x in (zb, w, n1, n2, near, ib))
        for k, p in enumerate(moments(zo, wo, n1o, n2o, dn3, io)):
            acc[k] = acc[k] + fold(p)
        for k, x in enumerate((wo, n1o, n2o)):
            rims[16 * k + 8 * end : 16 * k + 8 * end + 8, :] = x
    terms = gram_terms(acc)
    rows14 = jnp.concatenate(
        [jnp.sum(a, axis=0, keepdims=True) for a in terms] + [jnp.zeros((2, L), F32)], axis=0
    )
    a, rest = hi_lo(rows14)
    b, c = hi_lo(rest)
    parts = jnp.concatenate([c, b, a], axis=0).astype(BF16)
    sums = nt(jnp.ones((8, L), BF16), parts)
    sums = sums[:, 0:16] + sums[:, 16:32] + sums[:, 32:48]
    sums = jnp.concatenate([sums, jnp.zeros((8, L - 16), F32)], axis=1)
    part[...] = sums


def gather_kernel(hist, table, rims, wt, g_o, x_s, slab, slots, sem):
    copies = [pltpu.make_async_copy(hist.at[k], x_s.at[k], sem.at[k]) for k in range(4)]
    ready = pltpu.make_async_copy(table, slots, sem.at[4])
    ready.start()
    for copy in copies:
        copy.start()
    for k in range(4):
        copies[k].wait()
        if k:
            for t in range(LT):
                x_s[k, t, 0:8, :] = rims[16 * k - 16 : 16 * k - 8, lanes(t)]
                x_s[k, t, T - 8 :, :] = rims[16 * k - 8 : 16 * k, lanes(t)]

        def lay(i, carry):
            for b in range(4):
                for t in range(LT):
                    start = pl.multiple_of(i * 32 + 8 * b, 8)
                    to = (i * 32 + 8 * b) * SLAB + 4 * t + k
                    slab[pl.ds(to, 8, stride=SLAB), :] = x_s[k, t, pl.ds(start, 8), :]
            return carry

        lax.fori_loop(0, T // 32, lay, 0)
    lane, sub = iota((8, L), 1), iota((8, L), 0)
    ready.wait()
    for o in range(NO):
        acc = jnp.zeros((8, L), F32)
        for j in range(L):
            x = slab[pl.ds(slots[o, j], 8), :]
            acc = jnp.where(lane == j, pltpu.roll(x, slots[NO + o, j], 1), acc)
        g_o[8 * o : 8 * o + 8, :] = jnp.where(sub < 4, acc * wt[o : o + 1, :], 0.0)


def pack_kernel(g, rows, node, out):
    out[...] = g[...]
    total = jnp.sum(rows[...], axis=0, keepdims=True)
    for o in range(NO):
        out[8 * o + 4 : 8 * o + 5, :] = total
        out[8 * o + 5 : 8 * o + 6, :] = node[o : o + 1, :]


def solve(tot):
    lane = iota((1, L), 1)

    def pick(k):
        return jnp.sum(jnp.where(lane == k, tot, 0.0), axis=1, keepdims=True)

    h, b = {}, []
    k = 0
    for p in range(4):
        for q in range(p, 4):
            h[p, q] = pick(k)
            k += 1
        b.append(pick(k))
        k += 1
    floor = [3e-7 * h[p, p] for p in range(4)]
    inv = []
    for p in range(4):
        inv.append(jnp.where(h[p, p] > floor[p], 1.0 / h[p, p], 0.0))
        for q in range(p + 1, 4):
            f = h[p, q] * inv[p]
            for r in range(q, 4):
                h[q, r] = h[q, r] - f * h[p, r]
            b[q] = b[q] - f * b[p]
    c = [None] * 4
    for p in (3, 2, 1, 0):
        s = b[p]
        for q in range(p + 1, 4):
            s = s - h[p, q] * c[q]
        c[p] = s * inv[p]
    return [c[0]] + [c[k + 1] - Q[k] * c[0] for k in range(3)]


def combine_kernel(hist, ahead, coef, rims, out, h_s, x_s, sem_in, sem_out):
    n = T // STEPS
    load = [
        pltpu.make_async_copy(
            hist.at[pl.ds(AHEAD, 4 - AHEAD), :, pl.ds(i * n, n), :], h_s.at[i], sem_in.at[i]
        )
        for i in range(STEPS)
    ]
    save = [
        pltpu.make_async_copy(x_s.at[pl.ds(i * n, n), :], out.at[pl.ds(i * n, n), :], sem_out.at[i])
        for i in range(STEPS)
    ]
    for copy in load:
        copy.start()
    c = [coef[k : k + 1, 0:1] for k in range(4)]
    for i in range(STEPS):
        load[i].wait()
        for t in range(LT):
            h = [ahead[k, t, i * n : (i + 1) * n, :] for k in range(AHEAD)]
            h += [h_s[i, k, t] for k in range(4 - AHEAD)]
            x_s[i * n : (i + 1) * n, lanes(t)] = (c[0] * h[0] + c[1] * h[1]) + (
                c[2] * h[2] + c[3] * h[3]
            )
        for end, step, low in ((0, 0, 0), (1, STEPS - 1, n - 8)):
            if i == step:
                for t in range(LT):
                    x = c[0] * ahead[0, t, i * n + low : i * n + low + 8, :]
                    for k in range(3):
                        x += c[k + 1] * rims[16 * k + 8 * end : 16 * k + 8 * end + 8, lanes(t)]
                    x_s[i * n + low : i * n + low + 8, lanes(t)] = x
        save[i].start()
    for copy in save:
        copy.wait()


def coarse_neighbours(pos, u, row_1, row_2, from_l, from_r):
    above, below = from_pairs(pos, 0, row_1, row_2)
    above, below = above[7:8, :], below[0:1, :]
    above = jnp.where(at(pos, 0, above) > 0, above, 0.0)
    below = jnp.where(at(pos, 0, below) < 7, below, 0.0)
    r, lane = iota((CB, CB), 0), iota((CB, CB), 1)
    g, gl = iota((8, CB), 0), iota((8, CB), 1)
    turned_l = jnp.where(g == 0, 0.0, pltpu.roll(from_l, 1, 0))
    turned_r = jnp.where(g == 7, 0.0, pltpu.roll(from_r, 7, 0))
    place = at(pos, 1, from_l)
    from_l = jnp.where(place == 0, turned_l, from_l)
    from_r = jnp.where(place == NO - 1, turned_r, from_r)
    seam_l = tn(from_l, jnp.where(gl == g * GROUP, 1.0, 0.0), HI)
    seam_r = tn(from_r, jnp.where(gl == g * GROUP + GROUP - 1, 1.0, 0.0), HI)
    near = jnp.where(r == 0, above, pltpu.roll(u, 1, 0))
    near += jnp.where(r == CB - 1, below, pltpu.roll(u, CB - 1, 0))
    near += jnp.where(lane % GROUP == 0, seam_l, pltpu.roll(u, 1, 1))
    near += jnp.where(lane % GROUP == GROUP - 1, seam_r, pltpu.roll(u, CB - 1, 1))
    return near


def sweep(u, src, diag, near):
    return u + relaxation * (src - (diag * u - coarse_conductance * near)) / diag


def base_kernel(hist, blocks, pos, volt, row_1, row_2, near, ahead, b_s, sem):
    copy = pltpu.make_async_copy(hist.at[pl.ds(0, AHEAD)], ahead, sem.at[0])
    drops = pltpu.make_async_copy(blocks, b_s, sem.at[1])
    drops.start()
    copy.start()
    drops.wait()
    left, right = jnp.zeros((CB, CB), F32), jnp.zeros((CB, CB), F32)
    for o in range(NO):
        block = b_s[o * CB : (o + 1) * CB, :]
        ours = at(pos, 1, block)
        left = jnp.where(ours == (o + 1) % NO, block, left)
        right = jnp.where(ours == (o - 1) % NO, block, right)
    g, lane = iota((8, CB), 0), iota((8, CB), 1)
    from_l = nt(jnp.where(lane == g * GROUP + GROUP - 1, 1.0, 0.0), left, HI)
    from_r = nt(jnp.where(lane == g * GROUP, 1.0, 0.0), right, HI)
    near[...] = coarse_neighbours(pos, volt[...], row_1[:, W:], row_2[:, W:], from_l, from_r)
    copy.wait()


def sweep1_kernel(
    pos, arrived, volt, cleak, near, coef, u_o, src_o, cdiag, scale, c1, c2, r1, r2, r_s, c_s, v_s
):
    for o in range(NO):
        h = arrived[8 * o + 5 : 8 * o + 6, :].astype(jnp.int32)
        r_s[:, lanes(o)] = onehot(h >> 7, CB)
        c_s[:, lanes(o)] = onehot(h & (CB - 1), CB)
    diag = 4.0 * coarse_conductance + cleak[...] + via_conductance * nt(r_s[...], c_s[...])
    cdiag[...] = diag
    scale[...] = relaxation / diag
    tot = arrived[4:5, :]
    for o in range(1, NO):
        tot += arrived[8 * o + 4 : 8 * o + 5, :]
    d = solve(tot)
    sub = iota((8, L), 0)
    cf = jnp.zeros((8, L), F32)
    for k in range(4):
        cf = jnp.where(sub == k, d[k], cf)
    coef[...] = cf
    for o in range(NO):
        v = jnp.sum(arrived[8 * o : 8 * o + 8, :] * cf, axis=0, keepdims=True)
        hi, lo = hi_lo(v)
        on = c_s[:, lanes(o)]
        v_s[:, lanes(o)] = on * hi.astype(BF16)
        v_s[:, lanes(NO + o)] = on * lo.astype(BF16)
    src = nt(r_s[...], v_s[:, : NO * L]) + nt(r_s[...], v_s[:, NO * L :])
    u = sweep(volt[...], src, diag, near[...])
    u_o[...] = u
    src_o[...] = src
    g, gl = iota((8, CB), 0), iota((8, CB), 1)
    to_l = nt(jnp.where(gl == g * GROUP, 1.0, 0.0), u, HI)
    to_r = nt(jnp.where(gl == g * GROUP + GROUP - 1, 1.0, 0.0), u, HI)
    c1[...], c2[...] = pair_order(pos, 1, to_l, to_r)
    r1[...], r2[...] = pair_order(pos, 0, u[0:8, :], u[CB - 8 :, :])


def sweep2_kernel(pos, u, src, cdiag, scale, col_1, col_2, row_1, row_2, u_o):
    from_l, from_r = from_pairs(pos, 1, col_1[...], col_2[...])
    near = coarse_neighbours(pos, u[...], row_1[...], row_2[...], from_l, from_r)
    u_o[...] = u[...] + scale[...] * (src[...] - (cdiag[...] * u[...] - coarse_conductance * near))


VM = pl.BlockSpec(memory_space=pltpu.VMEM)
ANY = pl.BlockSpec(memory_space=pltpu.HBM)
vmem = pltpu.MemorySpace.VMEM
hbm = jax.ShapeDtypeStruct


def keep(*args):
    return [pltpu.with_memory_space_constraint(x, pltpu.VMEM) for x in args]


def leave(*args):
    return [pltpu.with_memory_space_constraint(x, pltpu.HBM) for x in args]


def call(body, outs, args, scratch=(), flops=0, any_in=0, any_out=0):
    specs = [ANY] * any_in + [VM] * (len(args) - any_in)
    return pl.pallas_call(
        body,
        out_shape=outs,
        in_specs=specs,
        out_specs=[ANY] * any_out + [VM] * (len(outs) - any_out),
        scratch_shapes=list(scratch),
        cost_estimate=pl.CostEstimate(flops=flops, bytes_accessed=0, transcendentals=0),
        compiler_params=pltpu.CompilerParams(vmem_limit_bytes=20 * 2**20),
    )(*args)


def pairs(axis, other, ring):
    n, m = lax.axis_size(axis), lax.axis_size(other)
    near = [(i, i ^ 1) for i in range(n)]
    far = []
    for i in range(n):
        for k in range(m):
            to = (((i + 1) ^ 1) - 1 & (n - 1), k)
            if not ring and i in (0, n - 1):
                to = (i, k ^ 1)
            ids = [(p, q) if axis == ROW else (q, p) for p, q in ((i, k), to)]
            far.append(tuple(r * lax.axis_size(COL) + c for r, c in ids))
    return near, sorted(far)


def exchange(axis, first, second, ring=False):
    near, far = pairs(axis, COL if axis == ROW else ROW, ring)
    if ring:
        n = lax.axis_size(axis)
        far = [(i, ((i + 1) ^ 1) - 1 & (n - 1)) for i in range(n)]
        return lax.ppermute(first, axis, near), lax.ppermute(second, axis, far)
    return lax.ppermute(first, axis, near), lax.ppermute(second, (ROW, COL), far)


def spread(x, axis=COL):
    return lax.all_to_all(x, axis, split_axis=0, concat_axis=0, tiled=True)


def per_device(load_amp, load_mask, leak, coarse_leak, coarse_init, via_fine, via_coarse, via_count):
    pos = jnp.where(
        lax.broadcasted_iota(jnp.int32, (8, W + CB), 0) == 0, lax.axis_index(ROW), lax.axis_index(COL)
    ).astype(jnp.int32)
    live = jnp.arange(L, dtype=jnp.int32)[None, :] < via_count.reshape(NO, 1)
    wt = jnp.where(live, via_conductance, 0.0).astype(F32)
    fine = via_fine.reshape(NO, L)
    coarse = via_coarse.reshape(NO, L)
    tile, block, slots = vmem((T, T), F32), vmem((CB, CB), F32), vmem((NO, L), F32)
    hot, chot = vmem((T, NO * L), BF16), vmem((CB, NO * L), BF16)
    hots = vmem((T, 2 * NO * L), BF16)
    rim16, side, seam = vmem((16, T), F32), vmem((8, T), F32), vmem((8, CB), F32)
    ext, packed = vmem((LT + 1, EXT, L), F32), ((L, L), F32)
    dmas = pltpu.SemaphoreType.DMA((4,))
    big = 20_000_000_000

    blocks = call(
        copies_kernel, [pltpu.MemorySpace.HBM((NO * CB, CB), F32)], leave(coarse_init),
        [pltpu.SemaphoreType.DMA((NO,))], any_out=1,
    )[0]
    blocks = spread(blocks)
    node, where, fine, via = call(
        parts_kernel,
        [slots, pltpu.MemorySpace.HBM((2 * NO, L), jnp.int32),
         vmem((NO, L), jnp.int32), pltpu.MemorySpace.HBM((T, T), F32)],
        leave(fine, coarse) + keep(wt), [hot, hot], flops=big,
    )
    zl, invd, strips, irims = call(
        diag_kernel, [tile, tile, rim16, rim16],
        leave(load_amp, load_mask, leak, via),
        [tile, vmem((T, T), jnp.int32), tile, tile, dmas], flops=big, any_in=4,
    )
    a, send_1, send_2, injected = call(
        strips_kernel, [hot, side, side, slots],
        keep(pos, blocks, node, fine, wt, strips),
    )
    col_1, col_2 = exchange(COL, send_1, send_2)
    z, zrims = call(
        rhs_kernel, [tile, rim16], keep(fine, injected, zl, invd, a), [hots], flops=big
    )
    rim = vmem((8, W + CB), F32)
    send_1, send_2, corners = call(
        edge_kernel, [rim, rim, vmem((64, L), F32)],
        keep(pos, zrims, irims, col_1, col_2, coarse_init)    )
    row_1, row_2 = exchange(ROW, send_1, send_2)
    hist, acc = call(
        basis_kernel, [pltpu.MemorySpace.HBM((4, LT, T, L), F32), vmem((8 * SUMS, L), F32)], keep(pos, z, invd, col_1, col_2),
        [ext] * 5 + [dmas], flops=big, any_out=1,
    )
    rims, part = call(
        rim_kernel, [vmem((48, T), F32), vmem((8, L), F32)],
        keep(pos, z, invd, corners, row_1, row_2, acc)    )
    rows = spread(part, ROW)
    g = call(
        gather_kernel, [vmem(*packed)], leave(hist, where) + keep(rims, wt),
        [vmem((4, LT, T, L), F32), vmem((T * SLAB + 8, L), F32),
         pltpu.MemorySpace.SMEM((2 * NO, L), jnp.int32), pltpu.SemaphoreType.DMA((5,))],
        flops=big, any_in=2,
    )[0]
    arrived = spread(call(pack_kernel, [vmem(*packed)], keep(g, rows, node))[0])
    near, ahead = call(
        base_kernel, [block, vmem((AHEAD, LT, T, L), F32)],
        leave(hist, blocks) + keep(pos, coarse_init, row_1, row_2),
        [vmem((NO * CB, CB), F32), dmas], flops=big, any_in=2,
    )
    coef, u, src, cdiag, scale, c1, c2, r1, r2 = call(
        sweep1_kernel, [seam, block, block, block, block, seam, seam, seam, seam],
        keep(pos, arrived, coarse_init, coarse_leak, near),
        [chot, chot, vmem((CB, 2 * NO * L), BF16)],
    )
    c1, c2 = exchange(COL, c1, c2, ring=True)
    r1, r2 = exchange(ROW, r1, r2)
    fine_drop = call(
        combine_kernel, [pltpu.MemorySpace.HBM((T, T), F32)], leave(hist) + keep(ahead, coef, rims),
        [vmem((STEPS, 4 - AHEAD, LT, T // STEPS, L), F32), tile, pltpu.SemaphoreType.DMA((STEPS,)),
         pltpu.SemaphoreType.DMA((STEPS,))], flops=big // 4, any_in=1, any_out=1,
    )[0]
    coarse_drop = call(
        sweep2_kernel, [hbm((CB, CB), F32)], keep(pos, u, src, cdiag, scale, c1, c2, r1, r2)    )[0]
    return fine_drop, coarse_drop


def solution(mesh):
    spec = P(ROW, COL)

    return jax.shard_map(
        per_device, mesh=mesh, in_specs=(spec,) * 8, out_specs=(spec, spec), check_vma=False
    )
```

```python
import jax
import jax.numpy as jnp
from jax import lax
from jax.experimental import pallas as pl
from jax.experimental.pallas import tpu as pltpu
from jax.sharding import PartitionSpec as P


F32 = jnp.float32
BF16 = jnp.bfloat16
HI = lax.Precision.HIGHEST
ROW, COL = "row", "col"

GROUP = 16
via_conductance = 2.0
coarse_conductance = 4.0
relaxation = 0.8

T = 512
CB = 128
NO = 16
L = 128
OFF = 16
EXT = OFF + T + 16
W = T + L

Q = (1.09375, 1.765625, 1.28125)
RHO = (1.0 - Q[0], Q[0] - Q[1], Q[1] - Q[2], Q[2])
LT = T // L
SLAB = 4 * LT + 1
SUMS = 8
AHEAD = 1
STEPS = 8


def iota(shape, dim):
    return lax.broadcasted_iota(jnp.int32, shape, dim)


def nt(a, b, precision=None):
    return lax.dot_general(
        a, b, (((1,), (1,)), ((), ())), precision=precision, preferred_element_type=F32
    )


def tn(a, b, precision=None):
    return lax.dot_general(
        a, b, (((0,), (0,)), ((), ())), precision=precision, preferred_element_type=F32
    )


def onehot(idx, n):
    return jnp.where(iota((n, idx.shape[1]), 0) == idx, 1.0, 0.0).astype(BF16)


def hi_lo(x):
    hi = x.astype(BF16).astype(F32)
    return hi, x - hi


def lanes(o):
    return slice(o * L, (o + 1) * L)


def at(pos, k, like):
    return jnp.broadcast_to(pos[k : k + 1, : like.shape[1]], like.shape)


def pair_order(pos, k, low, high):
    even = (at(pos, k, low) & 1) == 0
    return jnp.where(even, high, low), jnp.where(even, low, high)


def from_pairs(pos, k, first, second):
    even = (at(pos, k, first) & 1) == 0
    return jnp.where(even, second, first), jnp.where(even, first, second)


def diag_kernel(
    amp, mask, leak, via, zl, invd, strips, rims, amp_s, mask_s, leak_s, via_s, sem
):
    copies = [
        pltpu.make_async_copy(x, y, sem.at[k])
        for k, (x, y) in enumerate(
            ((leak, leak_s), (via, via_s), (amp, amp_s), (mask, mask_s))
        )
    ]
    for copy in copies:
        copy.start()
    for copy in copies:
        copy.wait()
    inv = 1.0 / (4.0 + leak_s[...] + via_s[...])
    z = amp_s[...] * mask_s[...].astype(F32) * inv
    zl[...] = z
    invd[...] = inv
    j, lane = iota((8, 2 * L), 0), iota((8, 2 * L), 1)
    pick = jnp.where(lane == jnp.where(j < 4, j, 2 * L - 8 + j), 1.0, 0.0).astype(BF16)
    for k, x in enumerate((z, inv)):
        hi, rest = hi_lo(jnp.concatenate([x[:, :L], x[:, T - L :]], axis=1))
        mid, lo = hi_lo(rest)
        strips[8 * k : 8 * k + 8, :] = (
            nt(pick, lo.astype(BF16)) + nt(pick, mid.astype(BF16)) + nt(pick, hi.astype(BF16))
        )
    rims[0:8, :] = inv[0:8]
    rims[8:16, :] = inv[T - 8 :]


def copies_kernel(volt, out, sem):
    copies = [
        pltpu.make_async_copy(volt, out.at[pl.ds(o * CB, CB), :], sem.at[o]) for o in range(NO)
    ]
    for copy in copies:
        copy.start()
    for copy in copies:
        copy.wait()


def parts_kernel(vf, vc, wt, node, slots, vf_o, via, a_s, b_s):
    f = vf[...]
    vf_o[...] = f
    slots[0:NO, :] = (f >> 9) * SLAB + ((f >> 7) & 3) * 4
    slots[NO:, :] = (iota((NO, L), 1) - f) & (L - 1)
    place = ((vc[...] >> 11) << 7) | (vc[...] & (CB - 1))
    node[...] = jnp.where(wt[...] > 0.0, place.astype(F32), -1.0)
    for o in range(NO):
        f = vf[o : o + 1, :]
        a_s[:, lanes(o)] = onehot(f // T, T)
        b_s[:, lanes(o)] = jnp.where(iota((T, L), 0) == f % T, wt[o : o + 1, :], 0.0).astype(BF16)
    via[...] = nt(a_s[...], b_s[...])


def strips_kernel(pos, blocks, node, vf, wt, strips, a_o, send_1, send_2, inj_o):
    for o in range(NO):
        at_node = node[o : o + 1, :].astype(jnp.int32)
        v1, rest = hi_lo(blocks[o * CB : (o + 1) * CB, :])
        v2, v3 = hi_lo(rest)
        v = jnp.concatenate([v3, v2, v1], axis=0).astype(BF16)
        y = jnp.dot(v, onehot(at_node & (CB - 1), CB), preferred_element_type=F32)
        y = y[:CB] + y[CB : 2 * CB] + y[2 * CB :]
        y = jnp.where(iota((CB, L), 0) == (at_node >> 7), y, 0.0)
        inj_o[o : o + 1, :] = jnp.sum(y, axis=0, keepdims=True) * wt[o : o + 1, :]
    j = iota((8, L), 0)
    colid = jnp.where(j < 4, j, T - 8 + j)
    hs, ls = [], []
    for o in range(NO):
        f = vf[o : o + 1, :]
        a_o[:, lanes(o)] = onehot(f // T, T)
        hi, lo = hi_lo(inj_o[o : o + 1, :])
        on = colid == f % T
        hs.append(jnp.where(on, hi, 0.0))
        ls.append(jnp.where(on, lo, 0.0))
    lhs = jnp.concatenate(
        [jnp.concatenate(hs, axis=1), jnp.concatenate(ls, axis=1)], axis=0
    ).astype(BF16)
    inj = nt(lhs, a_o[...])
    inv = strips[8:16, :]
    z = strips[0:8, :] + (inj[0:8] + inj[8:16]) * inv
    low = iota((8, T), 0) < 4
    to_l = jnp.where(low, z, pltpu.roll(inv, 4, 0))
    to_r = jnp.where(low, pltpu.roll(z, 4, 0), inv)
    send_1[...], send_2[...] = pair_order(pos, 1, to_l, to_r)


def rhs_kernel(vf, injected, zl, invd, a, z, rims, b_s):
    for o in range(NO):
        hi, lo = hi_lo(injected[o : o + 1, :])
        on = iota((T, L), 0) == vf[o : o + 1, :] % T
        b_s[:, lanes(o)] = jnp.where(on, hi, 0.0).astype(BF16)
        b_s[:, lanes(NO + o)] = jnp.where(on, lo, 0.0).astype(BF16)
    inj = nt(a[...], b_s[:, : NO * L]) + nt(a[...], b_s[:, NO * L :])
    zz = zl[...] + inj * invd[...]
    z[...] = zz
    rims[0:8, :] = zz[0:8]
    rims[8:16, :] = zz[T - 8 :]


def halo_columns(pos, gl, gr):
    place = at(pos, 1, gl)
    parts = []
    for x in (jnp.where(place < NO - 1, gr, 0.0), jnp.where(place > 0, gl, 0.0)):
        a, rest = hi_lo(x)
        b, c = hi_lo(rest)
        parts += [c, b, a]
    j, lane = iota((8, 2 * L), 0), iota((8, 2 * L), 1)
    to_r = jnp.where(lane == jnp.where(j < 4, j, L + j - 4), 1.0, 0.0)
    to_l = jnp.where(lane == jnp.where(j < 4, 124 + j, L + 120 + j), 1.0, 0.0)
    place = jnp.concatenate([to_r] * 3 + [to_l] * 3, axis=0)
    out = tn(jnp.concatenate(parts, axis=0).astype(BF16), place.astype(BF16))
    return out[:, :L], out[:, L:]


def edge_kernel(pos, zr, ir, col_1, col_2, volt, send_1, send_2, corners):
    got_l, got_r = from_pairs(pos, 1, col_1[...], col_2[...])
    zt, it = halo_columns(pos, got_l[:, :L], got_r[:, :L])
    zb, ib = halo_columns(pos, got_l[:, T - L : T], got_r[:, T - L : T])
    for k, x in enumerate((zt[0:16], zb[L - 16 :], it[0:16], ib[L - 16 :])):
        corners[16 * k : 16 * k + 16, :] = x
    low = iota((8, W), 0) < 4
    zt = jnp.concatenate([zr[0:8, :], zt[0:8]], axis=1)
    it = jnp.concatenate([ir[0:8, :], it[0:8]], axis=1)
    zb = jnp.concatenate([zr[8:16, :], zb[L - 8 :]], axis=1)
    ib = jnp.concatenate([ir[8:16, :], ib[L - 8 :]], axis=1)
    to_u = jnp.where(low, zt, pltpu.roll(it, 4, 0))
    to_d = jnp.where(low, pltpu.roll(zb, 4, 0), ib)
    send_1[:, :W], send_2[:, :W] = pair_order(pos, 0, to_u, to_d)
    send_1[:, W:], send_2[:, W:] = pair_order(pos, 0, volt[0:8, :], volt[CB - 8 :, :])


def beside(block):
    n = block.shape[0]
    rows = pltpu.roll(block, 1, 0) + pltpu.roll(block, n - 1, 0)
    return rows + (pltpu.roll(block, 1, 1) + pltpu.roll(block, W - 1, 1))


def near_tiles(ref, start, rows):
    mid = [ref[t, pl.ds(start, rows), :] for t in range(LT + 1)]
    low = [pltpu.roll(m, 1, 1) for m in mid]
    high = [pltpu.roll(m, L - 1, 1) for m in mid]
    lane = iota((rows, L), 1)
    near = []
    for t in range(LT + 1):
        rows_sum = ref[t, pl.ds(start - 1, rows), :] + ref[t, pl.ds(start + 1, rows), :]
        left = jnp.where(lane == 0, low[t - 1], low[t])
        right = jnp.where(lane == L - 1, high[(t + 1) % (LT + 1)], high[t])
        near.append(rows_sum + (left + right))
    return mid, near


def fold(p):
    return (p[:, 0:128] + p[:, 128:256]) + (p[:, 256:384] + p[:, 384:512])


def moments(z, w, n1, n2, dn3, inv):
    d = 1.0 / inv
    dz, dw, dn1, dn2 = d * z, d * w, d * n1, d * n2
    return dz * z, dz * w, dw * w, dw * n1, dn1 * n1, dn1 * n2, dn2 * n2, n2 * dn3


def basis_kernel(pos, z, invd, col_1, col_2, hist, acc_o, ie, ze, we, n1e, n2e, sem):
    zc, ic = halo_columns(pos, *from_pairs(pos, 1, col_1[:, :T], col_2[:, :T]))
    zero = jnp.zeros((OFF, L), F32)
    own = pl.ds(OFF, T)
    for e in (ie, ze, we, n1e, n2e):
        for t in range(LT + 1):
            e[t, 0:OFF, :] = zero
            e[t, OFF + T :, :] = zero
    for t in range(LT):
        ze[t, own, :] = z[:, lanes(t)]
        ie[t, own, :] = invd[:, lanes(t)]
    ze[LT, own, :] = zc
    ie[LT, own, :] = ic
    rows = 128

    def save(k, e):
        copy = pltpu.make_async_copy(e.at[pl.ds(0, LT), own, :], hist.at[k], sem.at[k])
        copy.start()
        return copy

    def apply_to(src, dst, minus):
        def step(i, carry):
            start = pl.multiple_of(OFF + i * rows, 8)
            mid, near = near_tiles(src, start, rows)
            for t in range(LT + 1):
                y = near[t] * ie[t, pl.ds(start, rows), :]
                dst[t, pl.ds(start, rows), :] = mid[t] - y if minus else y
            return carry

        lax.fori_loop(0, T // rows, step, 0)

    copies = [save(0, ze)]
    apply_to(ze, we, True)
    copies.append(save(1, we))
    apply_to(we, n1e, False)
    copies.append(save(2, n1e))
    apply_to(n1e, n2e, False)
    copies.append(save(3, n2e))

    acc = [jnp.zeros((8, L), F32) for _ in range(SUMS)]
    ends = list(range(0, T + 1, 64))
    ends[0], ends[-1] = 8, T - 8
    for low, high in zip(ends[:-1], ends[1:]):
        start, rows = OFF + low, high - low
        n2, dn3 = near_tiles(n2e, start, rows)
        for t in range(LT):
            z8, w8, n18, i8 = (e[t, pl.ds(start, rows), :] for e in (ze, we, n1e, ie))
            for k, p in enumerate(moments(z8, w8, n18, n2[t], dn3[t], i8)):
                for q in range(0, rows, 8):
                    acc[k] = acc[k] + p[q : q + 8]
    for k in range(SUMS):
        acc_o[8 * k : 8 * k + 8, :] = acc[k]
    for copy in copies:
        copy.wait()


def gram_terms(acc, powers):
    g0, q0 = acc[0], acc[1]
    m = acc[2:]
    r = [q0, q0 - m[0], q0 - m[0] - m[1]]
    b0, h00 = g0, q0
    for k in range(3):
        h00 = h00 - Q[k] * m[k]
        b0 = b0 - Q[k] * r[k]
    for k in range(6):
        f = sum(Q[j] * RHO[k - j] for j in range(3) if 0 <= k - j < 4)
        h00 = h00 - f * m[k]

    def times(p, q):
        out = [0.0] * (len(p) + len(q) - 1)
        for i, x in enumerate(p):
            for j, y in enumerate(q):
                out[i + j] += x * y
        return out

    def total(p, values):
        out = None
        for x, v in zip(p, values):
            if x != 0.0:
                out = x * v if out is None else out + x * v
        return out

    out = [h00] + [total(times(RHO, p), m) for p in powers] + [b0]
    for i in range(3):
        out += [total(times(times(powers[i], powers[k]), (1.0, -1.0)), m) for k in range(i, 3)]
        out.append(total(powers[i], r))
    return out


PLAIN = ((1.0,), (0.0, 1.0), (0.0, 0.0, 1.0))
SHIFTED = ((1.0,), (1.0, 1.0), (1.0, 2.0, 1.0))


def rim_kernel(pos, z, invd, corners, row_1, row_2, acc_i, rims, part):
    sub = iota((8, W), 0)
    ours = at(pos, 0, sub)
    above, below = (sub >= 4) & (ours > 0), (sub < 4) & (ours < 7)
    top, bot = from_pairs(pos, 0, row_1[:, :W], row_2[:, :W])
    acc = [acc_i[8 * k : 8 * k + 8, :] for k in range(SUMS)]
    for end in (0, 1):
        rows = slice(0, 16) if end == 0 else slice(T - 16, T)
        zc, ic = corners[16 * end : 16 * end + 16, :], corners[32 + 16 * end : 48 + 16 * end, :]
        z16 = jnp.concatenate([z[rows, :], zc], axis=1)
        i16 = jnp.concatenate([invd[rows, :], ic], axis=1)
        if end == 0:
            zb = jnp.concatenate([jnp.where(above, pltpu.roll(top, 4, 0), 0.0), z16], axis=0)
            ib = jnp.concatenate([jnp.where(above, top, 0.0), i16], axis=0)
            own = slice(8, 16)
        else:
            zb = jnp.concatenate([z16, jnp.where(below, bot, 0.0)], axis=0)
            ib = jnp.concatenate([i16, jnp.where(below, pltpu.roll(bot, 4, 0), 0.0)], axis=0)
            own = slice(8, 16)
        w = zb - ib * beside(zb)
        n1 = ib * beside(w)
        n2 = ib * beside(n1)
        near = beside(n2)
        zo, wo, n1o, n2o, dn3, io = (x[own, :T] for x in (zb, w, n1, n2, near, ib))
        for k, p in enumerate(moments(zo, wo, n1o, n2o, dn3, io)):
            acc[k] = acc[k] + fold(p)
        for k, x in enumerate((wo, n1o, n2o)):
            rims[16 * k + 8 * end : 16 * k + 8 * end + 8, :] = x
    two = [jnp.zeros((2, L), F32)]
    rows = []
    for powers in (PLAIN, SHIFTED):
        terms = gram_terms(acc, powers)
        rows += [jnp.sum(a, axis=0, keepdims=True) for a in terms] + two
    a, rest = hi_lo(jnp.concatenate(rows, axis=0))
    b, c = hi_lo(rest)
    parts = jnp.concatenate([c, b, a], axis=0).astype(BF16)
    sums = nt(jnp.ones((8, L), BF16), parts)
    sums = sums[:, 0:32] + sums[:, 32:64] + sums[:, 64:96]
    sums = jnp.concatenate([sums, jnp.zeros((8, L - 32), F32)], axis=1)
    part[...] = sums


def gather_kernel(hist, table, rims, wt, g_o, x_s, slab, slots, sem):
    copies = [pltpu.make_async_copy(hist.at[k], x_s.at[k], sem.at[k]) for k in range(4)]
    ready = pltpu.make_async_copy(table, slots, sem.at[4])
    ready.start()
    for copy in copies:
        copy.start()
    for k in range(4):
        copies[k].wait()
        if k:
            for t in range(LT):
                x_s[k, t, 0:8, :] = rims[16 * k - 16 : 16 * k - 8, lanes(t)]
                x_s[k, t, T - 8 :, :] = rims[16 * k - 8 : 16 * k, lanes(t)]

        def lay(i, carry):
            for b in range(4):
                for t in range(LT):
                    start = pl.multiple_of(i * 32 + 8 * b, 8)
                    to = (i * 32 + 8 * b) * SLAB + 4 * t + k
                    slab[pl.ds(to, 8, stride=SLAB), :] = x_s[k, t, pl.ds(start, 8), :]
            return carry

        lax.fori_loop(0, T // 32, lay, 0)
    lane, sub = iota((8, L), 1), iota((8, L), 0)
    ready.wait()
    for o in range(NO):
        acc = jnp.zeros((8, L), F32)
        for j in range(L):
            x = slab[pl.ds(slots[o, j], 8), :]
            acc = jnp.where(lane == j, pltpu.roll(x, slots[NO + o, j], 1), acc)
        g_o[8 * o : 8 * o + 8, :] = jnp.where(sub < 4, acc * wt[o : o + 1, :], 0.0)


def pack_kernel(g, rows, node, out):
    out[...] = g[...]
    total = jnp.sum(rows[...], axis=0, keepdims=True)
    for o in range(NO):
        out[8 * o + 4 : 8 * o + 5, :] = total
        out[8 * o + 5 : 8 * o + 6, :] = node[o : o + 1, :]


def solve(tot):
    lane = iota((1, L), 1)

    def lane_of(x, k):
        return jnp.sum(jnp.where(lane == k, x, 0.0), axis=1, keepdims=True)

    def pick(k):
        return jnp.where(lane == 0, lane_of(tot, k), lane_of(tot, 16 + k))

    h, b = {}, []
    k = 0
    for p in range(4):
        for q in range(p, 4):
            h[p, q] = pick(k)
            k += 1
        b.append(pick(k))
        k += 1
    size = [h[p, p] for p in range(4)]
    inv, worst = [], jnp.ones((1, L), F32)
    for p in range(4):
        inv.append(jnp.where(h[p, p] > 3e-7 * size[p], 1.0 / h[p, p], 0.0))
        worst = jnp.minimum(worst, jnp.where(size[p] > 0.0, h[p, p] / size[p], 0.0))
        for q in range(p + 1, 4):
            f = h[p, q] * inv[p]
            for r in range(q, 4):
                h[q, r] = h[q, r] - f * h[p, r]
            b[q] = b[q] - f * b[p]
    c = [None] * 4
    for p in (3, 2, 1, 0):
        s = b[p]
        for q in range(p + 1, 4):
            s = s - h[p, q] * c[q]
        c[p] = s * inv[p]
    shifted = lane_of(worst, 1) > lane_of(worst, 0)
    plain = [lane_of(x, 0) for x in c]
    other = [lane_of(x, 1) for x in c]
    other[1:] = [other[1] + other[2] + other[3], other[2] + 2.0 * other[3], other[3]]
    c = [jnp.where(shifted, y, x) for x, y in zip(plain, other)]
    return [c[0]] + [c[k + 1] - Q[k] * c[0] for k in range(3)]


def combine_kernel(hist, ahead, coef, rims, out, h_s, x_s, sem_in, sem_out):
    n = T // STEPS
    load = [
        pltpu.make_async_copy(
            hist.at[pl.ds(AHEAD, 4 - AHEAD), :, pl.ds(i * n, n), :], h_s.at[i], sem_in.at[i]
        )
        for i in range(STEPS)
    ]
    save = [
        pltpu.make_async_copy(x_s.at[pl.ds(i * n, n), :], out.at[pl.ds(i * n, n), :], sem_out.at[i])
        for i in range(STEPS)
    ]
    for copy in load:
        copy.start()
    c = [coef[k : k + 1, 0:1] for k in range(4)]
    for i in range(STEPS):
        load[i].wait()
        for t in range(LT):
            h = [ahead[k, t, i * n : (i + 1) * n, :] for k in range(AHEAD)]
            h += [h_s[i, k, t] for k in range(4 - AHEAD)]
            x_s[i * n : (i + 1) * n, lanes(t)] = (c[0] * h[0] + c[1] * h[1]) + (
                c[2] * h[2] + c[3] * h[3]
            )
        for end, step, low in ((0, 0, 0), (1, STEPS - 1, n - 8)):
            if i == step:
                for t in range(LT):
                    x = c[0] * ahead[0, t, i * n + low : i * n + low + 8, :]
                    for k in range(3):
                        x += c[k + 1] * rims[16 * k + 8 * end : 16 * k + 8 * end + 8, lanes(t)]
                    x_s[i * n + low : i * n + low + 8, lanes(t)] = x
        save[i].start()
    for copy in save:
        copy.wait()


def coarse_neighbours(pos, u, row_1, row_2, from_l, from_r):
    above, below = from_pairs(pos, 0, row_1, row_2)
    above, below = above[7:8, :], below[0:1, :]
    above = jnp.where(at(pos, 0, above) > 0, above, 0.0)
    below = jnp.where(at(pos, 0, below) < 7, below, 0.0)
    r, lane = iota((CB, CB), 0), iota((CB, CB), 1)
    g, gl = iota((8, CB), 0), iota((8, CB), 1)
    turned_l = jnp.where(g == 0, 0.0, pltpu.roll(from_l, 1, 0))
    turned_r = jnp.where(g == 7, 0.0, pltpu.roll(from_r, 7, 0))
    place = at(pos, 1, from_l)
    from_l = jnp.where(place == 0, turned_l, from_l)
    from_r = jnp.where(place == NO - 1, turned_r, from_r)
    seam_l = tn(from_l, jnp.where(gl == g * GROUP, 1.0, 0.0), HI)
    seam_r = tn(from_r, jnp.where(gl == g * GROUP + GROUP - 1, 1.0, 0.0), HI)
    near = jnp.where(r == 0, above, pltpu.roll(u, 1, 0))
    near += jnp.where(r == CB - 1, below, pltpu.roll(u, CB - 1, 0))
    near += jnp.where(lane % GROUP == 0, seam_l, pltpu.roll(u, 1, 1))
    near += jnp.where(lane % GROUP == GROUP - 1, seam_r, pltpu.roll(u, CB - 1, 1))
    return near


def sweep(u, src, diag, near):
    return u + relaxation * (src - (diag * u - coarse_conductance * near)) / diag


def base_kernel(hist, blocks, pos, volt, row_1, row_2, near, ahead, b_s, sem):
    copy = pltpu.make_async_copy(hist.at[pl.ds(0, AHEAD)], ahead, sem.at[0])
    drops = pltpu.make_async_copy(blocks, b_s, sem.at[1])
    drops.start()
    copy.start()
    drops.wait()
    left, right = jnp.zeros((CB, CB), F32), jnp.zeros((CB, CB), F32)
    for o in range(NO):
        block = b_s[o * CB : (o + 1) * CB, :]
        ours = at(pos, 1, block)
        left = jnp.where(ours == (o + 1) % NO, block, left)
        right = jnp.where(ours == (o - 1) % NO, block, right)
    g, lane = iota((8, CB), 0), iota((8, CB), 1)
    from_l = nt(jnp.where(lane == g * GROUP + GROUP - 1, 1.0, 0.0), left, HI)
    from_r = nt(jnp.where(lane == g * GROUP, 1.0, 0.0), right, HI)
    near[...] = coarse_neighbours(pos, volt[...], row_1[:, W:], row_2[:, W:], from_l, from_r)
    copy.wait()


def sweep1_kernel(
    pos, arrived, volt, cleak, near, coef, u_o, src_o, cdiag, scale, c1, c2, r1, r2, r_s, c_s, v_s
):
    for o in range(NO):
        h = arrived[8 * o + 5 : 8 * o + 6, :].astype(jnp.int32)
        r_s[:, lanes(o)] = onehot(h >> 7, CB)
        c_s[:, lanes(o)] = onehot(h & (CB - 1), CB)
    diag = 4.0 * coarse_conductance + cleak[...] + via_conductance * nt(r_s[...], c_s[...])
    cdiag[...] = diag
    scale[...] = relaxation / diag
    tot = arrived[4:5, :]
    for o in range(1, NO):
        tot += arrived[8 * o + 4 : 8 * o + 5, :]
    d = solve(tot)
    sub = iota((8, L), 0)
    cf = jnp.zeros((8, L), F32)
    for k in range(4):
        cf = jnp.where(sub == k, d[k], cf)
    coef[...] = cf
    for o in range(NO):
        v = jnp.sum(arrived[8 * o : 8 * o + 8, :] * cf, axis=0, keepdims=True)
        hi, lo = hi_lo(v)
        on = c_s[:, lanes(o)]
        v_s[:, lanes(o)] = on * hi.astype(BF16)
        v_s[:, lanes(NO + o)] = on * lo.astype(BF16)
    src = nt(r_s[...], v_s[:, : NO * L]) + nt(r_s[...], v_s[:, NO * L :])
    u = sweep(volt[...], src, diag, near[...])
    u_o[...] = u
    src_o[...] = src
    g, gl = iota((8, CB), 0), iota((8, CB), 1)
    to_l = nt(jnp.where(gl == g * GROUP, 1.0, 0.0), u, HI)
    to_r = nt(jnp.where(gl == g * GROUP + GROUP - 1, 1.0, 0.0), u, HI)
    c1[...], c2[...] = pair_order(pos, 1, to_l, to_r)
    r1[...], r2[...] = pair_order(pos, 0, u[0:8, :], u[CB - 8 :, :])


def sweep2_kernel(pos, u, src, cdiag, scale, col_1, col_2, row_1, row_2, u_o):
    from_l, from_r = from_pairs(pos, 1, col_1[...], col_2[...])
    near = coarse_neighbours(pos, u[...], row_1[...], row_2[...], from_l, from_r)
    u_o[...] = u[...] + scale[...] * (src[...] - (cdiag[...] * u[...] - coarse_conductance * near))


VM = pl.BlockSpec(memory_space=pltpu.VMEM)
ANY = pl.BlockSpec(memory_space=pltpu.HBM)
vmem = pltpu.MemorySpace.VMEM
hbm = jax.ShapeDtypeStruct


def keep(*args):
    return [pltpu.with_memory_space_constraint(x, pltpu.VMEM) for x in args]


def leave(*args):
    return [pltpu.with_memory_space_constraint(x, pltpu.HBM) for x in args]


def call(body, outs, args, scratch=(), flops=0, any_in=0, any_out=0):
    specs = [ANY] * any_in + [VM] * (len(args) - any_in)
    return pl.pallas_call(
        body,
        out_shape=outs,
        in_specs=specs,
        out_specs=[ANY] * any_out + [VM] * (len(outs) - any_out),
        scratch_shapes=list(scratch),
        cost_estimate=pl.CostEstimate(flops=flops, bytes_accessed=0, transcendentals=0),
        compiler_params=pltpu.CompilerParams(vmem_limit_bytes=20 * 2**20),
    )(*args)


def pairs(axis, other, ring):
    n, m = lax.axis_size(axis), lax.axis_size(other)
    near = [(i, i ^ 1) for i in range(n)]
    far = []
    for i in range(n):
        for k in range(m):
            to = (((i + 1) ^ 1) - 1 & (n - 1), k)
            if not ring and i in (0, n - 1):
                to = (i, k ^ 1)
            ids = [(p, q) if axis == ROW else (q, p) for p, q in ((i, k), to)]
            far.append(tuple(r * lax.axis_size(COL) + c for r, c in ids))
    return near, sorted(far)


def exchange(axis, first, second, ring=False):
    near, far = pairs(axis, COL if axis == ROW else ROW, ring)
    if ring:
        n = lax.axis_size(axis)
        far = [(i, ((i + 1) ^ 1) - 1 & (n - 1)) for i in range(n)]
        return lax.ppermute(first, axis, near), lax.ppermute(second, axis, far)
    return lax.ppermute(first, axis, near), lax.ppermute(second, (ROW, COL), far)


def spread(x, axis=COL):
    return lax.all_to_all(x, axis, split_axis=0, concat_axis=0, tiled=True)


def per_device(load_amp, load_mask, leak, coarse_leak, coarse_init, via_fine, via_coarse, via_count):
    pos = jnp.where(
        lax.broadcasted_iota(jnp.int32, (8, W + CB), 0) == 0, lax.axis_index(ROW), lax.axis_index(COL)
    ).astype(jnp.int32)
    live = jnp.arange(L, dtype=jnp.int32)[None, :] < via_count.reshape(NO, 1)
    wt = jnp.where(live, via_conductance, 0.0).astype(F32)
    fine = via_fine.reshape(NO, L)
    coarse = via_coarse.reshape(NO, L)
    tile, block, slots = vmem((T, T), F32), vmem((CB, CB), F32), vmem((NO, L), F32)
    hot, chot = vmem((T, NO * L), BF16), vmem((CB, NO * L), BF16)
    hots = vmem((T, 2 * NO * L), BF16)
    rim16, side, seam = vmem((16, T), F32), vmem((8, T), F32), vmem((8, CB), F32)
    ext, packed = vmem((LT + 1, EXT, L), F32), ((L, L), F32)
    dmas = pltpu.SemaphoreType.DMA((4,))
    big = 20_000_000_000

    blocks = call(
        copies_kernel, [pltpu.MemorySpace.HBM((NO * CB, CB), F32)], leave(coarse_init),
        [pltpu.SemaphoreType.DMA((NO,))], any_out=1,
    )[0]
    blocks = spread(blocks)
    node, where, fine, via = call(
        parts_kernel,
        [slots, pltpu.MemorySpace.HBM((2 * NO, L), jnp.int32),
         vmem((NO, L), jnp.int32), pltpu.MemorySpace.HBM((T, T), F32)],
        leave(fine, coarse) + keep(wt), [hot, hot], flops=big,
    )
    zl, invd, strips, irims = call(
        diag_kernel, [tile, tile, rim16, rim16],
        leave(load_amp, load_mask, leak, via),
        [tile, vmem((T, T), jnp.int32), tile, tile, dmas], flops=big, any_in=4,
    )
    a, send_1, send_2, injected = call(
        strips_kernel, [hot, side, side, slots],
        keep(pos, blocks, node, fine, wt, strips),
    )
    col_1, col_2 = exchange(COL, send_1, send_2)
    z, zrims = call(
        rhs_kernel, [tile, rim16], keep(fine, injected, zl, invd, a), [hots], flops=big
    )
    rim = vmem((8, W + CB), F32)
    send_1, send_2, corners = call(
        edge_kernel, [rim, rim, vmem((64, L), F32)],
        keep(pos, zrims, irims, col_1, col_2, coarse_init)    )
    row_1, row_2 = exchange(ROW, send_1, send_2)
    hist, acc = call(
        basis_kernel, [pltpu.MemorySpace.HBM((4, LT, T, L), F32), vmem((8 * SUMS, L), F32)], keep(pos, z, invd, col_1, col_2),
        [ext] * 5 + [dmas], flops=big, any_out=1,
    )
    rims, part = call(
        rim_kernel, [vmem((48, T), F32), vmem((8, L), F32)],
        keep(pos, z, invd, corners, row_1, row_2, acc)    )
    rows = spread(part, ROW)
    g = call(
        gather_kernel, [vmem(*packed)], leave(hist, where) + keep(rims, wt),
        [vmem((4, LT, T, L), F32), vmem((T * SLAB + 8, L), F32),
         pltpu.MemorySpace.SMEM((2 * NO, L), jnp.int32), pltpu.SemaphoreType.DMA((5,))],
        flops=big, any_in=2,
    )[0]
    arrived = spread(call(pack_kernel, [vmem(*packed)], keep(g, rows, node))[0])
    near, ahead = call(
        base_kernel, [block, vmem((AHEAD, LT, T, L), F32)],
        leave(hist, blocks) + keep(pos, coarse_init, row_1, row_2),
        [vmem((NO * CB, CB), F32), dmas], flops=big, any_in=2,
    )
    coef, u, src, cdiag, scale, c1, c2, r1, r2 = call(
        sweep1_kernel, [seam, block, block, block, block, seam, seam, seam, seam],
        keep(pos, arrived, coarse_init, coarse_leak, near),
        [chot, chot, vmem((CB, 2 * NO * L), BF16)],
    )
    c1, c2 = exchange(COL, c1, c2, ring=True)
    r1, r2 = exchange(ROW, r1, r2)
    fine_drop = call(
        combine_kernel, [pltpu.MemorySpace.HBM((T, T), F32)], leave(hist) + keep(ahead, coef, rims),
        [vmem((STEPS, 4 - AHEAD, LT, T // STEPS, L), F32), tile, pltpu.SemaphoreType.DMA((STEPS,)),
         pltpu.SemaphoreType.DMA((STEPS,))], flops=big // 4, any_in=1, any_out=1,
    )[0]
    coarse_drop = call(
        sweep2_kernel, [hbm((CB, CB), F32)], keep(pos, u, src, cdiag, scale, c1, c2, r1, r2)    )[0]
    return fine_drop, coarse_drop


def solution(mesh):
    spec = P(ROW, COL)

    return jax.shard_map(
        per_device, mesh=mesh, in_specs=(spec,) * 8, out_specs=(spec, spec), check_vma=False
    )
```

```python
import jax
import jax.numpy as jnp
from jax import lax
from jax.experimental import pallas as pl
from jax.experimental.pallas import tpu as pltpu
from jax.sharding import PartitionSpec as P


F32 = jnp.float32
BF16 = jnp.bfloat16
HI = lax.Precision.HIGHEST
ROW, COL = "row", "col"

GROUP = 16
via_conductance = 2.0
coarse_conductance = 4.0
relaxation = 0.8

T = 512
CB = 128
NO = 16
L = 128
OFF = 16
EXT = OFF + T + 16
W = T + L

Q = (1.09375, 1.765625, 1.28125)
RHO = (1.0 - Q[0], Q[0] - Q[1], Q[1] - Q[2], Q[2])
LT = T // L
SLAB = 4 * LT + 1
SUMS = 8
AHEAD = 1
STEPS = 8


def iota(shape, dim):
    return lax.broadcasted_iota(jnp.int32, shape, dim)


def nt(a, b, precision=None):
    return lax.dot_general(
        a, b, (((1,), (1,)), ((), ())), precision=precision, preferred_element_type=F32
    )


def tn(a, b, precision=None):
    return lax.dot_general(
        a, b, (((0,), (0,)), ((), ())), precision=precision, preferred_element_type=F32
    )


def onehot(idx, n):
    return jnp.where(iota((n, idx.shape[1]), 0) == idx, 1.0, 0.0).astype(BF16)


def hi_lo(x):
    hi = x.astype(BF16).astype(F32)
    return hi, x - hi


def lanes(o):
    return slice(o * L, (o + 1) * L)


def at(pos, k, like):
    return jnp.broadcast_to(pos[k : k + 1, : like.shape[1]], like.shape)


def pair_order(pos, k, low, high):
    even = (at(pos, k, low) & 1) == 0
    return jnp.where(even, high, low), jnp.where(even, low, high)


def from_pairs(pos, k, first, second):
    even = (at(pos, k, first) & 1) == 0
    return jnp.where(even, second, first), jnp.where(even, first, second)


def diag_kernel(
    amp, mask, leak, via, zl, invd, strips, rims, amp_s, mask_s, leak_s, via_s, sem
):
    copies = [
        pltpu.make_async_copy(x, y, sem.at[k])
        for k, (x, y) in enumerate(
            ((leak, leak_s), (via, via_s), (amp, amp_s), (mask, mask_s))
        )
    ]
    for copy in copies:
        copy.start()
    for copy in copies:
        copy.wait()
    inv = 1.0 / (4.0 + leak_s[...] + via_s[...])
    z = amp_s[...] * mask_s[...].astype(F32) * inv
    zl[...] = z
    invd[...] = inv
    j, lane = iota((8, 2 * L), 0), iota((8, 2 * L), 1)
    pick = jnp.where(lane == jnp.where(j < 4, j, 2 * L - 8 + j), 1.0, 0.0).astype(BF16)
    for k, x in enumerate((z, inv)):
        hi, rest = hi_lo(jnp.concatenate([x[:, :L], x[:, T - L :]], axis=1))
        mid, lo = hi_lo(rest)
        strips[8 * k : 8 * k + 8, :] = (
            nt(pick, lo.astype(BF16)) + nt(pick, mid.astype(BF16)) + nt(pick, hi.astype(BF16))
        )
    rims[0:8, :] = inv[0:8]
    rims[8:16, :] = inv[T - 8 :]


def copies_kernel(volt, out):
    for o in range(NO):
        out[o * CB : (o + 1) * CB, :] = volt[...]


def parts_kernel(vf, vc, wt, node, slots, vf_o, via, a_s, b_s):
    f = vf[...]
    vf_o[...] = f
    slots[0:NO, :] = (f >> 9) * SLAB + ((f >> 7) & 3) * 4
    slots[NO:, :] = (iota((NO, L), 1) - f) & (L - 1)
    place = ((vc[...] >> 11) << 7) | (vc[...] & (CB - 1))
    node[...] = jnp.where(wt[...] > 0.0, place.astype(F32), -1.0)
    for o in range(NO):
        f = vf[o : o + 1, :]
        a_s[:, lanes(o)] = onehot(f // T, T)
        b_s[:, lanes(o)] = jnp.where(iota((T, L), 0) == f % T, wt[o : o + 1, :], 0.0).astype(BF16)
    via[...] = nt(a_s[...], b_s[...])


def strips_kernel(pos, blocks, node, vf, wt, strips, a_o, send_1, send_2, inj_o):
    for o in range(NO):
        at_node = node[o : o + 1, :].astype(jnp.int32)
        v1, rest = hi_lo(blocks[o * CB : (o + 1) * CB, :])
        v2, v3 = hi_lo(rest)
        v = jnp.concatenate([v3, v2, v1], axis=0).astype(BF16)
        y = jnp.dot(v, onehot(at_node & (CB - 1), CB), preferred_element_type=F32)
        y = y[:CB] + y[CB : 2 * CB] + y[2 * CB :]
        y = jnp.where(iota((CB, L), 0) == (at_node >> 7), y, 0.0)
        inj_o[o : o + 1, :] = jnp.sum(y, axis=0, keepdims=True) * wt[o : o + 1, :]
    j = iota((8, L), 0)
    colid = jnp.where(j < 4, j, T - 8 + j)
    hs, ls = [], []
    for o in range(NO):
        f = vf[o : o + 1, :]
        a_o[:, lanes(o)] = onehot(f // T, T)
        hi, lo = hi_lo(inj_o[o : o + 1, :])
        on = colid == f % T
        hs.append(jnp.where(on, hi, 0.0))
        ls.append(jnp.where(on, lo, 0.0))
    lhs = jnp.concatenate(
        [jnp.concatenate(hs, axis=1), jnp.concatenate(ls, axis=1)], axis=0
    ).astype(BF16)
    inj = nt(lhs, a_o[...])
    inv = strips[8:16, :]
    z = strips[0:8, :] + (inj[0:8] + inj[8:16]) * inv
    low = iota((8, T), 0) < 4
    to_l = jnp.where(low, z, pltpu.roll(inv, 4, 0))
    to_r = jnp.where(low, pltpu.roll(z, 4, 0), inv)
    send_1[...], send_2[...] = pair_order(pos, 1, to_l, to_r)


def rhs_kernel(vf, injected, zl, invd, a, z, rims, b_s):
    for o in range(NO):
        hi, lo = hi_lo(injected[o : o + 1, :])
        on = iota((T, L), 0) == vf[o : o + 1, :] % T
        b_s[:, lanes(o)] = jnp.where(on, hi, 0.0).astype(BF16)
        b_s[:, lanes(NO + o)] = jnp.where(on, lo, 0.0).astype(BF16)
    inj = nt(a[...], b_s[:, : NO * L]) + nt(a[...], b_s[:, NO * L :])
    zz = zl[...] + inj * invd[...]
    z[...] = zz
    rims[0:8, :] = zz[0:8]
    rims[8:16, :] = zz[T - 8 :]


def halo_columns(pos, gl, gr):
    place = at(pos, 1, gl)
    parts = []
    for x in (jnp.where(place < NO - 1, gr, 0.0), jnp.where(place > 0, gl, 0.0)):
        a, rest = hi_lo(x)
        b, c = hi_lo(rest)
        parts += [c, b, a]
    j, lane = iota((8, 2 * L), 0), iota((8, 2 * L), 1)
    to_r = jnp.where(lane == jnp.where(j < 4, j, L + j - 4), 1.0, 0.0)
    to_l = jnp.where(lane == jnp.where(j < 4, 124 + j, L + 120 + j), 1.0, 0.0)
    place = jnp.concatenate([to_r] * 3 + [to_l] * 3, axis=0)
    out = tn(jnp.concatenate(parts, axis=0).astype(BF16), place.astype(BF16))
    return out[:, :L], out[:, L:]


def edge_kernel(pos, zr, ir, col_1, col_2, volt, send_1, send_2, corners):
    got_l, got_r = from_pairs(pos, 1, col_1[...], col_2[...])
    zt, it = halo_columns(pos, got_l[:, :L], got_r[:, :L])
    zb, ib = halo_columns(pos, got_l[:, T - L : T], got_r[:, T - L : T])
    for k, x in enumerate((zt[0:16], zb[L - 16 :], it[0:16], ib[L - 16 :])):
        corners[16 * k : 16 * k + 16, :] = x
    low = iota((8, W), 0) < 4
    zt = jnp.concatenate([zr[0:8, :], zt[0:8]], axis=1)
    it = jnp.concatenate([ir[0:8, :], it[0:8]], axis=1)
    zb = jnp.concatenate([zr[8:16, :], zb[L - 8 :]], axis=1)
    ib = jnp.concatenate([ir[8:16, :], ib[L - 8 :]], axis=1)
    to_u = jnp.where(low, zt, pltpu.roll(it, 4, 0))
    to_d = jnp.where(low, pltpu.roll(zb, 4, 0), ib)
    send_1[:, :W], send_2[:, :W] = pair_order(pos, 0, to_u, to_d)
    send_1[:, W:], send_2[:, W:] = pair_order(pos, 0, volt[0:8, :], volt[CB - 8 :, :])


def beside(block):
    n = block.shape[0]
    rows = pltpu.roll(block, 1, 0) + pltpu.roll(block, n - 1, 0)
    return rows + (pltpu.roll(block, 1, 1) + pltpu.roll(block, W - 1, 1))


def near_tiles(ref, start, rows):
    mid = [ref[t, pl.ds(start, rows), :] for t in range(LT + 1)]
    low = [pltpu.roll(m, 1, 1) for m in mid]
    high = [pltpu.roll(m, L - 1, 1) for m in mid]
    lane = iota((rows, L), 1)
    near = []
    for t in range(LT + 1):
        rows_sum = ref[t, pl.ds(start - 1, rows), :] + ref[t, pl.ds(start + 1, rows), :]
        left = jnp.where(lane == 0, low[t - 1], low[t])
        right = jnp.where(lane == L - 1, high[(t + 1) % (LT + 1)], high[t])
        near.append(rows_sum + (left + right))
    return mid, near


def fold(p):
    return (p[:, 0:128] + p[:, 128:256]) + (p[:, 256:384] + p[:, 384:512])


def moments(z, w, n1, n2, dn3, inv):
    d = 1.0 / inv
    dz, dw, dn1, dn2 = d * z, d * w, d * n1, d * n2
    return dz * z, dz * w, dw * w, dw * n1, dn1 * n1, dn1 * n2, dn2 * n2, n2 * dn3


def basis_kernel(pos, z, invd, col_1, col_2, hist, acc_o, ie, ze, we, n1e, n2e, sem):
    zc, ic = halo_columns(pos, *from_pairs(pos, 1, col_1[:, :T], col_2[:, :T]))
    zero = jnp.zeros((OFF, L), F32)
    own = pl.ds(OFF, T)
    for e in (ie, ze, we, n1e, n2e):
        for t in range(LT + 1):
            e[t, 0:OFF, :] = zero
            e[t, OFF + T :, :] = zero
    for t in range(LT):
        ze[t, own, :] = z[:, lanes(t)]
        ie[t, own, :] = invd[:, lanes(t)]
    ze[LT, own, :] = zc
    ie[LT, own, :] = ic
    rows = 128

    def save(k, e):
        copy = pltpu.make_async_copy(e.at[pl.ds(0, LT), own, :], hist.at[k], sem.at[k])
        copy.start()
        return copy

    def apply_to(src, dst, minus):
        def step(i, carry):
            start = pl.multiple_of(OFF + i * rows, 8)
            mid, near = near_tiles(src, start, rows)
            for t in range(LT + 1):
                y = near[t] * ie[t, pl.ds(start, rows), :]
                dst[t, pl.ds(start, rows), :] = mid[t] - y if minus else y
            return carry

        lax.fori_loop(0, T // rows, step, 0)

    copies = [save(0, ze)]
    apply_to(ze, we, True)
    copies.append(save(1, we))
    apply_to(we, n1e, False)
    copies.append(save(2, n1e))
    apply_to(n1e, n2e, False)
    copies.append(save(3, n2e))

    acc = [jnp.zeros((8, L), F32) for _ in range(SUMS)]
    ends = list(range(0, T + 1, 64))
    ends[0], ends[-1] = 8, T - 8
    for low, high in zip(ends[:-1], ends[1:]):
        start, rows = OFF + low, high - low
        n2, dn3 = near_tiles(n2e, start, rows)
        for t in range(LT):
            z8, w8, n18, i8 = (e[t, pl.ds(start, rows), :] for e in (ze, we, n1e, ie))
            for k, p in enumerate(moments(z8, w8, n18, n2[t], dn3[t], i8)):
                for q in range(0, rows, 8):
                    acc[k] = acc[k] + p[q : q + 8]
    for k in range(SUMS):
        acc_o[8 * k : 8 * k + 8, :] = acc[k]
    for copy in copies:
        copy.wait()


def gram_terms(acc, powers):
    g0, q0 = acc[0], acc[1]
    m = acc[2:]
    r = [q0, q0 - m[0], q0 - m[0] - m[1]]
    b0, h00 = g0, q0
    for k in range(3):
        h00 = h00 - Q[k] * m[k]
        b0 = b0 - Q[k] * r[k]
    for k in range(6):
        f = sum(Q[j] * RHO[k - j] for j in range(3) if 0 <= k - j < 4)
        h00 = h00 - f * m[k]

    def times(p, q):
        out = [0.0] * (len(p) + len(q) - 1)
        for i, x in enumerate(p):
            for j, y in enumerate(q):
                out[i + j] += x * y
        return out

    def total(p, values):
        out = None
        for x, v in zip(p, values):
            if x != 0.0:
                out = x * v if out is None else out + x * v
        return out

    out = [h00] + [total(times(RHO, p), m) for p in powers] + [b0]
    for i in range(3):
        out += [total(times(times(powers[i], powers[k]), (1.0, -1.0)), m) for k in range(i, 3)]
        out.append(total(powers[i], r))
    return out


PLAIN = ((1.0,), (0.0, 1.0), (0.0, 0.0, 1.0))
SHIFTED = ((1.0,), (1.0, 1.0), (1.0, 2.0, 1.0))


def rim_kernel(pos, z, invd, corners, row_1, row_2, acc_i, rims, part):
    sub = iota((8, W), 0)
    ours = at(pos, 0, sub)
    above, below = (sub >= 4) & (ours > 0), (sub < 4) & (ours < 7)
    top, bot = from_pairs(pos, 0, row_1[:, :W], row_2[:, :W])
    acc = [acc_i[8 * k : 8 * k + 8, :] for k in range(SUMS)]
    for end in (0, 1):
        rows = slice(0, 16) if end == 0 else slice(T - 16, T)
        zc, ic = corners[16 * end : 16 * end + 16, :], corners[32 + 16 * end : 48 + 16 * end, :]
        z16 = jnp.concatenate([z[rows, :], zc], axis=1)
        i16 = jnp.concatenate([invd[rows, :], ic], axis=1)
        if end == 0:
            zb = jnp.concatenate([jnp.where(above, pltpu.roll(top, 4, 0), 0.0), z16], axis=0)
            ib = jnp.concatenate([jnp.where(above, top, 0.0), i16], axis=0)
            own = slice(8, 16)
        else:
            zb = jnp.concatenate([z16, jnp.where(below, bot, 0.0)], axis=0)
            ib = jnp.concatenate([i16, jnp.where(below, pltpu.roll(bot, 4, 0), 0.0)], axis=0)
            own = slice(8, 16)
        w = zb - ib * beside(zb)
        n1 = ib * beside(w)
        n2 = ib * beside(n1)
        near = beside(n2)
        zo, wo, n1o, n2o, dn3, io = (x[own, :T] for x in (zb, w, n1, n2, near, ib))
        for k, p in enumerate(moments(zo, wo, n1o, n2o, dn3, io)):
            acc[k] = acc[k] + fold(p)
        for k, x in enumerate((wo, n1o, n2o)):
            rims[16 * k + 8 * end : 16 * k + 8 * end + 8, :] = x
    two = [jnp.zeros((2, L), F32)]
    rows = []
    for powers in (PLAIN, SHIFTED):
        terms = gram_terms(acc, powers)
        rows += [jnp.sum(a, axis=0, keepdims=True) for a in terms] + two
    a, rest = hi_lo(jnp.concatenate(rows, axis=0))
    b, c = hi_lo(rest)
    parts = jnp.concatenate([c, b, a], axis=0).astype(BF16)
    sums = nt(jnp.ones((8, L), BF16), parts)
    sums = sums[:, 0:32] + sums[:, 32:64] + sums[:, 64:96]
    sums = jnp.concatenate([sums, jnp.zeros((8, L - 32), F32)], axis=1)
    part[...] = sums


def gather_kernel(hist, table, rims, wt, g_o, x_s, slab, slots, sem):
    copies = [pltpu.make_async_copy(hist.at[k], x_s.at[k], sem.at[k]) for k in range(4)]
    ready = pltpu.make_async_copy(table, slots, sem.at[4])
    ready.start()
    for copy in copies:
        copy.start()
    for k in range(4):
        copies[k].wait()
        if k:
            for t in range(LT):
                x_s[k, t, 0:8, :] = rims[16 * k - 16 : 16 * k - 8, lanes(t)]
                x_s[k, t, T - 8 :, :] = rims[16 * k - 8 : 16 * k, lanes(t)]

        def lay(i, carry):
            for b in range(4):
                for t in range(LT):
                    start = pl.multiple_of(i * 32 + 8 * b, 8)
                    to = (i * 32 + 8 * b) * SLAB + 4 * t + k
                    slab[pl.ds(to, 8, stride=SLAB), :] = x_s[k, t, pl.ds(start, 8), :]
            return carry

        lax.fori_loop(0, T // 32, lay, 0)
    lane, sub = iota((8, L), 1), iota((8, L), 0)
    ready.wait()
    for o in range(NO):
        acc = jnp.zeros((8, L), F32)
        for j in range(L):
            x = slab[pl.ds(slots[o, j], 8), :]
            acc = jnp.where(lane == j, pltpu.roll(x, slots[NO + o, j], 1), acc)
        g_o[8 * o : 8 * o + 8, :] = jnp.where(sub < 4, acc * wt[o : o + 1, :], 0.0)


def pack_kernel(g, rows, node, out):
    out[...] = g[...]
    total = jnp.sum(rows[...], axis=0, keepdims=True)
    for o in range(NO):
        out[8 * o + 4 : 8 * o + 5, :] = total
        out[8 * o + 5 : 8 * o + 6, :] = node[o : o + 1, :]


def solve(tot):
    lane = iota((1, L), 1)

    def lane_of(x, k):
        return jnp.sum(jnp.where(lane == k, x, 0.0), axis=1, keepdims=True)

    def pick(k):
        return jnp.where(lane == 0, lane_of(tot, k), lane_of(tot, 16 + k))

    h, b = {}, []
    k = 0
    for p in range(4):
        for q in range(p, 4):
            h[p, q] = pick(k)
            k += 1
        b.append(pick(k))
        k += 1
    size = [h[p, p] for p in range(4)]
    inv, worst = [], jnp.ones((1, L), F32)
    for p in range(4):
        inv.append(jnp.where(h[p, p] > 3e-7 * size[p], 1.0 / h[p, p], 0.0))
        worst = jnp.minimum(worst, jnp.where(size[p] > 0.0, h[p, p] / size[p], 0.0))
        for q in range(p + 1, 4):
            f = h[p, q] * inv[p]
            for r in range(q, 4):
                h[q, r] = h[q, r] - f * h[p, r]
            b[q] = b[q] - f * b[p]
    c = [None] * 4
    for p in (3, 2, 1, 0):
        s = b[p]
        for q in range(p + 1, 4):
            s = s - h[p, q] * c[q]
        c[p] = s * inv[p]
    shifted = lane_of(worst, 1) > lane_of(worst, 0)
    plain = [lane_of(x, 0) for x in c]
    other = [lane_of(x, 1) for x in c]
    other[1:] = [other[1] + other[2] + other[3], other[2] + 2.0 * other[3], other[3]]
    c = [jnp.where(shifted, y, x) for x, y in zip(plain, other)]
    return [c[0]] + [c[k + 1] - Q[k] * c[0] for k in range(3)]


def combine_kernel(hist, ahead, coef, rims, out, h_s, x_s, sem_in, sem_out):
    n = T // STEPS
    load = [
        pltpu.make_async_copy(
            hist.at[pl.ds(AHEAD, 4 - AHEAD), :, pl.ds(i * n, n), :], h_s.at[i], sem_in.at[i]
        )
        for i in range(STEPS)
    ]
    save = [
        pltpu.make_async_copy(x_s.at[pl.ds(i * n, n), :], out.at[pl.ds(i * n, n), :], sem_out.at[i])
        for i in range(STEPS)
    ]
    for copy in load:
        copy.start()
    c = [coef[k : k + 1, 0:1] for k in range(4)]
    for i in range(STEPS):
        load[i].wait()
        for t in range(LT):
            h = [ahead[k, t, i * n : (i + 1) * n, :] for k in range(AHEAD)]
            h += [h_s[i, k, t] for k in range(4 - AHEAD)]
            x_s[i * n : (i + 1) * n, lanes(t)] = (c[0] * h[0] + c[1] * h[1]) + (
                c[2] * h[2] + c[3] * h[3]
            )
        for end, step, low in ((0, 0, 0), (1, STEPS - 1, n - 8)):
            if i == step:
                for t in range(LT):
                    x = c[0] * ahead[0, t, i * n + low : i * n + low + 8, :]
                    for k in range(3):
                        x += c[k + 1] * rims[16 * k + 8 * end : 16 * k + 8 * end + 8, lanes(t)]
                    x_s[i * n + low : i * n + low + 8, lanes(t)] = x
        save[i].start()
    for copy in save:
        copy.wait()


def coarse_neighbours(pos, u, row_1, row_2, from_l, from_r):
    above, below = from_pairs(pos, 0, row_1, row_2)
    above, below = above[7:8, :], below[0:1, :]
    above = jnp.where(at(pos, 0, above) > 0, above, 0.0)
    below = jnp.where(at(pos, 0, below) < 7, below, 0.0)
    r, lane = iota((CB, CB), 0), iota((CB, CB), 1)
    g, gl = iota((8, CB), 0), iota((8, CB), 1)
    turned_l = jnp.where(g == 0, 0.0, pltpu.roll(from_l, 1, 0))
    turned_r = jnp.where(g == 7, 0.0, pltpu.roll(from_r, 7, 0))
    place = at(pos, 1, from_l)
    from_l = jnp.where(place == 0, turned_l, from_l)
    from_r = jnp.where(place == NO - 1, turned_r, from_r)
    seam_l = tn(from_l, jnp.where(gl == g * GROUP, 1.0, 0.0), HI)
    seam_r = tn(from_r, jnp.where(gl == g * GROUP + GROUP - 1, 1.0, 0.0), HI)
    near = jnp.where(r == 0, above, pltpu.roll(u, 1, 0))
    near += jnp.where(r == CB - 1, below, pltpu.roll(u, CB - 1, 0))
    near += jnp.where(lane % GROUP == 0, seam_l, pltpu.roll(u, 1, 1))
    near += jnp.where(lane % GROUP == GROUP - 1, seam_r, pltpu.roll(u, CB - 1, 1))
    return near


def sweep(u, src, diag, near):
    return u + relaxation * (src - (diag * u - coarse_conductance * near)) / diag


def base_kernel(hist, blocks, pos, volt, row_1, row_2, near, ahead, b_s, sem):
    copy = pltpu.make_async_copy(hist.at[pl.ds(0, AHEAD)], ahead, sem.at[0])
    drops = pltpu.make_async_copy(blocks, b_s, sem.at[1])
    drops.start()
    copy.start()
    drops.wait()
    left, right = jnp.zeros((CB, CB), F32), jnp.zeros((CB, CB), F32)
    for o in range(NO):
        block = b_s[o * CB : (o + 1) * CB, :]
        ours = at(pos, 1, block)
        left = jnp.where(ours == (o + 1) % NO, block, left)
        right = jnp.where(ours == (o - 1) % NO, block, right)
    g, lane = iota((8, CB), 0), iota((8, CB), 1)
    from_l = nt(jnp.where(lane == g * GROUP + GROUP - 1, 1.0, 0.0), left, HI)
    from_r = nt(jnp.where(lane == g * GROUP, 1.0, 0.0), right, HI)
    near[...] = coarse_neighbours(pos, volt[...], row_1[:, W:], row_2[:, W:], from_l, from_r)
    copy.wait()


def sweep1_kernel(
    pos, arrived, volt, cleak, near, coef, u_o, src_o, cdiag, scale, c1, c2, r1, r2, r_s, c_s, v_s
):
    for o in range(NO):
        h = arrived[8 * o + 5 : 8 * o + 6, :].astype(jnp.int32)
        r_s[:, lanes(o)] = onehot(h >> 7, CB)
        c_s[:, lanes(o)] = onehot(h & (CB - 1), CB)
    diag = 4.0 * coarse_conductance + cleak[...] + via_conductance * nt(r_s[...], c_s[...])
    cdiag[...] = diag
    scale[...] = relaxation / diag
    tot = arrived[4:5, :]
    for o in range(1, NO):
        tot += arrived[8 * o + 4 : 8 * o + 5, :]
    d = solve(tot)
    sub = iota((8, L), 0)
    cf = jnp.zeros((8, L), F32)
    for k in range(4):
        cf = jnp.where(sub == k, d[k], cf)
    coef[...] = cf
    for o in range(NO):
        v = jnp.sum(arrived[8 * o : 8 * o + 8, :] * cf, axis=0, keepdims=True)
        hi, lo = hi_lo(v)
        on = c_s[:, lanes(o)]
        v_s[:, lanes(o)] = on * hi.astype(BF16)
        v_s[:, lanes(NO + o)] = on * lo.astype(BF16)
    src = nt(r_s[...], v_s[:, : NO * L]) + nt(r_s[...], v_s[:, NO * L :])
    u = sweep(volt[...], src, diag, near[...])
    u_o[...] = u
    src_o[...] = src
    g, gl = iota((8, CB), 0), iota((8, CB), 1)
    to_l = nt(jnp.where(gl == g * GROUP, 1.0, 0.0), u, HI)
    to_r = nt(jnp.where(gl == g * GROUP + GROUP - 1, 1.0, 0.0), u, HI)
    c1[...], c2[...] = pair_order(pos, 1, to_l, to_r)
    r1[...], r2[...] = pair_order(pos, 0, u[0:8, :], u[CB - 8 :, :])


def sweep2_kernel(pos, u, src, cdiag, scale, col_1, col_2, row_1, row_2, u_o):
    from_l, from_r = from_pairs(pos, 1, col_1[...], col_2[...])
    near = coarse_neighbours(pos, u[...], row_1[...], row_2[...], from_l, from_r)
    u_o[...] = u[...] + scale[...] * (src[...] - (cdiag[...] * u[...] - coarse_conductance * near))


VM = pl.BlockSpec(memory_space=pltpu.VMEM)
ANY = pl.BlockSpec(memory_space=pltpu.HBM)
vmem = pltpu.MemorySpace.VMEM
hbm = jax.ShapeDtypeStruct


def keep(*args):
    return [pltpu.with_memory_space_constraint(x, pltpu.VMEM) for x in args]


def leave(*args):
    return [pltpu.with_memory_space_constraint(x, pltpu.HBM) for x in args]


def call(body, outs, args, scratch=(), flops=0, any_in=0, any_out=0):
    specs = [ANY] * any_in + [VM] * (len(args) - any_in)
    return pl.pallas_call(
        body,
        out_shape=outs,
        in_specs=specs,
        out_specs=[ANY] * any_out + [VM] * (len(outs) - any_out),
        scratch_shapes=list(scratch),
        cost_estimate=pl.CostEstimate(flops=flops, bytes_accessed=0, transcendentals=0),
        compiler_params=pltpu.CompilerParams(vmem_limit_bytes=20 * 2**20),
    )(*args)


def pairs(axis, other, ring):
    n, m = lax.axis_size(axis), lax.axis_size(other)
    near = [(i, i ^ 1) for i in range(n)]
    far = []
    for i in range(n):
        for k in range(m):
            to = (((i + 1) ^ 1) - 1 & (n - 1), k)
            if not ring and i in (0, n - 1):
                to = (i, k ^ 1)
            ids = [(p, q) if axis == ROW else (q, p) for p, q in ((i, k), to)]
            far.append(tuple(r * lax.axis_size(COL) + c for r, c in ids))
    return near, sorted(far)


def exchange(axis, first, second, ring=False):
    near, far = pairs(axis, COL if axis == ROW else ROW, ring)
    if ring:
        n = lax.axis_size(axis)
        far = [(i, ((i + 1) ^ 1) - 1 & (n - 1)) for i in range(n)]
        return lax.ppermute(first, axis, near), lax.ppermute(second, axis, far)
    return lax.ppermute(first, axis, near), lax.ppermute(second, (ROW, COL), far)


def spread(x, axis=COL):
    return lax.all_to_all(x, axis, split_axis=0, concat_axis=0, tiled=True)


def per_device(load_amp, load_mask, leak, coarse_leak, coarse_init, via_fine, via_coarse, via_count):
    pos = jnp.where(
        lax.broadcasted_iota(jnp.int32, (8, W + CB), 0) == 0, lax.axis_index(ROW), lax.axis_index(COL)
    ).astype(jnp.int32)
    live = jnp.arange(L, dtype=jnp.int32)[None, :] < via_count.reshape(NO, 1)
    wt = jnp.where(live, via_conductance, 0.0).astype(F32)
    fine = via_fine.reshape(NO, L)
    coarse = via_coarse.reshape(NO, L)
    tile, block, slots = vmem((T, T), F32), vmem((CB, CB), F32), vmem((NO, L), F32)
    hot, chot = vmem((T, NO * L), BF16), vmem((CB, NO * L), BF16)
    hots = vmem((T, 2 * NO * L), BF16)
    rim16, side, seam = vmem((16, T), F32), vmem((8, T), F32), vmem((8, CB), F32)
    ext, packed = vmem((LT + 1, EXT, L), F32), ((L, L), F32)
    dmas = pltpu.SemaphoreType.DMA((4,))
    big = 20_000_000_000

    blocks = call(
        copies_kernel, [pltpu.MemorySpace.HBM((NO * CB, CB), F32)], leave(coarse_init),
    )[0]
    blocks = spread(blocks)
    node, where, fine, via = call(
        parts_kernel,
        [slots, pltpu.MemorySpace.HBM((2 * NO, L), jnp.int32),
         vmem((NO, L), jnp.int32), pltpu.MemorySpace.HBM((T, T), F32)],
        leave(fine, coarse) + keep(wt), [hot, hot], flops=big,
    )
    zl, invd, strips, irims = call(
        diag_kernel, [tile, tile, rim16, rim16],
        leave(load_amp, load_mask, leak, via),
        [tile, vmem((T, T), jnp.int32), tile, tile, dmas], flops=big, any_in=4,
    )
    a, send_1, send_2, injected = call(
        strips_kernel, [hot, side, side, slots],
        keep(pos, blocks, node, fine, wt, strips),
    )
    col_1, col_2 = exchange(COL, send_1, send_2)
    z, zrims = call(
        rhs_kernel, [tile, rim16], keep(fine, injected, zl, invd, a), [hots], flops=big
    )
    rim = vmem((8, W + CB), F32)
    send_1, send_2, corners = call(
        edge_kernel, [rim, rim, vmem((64, L), F32)],
        keep(pos, zrims, irims, col_1, col_2, coarse_init)    )
    row_1, row_2 = exchange(ROW, send_1, send_2)
    hist, acc = call(
        basis_kernel, [pltpu.MemorySpace.HBM((4, LT, T, L), F32), vmem((8 * SUMS, L), F32)], keep(pos, z, invd, col_1, col_2),
        [ext] * 5 + [dmas], flops=big, any_out=1,
    )
    rims, part = call(
        rim_kernel, [vmem((48, T), F32), vmem((8, L), F32)],
        keep(pos, z, invd, corners, row_1, row_2, acc)    )
    rows = spread(part, ROW)
    g = call(
        gather_kernel, [vmem(*packed)], leave(hist, where) + keep(rims, wt),
        [vmem((4, LT, T, L), F32), vmem((T * SLAB + 8, L), F32),
         pltpu.MemorySpace.SMEM((2 * NO, L), jnp.int32), pltpu.SemaphoreType.DMA((5,))],
        flops=big, any_in=2,
    )[0]
    arrived = spread(call(pack_kernel, [vmem(*packed)], keep(g, rows, node))[0])
    near, ahead = call(
        base_kernel, [block, vmem((AHEAD, LT, T, L), F32)],
        leave(hist, blocks) + keep(pos, coarse_init, row_1, row_2),
        [vmem((NO * CB, CB), F32), dmas], flops=big, any_in=2,
    )
    coef, u, src, cdiag, scale, c1, c2, r1, r2 = call(
        sweep1_kernel, [seam, block, block, block, block, seam, seam, seam, seam],
        keep(pos, arrived, coarse_init, coarse_leak, near),
        [chot, chot, vmem((CB, 2 * NO * L), BF16)],
    )
    c1, c2 = exchange(COL, c1, c2, ring=True)
    r1, r2 = exchange(ROW, r1, r2)
    fine_drop = call(
        combine_kernel, [pltpu.MemorySpace.HBM((T, T), F32)], leave(hist) + keep(ahead, coef, rims),
        [vmem((STEPS, 4 - AHEAD, LT, T // STEPS, L), F32), tile, pltpu.SemaphoreType.DMA((STEPS,)),
         pltpu.SemaphoreType.DMA((STEPS,))], flops=big // 4, any_in=1, any_out=1,
    )[0]
    coarse_drop = call(
        sweep2_kernel, [hbm((CB, CB), F32)], keep(pos, u, src, cdiag, scale, c1, c2, r1, r2)    )[0]
    return fine_drop, coarse_drop


def solution(mesh):
    spec = P(ROW, COL)

    return jax.shard_map(
        per_device, mesh=mesh, in_specs=(spec,) * 8, out_specs=(spec, spec), check_vma=False
    )
```
